128 devices in a mesh: sys: 1, zdom: 64 (over z, y, x), ydom: 2 (over core).
Axes of the slice: x: 4, y: 4, z: 4, core: 2. Of those that a mesh axis runs over, the one named last changes fastest.
Arguments:
- charge: float32 [2097152], P(('sys', 'ydom', 'zdom'))
- real_mask: int32 [2097152], P(('sys', 'ydom', 'zdom'))
- grid_idx: int32 [2097152, 3], P(('sys', 'ydom', 'zdom'))
- spline_w: float32 [2097152, 3, 4], P(('sys', 'ydom', 'zdom'))
- influence: float32 [256, 256, 256], P(('sys', 'ydom'), 'zdom')
Outputs:
- output 1: float32 [256, 256, 256], P(('sys', 'ydom'), 'zdom')
- output 2: float32 [1], P('sys')
All inputs are finite; a program needn't handle non-finite values.
Results may differ from the reference program's by a relative error of at most 0.001.
Values are sent between devices in bfloat16 or wider.
A program may use at most 1 GiB of HBM per device.

```python
import jax
import jax.numpy as jnp
from jax import lax

GRID_SIDE = 256
PER_DEV = 16384
Y_DEVS = 2
Z_DEVS = 64


def bspline_weights(frac_part):
    frac_sq = frac_part * frac_part
    frac_cube = frac_sq * frac_part
    w_zero = (1.0 - frac_part) * (1.0 - frac_part) * (1.0 - frac_part) / 6.0
    w_one = (3.0 * frac_cube - 6.0 * frac_sq + 4.0) / 6.0
    w_two = (-3.0 * frac_cube + 3.0 * frac_sq + 3.0 * frac_part + 1.0) / 6.0
    w_three = frac_cube / 6.0
    return jnp.stack([w_zero, w_one, w_two, w_three], axis=-1)


def edge_index(key, count, length):
    key_near, key_edge, key_any = jax.random.split(key, 3)
    near_edge = jax.random.randint(key_near, (count,), 0, 2)
    at_edge = length - 3 + jax.random.randint(key_edge, (count,), 0, 3)
    anywhere = jax.random.randint(key_any, (count,), 0, length)
    return jnp.where(near_edge == 1, at_edge, anywhere)


def setup_inputs(seed: int = 0, part: int = 0) -> dict:
    dev_count = Y_DEVS * Z_DEVS
    slot_count = dev_count * PER_DEV
    len_y = GRID_SIDE // Y_DEVS
    len_z = GRID_SIDE // Z_DEVS
    sub_keys = jax.random.split(jax.random.fold_in(jax.random.key(seed), part), 8)
    real_count = jax.random.randint(sub_keys[0], (dev_count, 1), PER_DEV // 8, PER_DEV + 1)
    slot_rank = jax.random.randint(sub_keys[1], (dev_count, PER_DEV), 0, PER_DEV)
    real_mask = (slot_rank < real_count).astype(jnp.int32).reshape(slot_count)
    x_idx = jax.random.randint(sub_keys[2], (slot_count,), 0, GRID_SIDE)
    y_idx = edge_index(sub_keys[3], slot_count, len_y)
    z_idx = edge_index(sub_keys[4], slot_count, len_z)
    grid_idx = jnp.stack([x_idx, y_idx, z_idx], axis=1).astype(jnp.int32)
    charge = jax.random.normal(sub_keys[5], (slot_count,), jnp.float32)
    frac_part = jax.random.uniform(sub_keys[6], (slot_count, 3), jnp.float32)
    spline_w = bspline_weights(frac_part).astype(jnp.float32)
    influence = jax.random.uniform(sub_keys[7], (GRID_SIDE, GRID_SIDE, GRID_SIDE), jnp.float32, 0.5, 1.5) * (20.0 / slot_count)
    return {'charge': charge, 'real_mask': real_mask, 'grid_idx': grid_idx, 'spline_w': spline_w, 'influence': influence}


def reference(charge, real_mask, grid_idx, spline_w, influence):
    slot_count = Y_DEVS * Z_DEVS * PER_DEV
    len_y = GRID_SIDE // Y_DEVS
    len_z = GRID_SIDE // Z_DEVS
    device = jnp.arange(slot_count) // PER_DEV
    base_x = grid_idx[:, 0]
    base_y = grid_idx[:, 1] + (device // Z_DEVS) * len_y
    base_z = grid_idx[:, 2] + (device % Z_DEVS) * len_z
    weight = charge * real_mask.astype(charge.dtype)

    def add_tap(flat_grid, tap_id):
        off_x = tap_id // 16
        off_y = (tap_id // 4) % 4
        off_z = tap_id % 4
        pos_x = (base_x + off_x) % GRID_SIDE
        pos_y = (base_y + off_y) % GRID_SIDE
        pos_z = (base_z + off_z) % GRID_SIDE
        tap_value = weight * spline_w[:, 0, off_x] * spline_w[:, 1, off_y] * spline_w[:, 2, off_z]
        flat_idx = (pos_x * GRID_SIDE + pos_y) * GRID_SIDE + pos_z
        return flat_grid.at[flat_idx].add(tap_value), None

    flat_grid = lax.scan(add_tap, jnp.zeros((GRID_SIDE * GRID_SIDE * GRID_SIDE,), charge.dtype), jnp.arange(64))[0]
    charge_grid = flat_grid.reshape(GRID_SIDE, GRID_SIDE, GRID_SIDE)
    spectrum = jnp.fft.fftn(charge_grid)
    mode_energy = 0.5 * influence * (spectrum.real * spectrum.real + spectrum.imag * spectrum.imag)
    energy = jnp.sum(mode_energy) / (GRID_SIDE * GRID_SIDE * GRID_SIDE)
    return mode_energy, jnp.reshape(energy, (1,))
```

```python
import functools
import math
import jax
import jax.numpy as jnp
from jax import lax
from jax.experimental import pallas as pl
from jax.experimental.pallas import tpu as pltpu
from jax.sharding import PartitionSpec as P

PRECISE = lax.Precision.HIGHEST
GHOST_PLANES = 3
F32 = jnp.float32
BF16 = jnp.bfloat16
SUB = 256
CHUNK = 1024


def split_bf16(value):
    high = value.astype(BF16)
    return high, (value - high.astype(F32)).astype(BF16)


def dot_t(lhs, rhs):
    return lax.dot_general(lhs, rhs, (((1,), (1,)), ((), ())), preferred_element_type=F32)


def spread_kernel(len_y, q_ref, m_ref, idx_ref, w_ref, out_ref, xh_ref, xl_ref, ph_ref, pl_ref):
    grid_n = out_ref.shape[1]

    @pl.when(pl.program_id(0) == 0)
    def _():
        out_ref[...] = jnp.zeros_like(out_ref)

    total = None
    for sub in range(CHUNK // SUB):
        slot = sub % 2
        cols = pl.ds(sub * SUB, SUB)
        weight = q_ref[:, cols] * m_ref[:, cols].astype(F32)
        tap = lax.broadcasted_iota(jnp.int32, (4, SUB), 0)
        pos_x = ((idx_ref[0:1, cols] + tap) % grid_n).astype(F32).astype(BF16)
        pos_y = idx_ref[1:2, cols] + tap
        pos_z = idx_ref[2:3, cols] + tap
        wxh, wxl = split_bf16(w_ref[0, :, cols] * weight)
        wy = w_ref[1, :, cols]
        wz = w_ref[2, :, cols]

        row_x = lax.broadcasted_iota(jnp.int32, (grid_n, SUB), 0).astype(F32).astype(BF16)
        line_h = jnp.zeros((grid_n, SUB), BF16)
        line_l = jnp.zeros((grid_n, SUB), BF16)
        for s in range(4):
            hit = row_x == pos_x[s:s + 1]
            line_h = jnp.where(hit, wxh[s:s + 1], line_h)
            line_l = jnp.where(hit, wxl[s:s + 1], line_l)
        xh_ref[slot] = line_h
        xl_ref[slot] = line_l

        row_8 = lax.broadcasted_iota(jnp.int32, (8, SUB), 0)
        line_z = jnp.zeros((8, SUB), F32)
        ghost_y = jnp.zeros((8, SUB), F32)
        row_y = lax.broadcasted_iota(jnp.int32, (len_y, SUB), 0)
        line_y = jnp.zeros((len_y, SUB), F32)
        for t in range(4):
            line_z = jnp.where(row_8 == pos_z[t:t + 1], wz[t:t + 1], line_z)
            ghost_y = jnp.where(row_8 + len_y == pos_y[t:t + 1], wy[t:t + 1], ghost_y)
            line_y = jnp.where(row_y == pos_y[t:t + 1], wy[t:t + 1], line_y)
        for z in range(7):
            high, low = split_bf16(line_y * line_z[z:z + 1])
            ph_ref[slot, z * len_y:(z + 1) * len_y, :] = high
            pl_ref[slot, z * len_y:(z + 1) * len_y, :] = low
        ghosts = jnp.concatenate([line_z * ghost_y[g:g + 1] for g in range(3)] + [jnp.zeros((8, SUB), F32)], axis=0)
        high, low = split_bf16(ghosts)
        ph_ref[slot, 7 * len_y:, :] = high
        pl_ref[slot, 7 * len_y:, :] = low

        part = dot_t(ph_ref[slot], xh_ref[slot]) + dot_t(pl_ref[slot], xh_ref[slot]) + dot_t(ph_ref[slot], xl_ref[slot])
        out_ref[...] += part


def spread_block(charge, real_mask, grid_idx, spline_w, grid_n, len_y, len_z):
    slots = charge.shape[0]
    rows = (len_z + 3) * len_y + 32
    return pl.pallas_call(
        functools.partial(spread_kernel, len_y),
        grid=(slots // CHUNK,),
        in_specs=[
            pl.BlockSpec((1, CHUNK), lambda i: (0, i)),
            pl.BlockSpec((1, CHUNK), lambda i: (0, i)),
            pl.BlockSpec((3, CHUNK), lambda i: (0, i)),
            pl.BlockSpec((3, 4, CHUNK), lambda i: (0, 0, i)),
        ],
        out_specs=pl.BlockSpec((rows, grid_n), lambda i: (0, 0)),
        out_shape=jax.ShapeDtypeStruct((rows, grid_n), F32),
        scratch_shapes=[pltpu.VMEM((2, grid_n, SUB), BF16), pltpu.VMEM((2, grid_n, SUB), BF16), pltpu.VMEM((2, rows, SUB), BF16), pltpu.VMEM((2, rows, SUB), BF16)],
        name="spread",
    )(charge.reshape(1, slots), real_mask.reshape(1, slots), grid_idx.T, jnp.transpose(spline_w, (1, 2, 0)))


def dft_parts(grid_n, freq_rows):
    phase_idx = (freq_rows[:, None] * jnp.arange(grid_n)[None, :]) % grid_n
    angle_rad = phase_idx.astype(jnp.float32) * (2.0 * math.pi / grid_n)
    return jnp.cos(angle_rad), jnp.sin(angle_rad)


def real_dft(cos_part, sine_part):
    return jnp.stack([cos_part, -sine_part])


def complex_dft(cos_part, sine_part):
    return jnp.stack([jnp.stack([cos_part, sine_part]), jnp.stack([-sine_part, cos_part])])


def fold_ghosts(ext_block, axis_name, axis_size, axis_dim, length):
    ghost_slab = lax.slice_in_dim(ext_block, length, length + GHOST_PLANES, axis=axis_dim)
    recv_slab = lax.ppermute(ghost_slab, axis_name, [(source, (source + 1) % axis_size) for source in range(axis_size)])
    head_planes = lax.slice_in_dim(ext_block, 0, GHOST_PLANES, axis=axis_dim) + recv_slab
    rest_planes = lax.slice_in_dim(ext_block, GHOST_PLANES, length, axis=axis_dim)
    return jnp.concatenate([head_planes, rest_planes], axis=axis_dim)


def sum_kernel(y_devs, z_devs, part_ref, out_ref, all_ref, send_sem, recv_sem):
    my_y = lax.axis_index('ydom')
    my_z = lax.axis_index('zdom')
    devs = y_devs * z_devs
    me = my_z * y_devs + my_y

    def place(step):
        other = lax.rem(me + step, devs)
        return {'zdom': other // y_devs, 'ydom': lax.rem(other, y_devs)}

    barrier = pltpu.get_barrier_semaphore()

    @pl.loop(1, devs)
    def _(step):
        pl.semaphore_signal(barrier, inc=1, device_id=place(step), device_id_type=pl.DeviceIdType.MESH)

    pl.semaphore_wait(barrier, devs - 1)

    def copy_to(step):
        return pltpu.make_async_remote_copy(src_ref=part_ref, dst_ref=all_ref.at[me], send_sem=send_sem.at[step], recv_sem=recv_sem.at[me], device_id=place(step), device_id_type=pl.DeviceIdType.MESH)

    def copy_from(source):
        return pltpu.make_async_remote_copy(src_ref=part_ref, dst_ref=all_ref.at[source], send_sem=send_sem.at[0], recv_sem=recv_sem.at[source], device_id=place(0), device_id_type=pl.DeviceIdType.MESH)

    @pl.loop(1, devs)
    def _(step):
        copy_to(step).start()

    all_ref[me] = part_ref[...]

    @pl.loop(1, devs)
    def _(step):
        copy_from(lax.rem(me + step, devs)).wait_recv()

    @pl.loop(1, devs)
    def _(step):
        copy_to(step).wait_send()

    out_ref[...] = jnp.sum(all_ref[...], axis=0)


def all_sum(tile, y_devs, z_devs):
    devs = y_devs * z_devs
    return pl.pallas_call(
        functools.partial(sum_kernel, y_devs, z_devs),
        out_shape=jax.ShapeDtypeStruct(tile.shape, F32),
        in_specs=[pl.BlockSpec(memory_space=pltpu.VMEM)],
        out_specs=pl.BlockSpec(memory_space=pltpu.VMEM),
        scratch_shapes=[pltpu.VMEM((devs,) + tile.shape, F32), pltpu.SemaphoreType.DMA((devs,)), pltpu.SemaphoreType.DMA((devs,))],
        compiler_params=pltpu.CompilerParams(collective_id=0, has_side_effects=True),
        name="all_sum",
    )(tile)


def solution(mesh):
    y_devs = mesh.shape['ydom']
    z_devs = mesh.shape['zdom']
    slot_spec = P(('sys', 'ydom', 'zdom'))
    mode_spec = P(('sys', 'ydom'), 'zdom', None)

    def local_energy(charge, real_mask, grid_idx, spline_w, influence):
        grid_n = influence.shape[2]
        len_y = grid_n // y_devs
        len_z = grid_n // z_devs
        flat = spread_block(charge, real_mask, grid_idx, spline_w, grid_n, len_y, len_z)
        planes = flat[:7 * len_y].reshape(7, len_y, grid_n)
        ghosts = flat[7 * len_y:7 * len_y + 24].reshape(3, 8, grid_n)[:, :7]
        extended = jnp.concatenate([planes, jnp.transpose(ghosts, (1, 0, 2))], axis=1)
        extended = jnp.transpose(extended, (2, 1, 0))
        folded_y = fold_ghosts(extended, 'ydom', y_devs, 1, len_y)
        charge_grid = fold_ghosts(folded_y, 'zdom', z_devs, 2, len_z)
        cos_part, sine_part = dft_parts(grid_n, jnp.arange(grid_n))
        full_dft = complex_dft(cos_part, sine_part)
        stage_x = jnp.einsum('rkx,xyz->rkyz', real_dft(cos_part, sine_part), charge_grid, precision=PRECISE, preferred_element_type=jnp.float32)
        stage_x = lax.all_to_all(stage_x, 'ydom', 1, 2, tiled=True)
        stage_y = jnp.einsum('abky,bxyz->axkz', full_dft, stage_x, precision=PRECISE, preferred_element_type=jnp.float32)
        stage_y = lax.all_to_all(stage_y, 'zdom', 2, 3, tiled=True)
        stage_z = jnp.einsum('abkz,bxyz->axyk', full_dft, stage_y, precision=PRECISE, preferred_element_type=jnp.float32)
        mode_energy = 0.5 * influence * (stage_z[0] * stage_z[0] + stage_z[1] * stage_z[1])
        tile = jnp.sum(mode_energy.reshape(8, -1, 128), axis=1)
        energy = jnp.sum(all_sum(tile, y_devs, z_devs)) / (grid_n * grid_n * grid_n)
        return mode_energy, jnp.reshape(energy, (1,))

    return jax.shard_map(local_energy, mesh=mesh, in_specs=(slot_spec, slot_spec, P(('sys', 'ydom', 'zdom'), None), P(('sys', 'ydom', 'zdom'), None, None), mode_spec), out_specs=(mode_spec, P('sys')), check_vma=False)
```

```python
import functools
import math
import jax
import jax.numpy as jnp
import numpy as np
from jax import lax
from jax.experimental import pallas as pl
from jax.experimental.pallas import tpu as pltpu
from jax.sharding import PartitionSpec as P

F32 = jnp.float32
BF16 = jnp.bfloat16
SUB = 256
CHUNK = 1024
GROUPS = ((0, 1), (2, 3), (4, 5), (6,))
STEP_AT = 5
CODE_MAX = 32767.0
MESH = pl.DeviceIdType.MESH


def split_bf16(value):
    high = value.astype(BF16)
    return high, (value - high.astype(F32)).astype(BF16)


def dot3(lhs, rhs):
    def dot(a, b):
        return jnp.dot(a, b, preferred_element_type=F32)
    return dot(lhs[0], rhs[0]) + dot(lhs[1], rhs[0]) + dot(lhs[0], rhs[1])


def np_split(value):
    value = np.asarray(value, np.float32)
    high = value.astype(BF16)
    return np.stack([high, (value - high.astype(np.float32)).astype(BF16)])


def dft_tables(grid_n, y_devs, z_devs):
    turn = 2.0 * np.pi / grid_n
    len_y, len_z = grid_n // y_devs, grid_n // z_devs
    x = np.arange(grid_n)
    freq = np.arange(grid_n)
    phase_x = (np.outer(x, freq) % grid_n) * turn
    table_x = np.stack([np_split(np.concatenate([np.cos(phase_x[:, i * len_y:(i + 1) * len_y]), -np.sin(phase_x[:, i * len_y:(i + 1) * len_y])], axis=1)) for i in range(y_devs)])
    phase_y = (np.outer(freq, x) % grid_n) * turn
    real = np.concatenate([np.cos(phase_y), np.sin(phase_y)], axis=1)
    imag = np.concatenate([-np.sin(phase_y), np.cos(phase_y)], axis=1)
    rows = np.stack([real.reshape(z_devs, len_z, 2 * grid_n), imag.reshape(z_devs, len_z, 2 * grid_n)], axis=1)
    table_y = np_split(rows.reshape(2 * grid_n, 2 * grid_n))
    table_z = []
    for first in (0, 2):
        pos = np.arange(z_devs)[:, None] * len_z + first + np.arange(2)[None, :]
        phase_z = ((freq[:, None, None] * pos[None]) % grid_n) * turn
        real = np.stack([np.cos(phase_z), np.sin(phase_z)], axis=3).reshape(grid_n, -1)
        imag = np.stack([-np.sin(phase_z), np.cos(phase_z)], axis=3).reshape(grid_n, -1)
        table_z.append(np_split(np.concatenate([real, imag], axis=0)))
    return table_x, table_y, np.stack(table_z)


def energy_kernel(y_devs, z_devs, q_ref, m_ref, idx_ref, w_ref, bc_hbm, tx_hbm, ty_hbm, tz_hbm, ek_hbm, sum_ref,
                  xh_ref, xl_ref, ph_ref, pl_ref, acc_ref, got_ref, grid_ref, mid_ref, code_ref, recv_ref, scale_ref, rscale_ref,
                  deq_ref, zed_ref, bc_ref, ek_ref, tx_ref, ty_ref, tz_ref, row_ref, rrow_ref,
                  load_sem, swap_sem, send_sem, recv_sem, ssend_sem, srecv_sem, row_sem):
    my_y = lax.axis_index('ydom')
    my_z = lax.axis_index('zdom')
    grid_n = xh_ref.shape[1]
    slots = q_ref.shape[1]
    len_y = grid_n // y_devs
    n_groups = len(GROUPS)
    barrier = pltpu.get_barrier_semaphore()
    partner = {'ydom': 1 - my_y}

    def chip(step):
        return (my_z + step) & (z_devs - 1)

    @pl.loop(1, z_devs)
    def _(step):
        pl.semaphore_signal(barrier, inc=1, device_id={'zdom': chip(step)}, device_id_type=MESH)

    pl.semaphore_signal(barrier, inc=1, device_id=partner, device_id_type=MESH)

    loads = [pltpu.make_async_copy(tx_hbm.at[my_y], tx_ref, load_sem.at[0]), pltpu.make_async_copy(ty_hbm, ty_ref, load_sem.at[1]),
             pltpu.make_async_copy(tz_hbm, tz_ref, load_sem.at[2]), pltpu.make_async_copy(bc_hbm, bc_ref, load_sem.at[3])]
    for load in loads:
        load.start()

    def swap(group):
        return pltpu.make_async_remote_copy(src_ref=acc_ref.at[group], dst_ref=got_ref.at[group], send_sem=swap_sem.at[0, group], recv_sem=swap_sem.at[1, group], device_id=partner, device_id_type=MESH)

    def send(group, step):
        other = chip(step)
        return (pltpu.make_async_remote_copy(src_ref=code_ref.at[group, other], dst_ref=recv_ref.at[group, my_z], send_sem=send_sem.at[group], recv_sem=recv_sem.at[group], device_id={'zdom': other}, device_id_type=MESH),
                pltpu.make_async_remote_copy(src_ref=scale_ref.at[group, pl.ds(0, 1)], dst_ref=rscale_ref.at[group, my_z, pl.ds(0, 1)], send_sem=ssend_sem.at[group], recv_sem=srecv_sem.at[group], device_id={'zdom': other}, device_id_type=MESH))

    def spread(group, base):
        planes = GROUPS[group]
        total = None
        for sub in range(CHUNK // SUB):
            slot = sub % 2
            cols = pl.ds(pl.multiple_of(base + sub * SUB, SUB), SUB)
            tap = lax.broadcasted_iota(jnp.int32, (4, SUB), 0)
            if group == 0:
                weight = q_ref[:, cols] * m_ref[:, cols].astype(F32)
                pos_x = ((idx_ref[0:1, cols] + tap) & (grid_n - 1)).astype(F32).astype(BF16)
                wxh, wxl = split_bf16(w_ref[0, :, cols] * weight)
                row_x = lax.broadcasted_iota(jnp.int32, (grid_n, SUB), 0).astype(F32).astype(BF16)
                line_h = jnp.zeros((grid_n, SUB), BF16)
                line_l = jnp.zeros((grid_n, SUB), BF16)
                for s in range(4):
                    hit = row_x == pos_x[s:s + 1]
                    line_h = jnp.where(hit, wxh[s:s + 1], line_h)
                    line_l = jnp.where(hit, wxl[s:s + 1], line_l)
                xh_ref[cols, :] = line_h.T
                xl_ref[cols, :] = line_l.T
            pos_y = idx_ref[1:2, cols] + tap
            pos_z = idx_ref[2:3, cols] + tap
            wy = w_ref[1, :, cols]
            wz = w_ref[2, :, cols]
            row_8 = lax.broadcasted_iota(jnp.int32, (8, SUB), 0)
            line_z = jnp.zeros((8, SUB), F32)
            ghost_y = jnp.zeros((8, SUB), F32)
            row_y = lax.broadcasted_iota(jnp.int32, (len_y, SUB), 0)
            line_y = jnp.zeros((len_y, SUB), F32)
            for t in range(4):
                line_z = jnp.where(row_8 == pos_z[t:t + 1], wz[t:t + 1], line_z)
                ghost_y = jnp.where(row_8 + len_y == pos_y[t:t + 1], wy[t:t + 1], ghost_y)
                line_y = jnp.where(row_y == pos_y[t:t + 1], wy[t:t + 1], line_y)
            for k, z in enumerate(planes):
                high, low = split_bf16(line_y * line_z[z:z + 1])
                ph_ref[slot, k * len_y:(k + 1) * len_y, :] = high
                pl_ref[slot, k * len_y:(k + 1) * len_y, :] = low
            ghosts = [ghost_y * line_z[z:z + 1] for z in planes]
            if len(planes) == 1:
                ghosts.append(jnp.zeros((8, SUB), F32))
            high, low = split_bf16(jnp.concatenate(ghosts, axis=0))
            top = len(planes) * len_y
            ph_ref[slot, top:top + 16, :] = high
            pl_ref[slot, top:top + 16, :] = low
            rows = pl.ds(0, top + 16)
            part = dot3((ph_ref[slot, rows, :], pl_ref[slot, rows, :]), (xh_ref[cols, :], xl_ref[cols, :]))
            total = part if total is None else total + part
        acc_ref[group, rows, :] += total

    def transform_send(group):
        planes = GROUPS[group]
        swap(group).wait()
        mine, theirs = my_y * len_y, (1 - my_y) * len_y
        for k in range(len(planes)):
            block = pl.ds(k * len_y, len_y)
            grid_ref[pl.ds(pl.multiple_of(k * grid_n + mine, len_y), len_y), :] = acc_ref[group, block, :]
            grid_ref[pl.ds(pl.multiple_of(k * grid_n + theirs, len_y), len_y), :] = got_ref[group, block, :]
        for k in range(len(planes)):
            ghost = pl.ds(len(planes) * len_y + 8 * k, 8)
            grid_ref[pl.ds(pl.multiple_of(k * grid_n + theirs, len_y), 8), :] += acc_ref[group, ghost, :]
            grid_ref[pl.ds(pl.multiple_of(k * grid_n + mine, len_y), 8), :] += got_ref[group, ghost, :]
        size = len(planes) * grid_n
        half = grid_n // 2
        mid_ref[pl.ds(0, size), :] = dot3(split_bf16(grid_ref[pl.ds(0, size), :]), (tx_ref[0], tx_ref[1]))
        columns = [jnp.concatenate([mid_ref[pl.ds(k * grid_n, grid_n), pl.ds(c * half, half)] for c in range(2)], axis=0) for k in range(len(planes))]
        modes = dot3((ty_ref[0], ty_ref[1]), split_bf16(jnp.concatenate(columns, axis=1)))
        grid_ref[:, pl.ds(0, len(planes) * half)] = modes
        peak = jnp.maximum(jnp.max(jnp.abs(modes), keepdims=True), 1e-30)
        parts = [(grid_ref[:, pl.ds(k * half, half)] * (CODE_MAX / peak)).reshape(z_devs, 8, half) for k in range(len(planes))]
        if len(planes) == 1:
            parts.append(jnp.zeros((z_devs, 8, half), F32))
        codes = jnp.round(jnp.concatenate(parts, axis=1)).astype(jnp.int32).astype(jnp.int16)
        code_ref[group] = codes
        scale_ref[group] = jnp.broadcast_to(peak * (1.0 / CODE_MAX), (8, 128))

        @pl.loop(1, z_devs)
        def _(step):
            for copy in send(group, step):
                copy.start()

        recv_ref[group, my_z] = code_ref[group, my_z]
        rscale_ref[group, my_z, pl.ds(0, 1)] = scale_ref[group, pl.ds(0, 1)]

    def decode(group):
        pltpu.make_async_copy(recv_ref.at[group, pl.ds(0, z_devs - 1)], recv_ref.at[group, pl.ds(0, z_devs - 1)], recv_sem.at[group]).wait()
        pltpu.make_async_copy(rscale_ref.at[group, pl.ds(0, z_devs - 1), pl.ds(0, 1)], rscale_ref.at[group, pl.ds(0, z_devs - 1), pl.ds(0, 1)], srecv_sem.at[group]).wait()
        return recv_ref[group].astype(jnp.int32).astype(F32) * rscale_ref[group, :, pl.ds(0, 1), :]

    def transform_z(part):
        flat = deq_ref.at[part]
        columns = [flat[pl.ds(ky, grid_n, stride=4), :] for ky in range(4)]
        zed = dot3((tz_ref[part, 0], tz_ref[part, 1]), split_bf16(jnp.concatenate(columns, axis=1)))
        if part == 0:
            zed_ref[...] = zed
        else:
            zed_ref[...] += zed

    acc_ref[...] = jnp.zeros_like(acc_ref)
    for group in range(n_groups):
        @pl.loop(0, slots // CHUNK)
        def _(i):
            spread(group, i * CHUNK)
            if group:
                @pl.when(i == STEP_AT)
                def _():
                    transform_send(group - 1)

        if group == 0:
            pl.semaphore_wait(barrier, z_devs)
            for load in loads:
                load.wait()
        swap(group).start()
    transform_send(n_groups - 1)

    rows = z_devs * 16
    first = decode(0)
    late = decode(2)
    deq_ref[0] = first.reshape(rows, 128)
    deq_ref[0, pl.ds(16, rows - 16), :] += late[:z_devs - 1].reshape(rows - 16, 128)
    deq_ref[0, pl.ds(0, 16), :] += late[z_devs - 1]
    transform_z(0)
    deq_ref[1] = decode(1).reshape(rows, 128)
    late = decode(3)
    deq_ref[1, pl.ds(16, rows - 16), :] += late[:z_devs - 1].reshape(rows - 16, 128)
    deq_ref[1, pl.ds(0, 16), :] += late[z_devs - 1]
    transform_z(1)

    half = grid_n // 2
    row = jnp.zeros((8, grid_n), F32)
    for ky in range(4):
        cols = pl.ds(ky * half, half)
        real, imag = zed_ref[pl.ds(0, grid_n), cols], zed_ref[pl.ds(grid_n, grid_n), cols]
        value = 0.5 * bc_ref[:, ky, :] * (real * real + imag * imag).T
        ek_ref[:, ky, :] = value
        row += jnp.sum(value.reshape(half // 8, 8, grid_n), axis=0)
    store = pltpu.make_async_copy(ek_ref, ek_hbm, load_sem.at[0])
    store.start()
    row_ref[0] = jnp.broadcast_to(jnp.sum(row[:, :half] + row[:, half:], axis=0, keepdims=True), (8, half))

    def pair_copy():
        return pltpu.make_async_remote_copy(src_ref=row_ref.at[0], dst_ref=row_ref.at[1], send_sem=row_sem.at[0], recv_sem=row_sem.at[1], device_id=partner, device_id_type=MESH)

    def row_copy(step):
        return pltpu.make_async_remote_copy(src_ref=row_ref.at[2, pl.ds(0, 1)], dst_ref=rrow_ref.at[my_z, pl.ds(0, 1)], send_sem=row_sem.at[2], recv_sem=row_sem.at[3], device_id={'zdom': chip(step)}, device_id_type=MESH)

    pair_copy().start()
    pair_copy().wait()
    row_ref[2] = row_ref[0] + row_ref[1]

    @pl.loop(1, z_devs)
    def _(step):
        row_copy(step).start()

    rrow_ref[my_z, pl.ds(0, 1)] = row_ref[2, pl.ds(0, 1)]
    others = rrow_ref.at[pl.ds(0, z_devs - 1), pl.ds(0, 1)]
    pltpu.make_async_copy(others, others, row_sem.at[3]).wait()
    sum_ref[0] = jnp.sum(rrow_ref[:, pl.ds(0, 1), :]) * (1.0 / (grid_n * grid_n * grid_n))
    pltpu.make_async_copy(others, others, row_sem.at[2]).wait()
    for group in range(n_groups):
        sent = code_ref.at[group, pl.ds(0, z_devs - 1)]
        pltpu.make_async_copy(sent, sent, send_sem.at[group]).wait()
        sent = rscale_ref.at[group, pl.ds(0, z_devs - 1), pl.ds(0, 1)]
        pltpu.make_async_copy(sent, sent, ssend_sem.at[group]).wait()
    store.wait()


def solution(mesh):
    y_devs = mesh.shape['ydom']
    z_devs = mesh.shape['zdom']
    slot_spec = P(('sys', 'ydom', 'zdom'))
    mode_spec = P(('sys', 'ydom'), 'zdom', None)

    def local_energy(charge, real_mask, grid_idx, spline_w, influence):
        grid_n = influence.shape[2]
        slots = charge.shape[0]
        half = grid_n // 2
        n_groups = len(GROUPS)
        table_x, table_y, table_z = dft_tables(grid_n, y_devs, z_devs)
        any_spec = pl.BlockSpec(memory_space=pl.ANY)
        vmem_spec = pl.BlockSpec(memory_space=pltpu.VMEM)
        rows = grid_n + 16
        mode_energy, energy = pl.pallas_call(
            functools.partial(energy_kernel, y_devs, z_devs),
            in_specs=[vmem_spec] * 4 + [any_spec] * 4,
            out_specs=[any_spec, pl.BlockSpec(memory_space=pltpu.SMEM)],
            out_shape=[jax.ShapeDtypeStruct(influence.shape, F32), jax.ShapeDtypeStruct((1,), F32)],
            scratch_shapes=[
                pltpu.VMEM((slots, grid_n), BF16), pltpu.VMEM((slots, grid_n), BF16),
                pltpu.VMEM((2, rows, SUB), BF16), pltpu.VMEM((2, rows, SUB), BF16),
                pltpu.VMEM((n_groups, rows, grid_n), F32), pltpu.VMEM((n_groups, rows, grid_n), F32),
                pltpu.VMEM((2 * grid_n, grid_n), F32), pltpu.VMEM((2 * grid_n, grid_n), F32),
                pltpu.VMEM((n_groups, z_devs, 16, half), jnp.int16), pltpu.VMEM((n_groups, z_devs, 16, half), jnp.int16),
                pltpu.VMEM((n_groups, 8, 128), F32), pltpu.VMEM((n_groups, z_devs, 8, 128), F32),
                pltpu.VMEM((2, z_devs * 16, half), F32), pltpu.VMEM((2 * grid_n, 4 * half), F32),
                pltpu.VMEM(influence.shape, F32), pltpu.VMEM(influence.shape, F32),
                pltpu.VMEM(table_x.shape[1:], BF16), pltpu.VMEM(table_y.shape, BF16), pltpu.VMEM(table_z.shape, BF16),
                pltpu.VMEM((3, 8, 128), F32), pltpu.VMEM((z_devs, 8, 128), F32),
                pltpu.SemaphoreType.DMA((4,)), pltpu.SemaphoreType.DMA((2, n_groups)),
                pltpu.SemaphoreType.DMA((n_groups,)), pltpu.SemaphoreType.DMA((n_groups,)),
                pltpu.SemaphoreType.DMA((n_groups,)), pltpu.SemaphoreType.DMA((n_groups,)),
                pltpu.SemaphoreType.DMA((4,)),
            ],
            compiler_params=pltpu.CompilerParams(collective_id=0, has_side_effects=True, vmem_limit_bytes=60 * 1024 * 1024),
            name="energy",
        )(charge.reshape(1, slots), real_mask.reshape(1, slots), grid_idx.T, jnp.transpose(spline_w, (1, 2, 0)), influence, jnp.asarray(table_x), jnp.asarray(table_y), jnp.asarray(table_z))
        return mode_energy, energy

    return jax.shard_map(local_energy, mesh=mesh, in_specs=(slot_spec, slot_spec, P(('sys', 'ydom', 'zdom'), None), P(('sys', 'ydom', 'zdom'), None, None), mode_spec), out_specs=(mode_spec, P('sys')), check_vma=False)
```

```python
import functools
import math
import jax
import jax.numpy as jnp
import numpy as np
from jax import lax
from jax.experimental import pallas as pl
from jax.experimental.pallas import tpu as pltpu
from jax.sharding import PartitionSpec as P

F32 = jnp.float32
BF16 = jnp.bfloat16
SUB = 256
CHUNK = 1024
GROUPS = ((0, 1, 2, 3), (4, 5), (6,))
STEP_AT = (0, 5, 7)
EARLY = 2048
CODE_MAX = 32767.0
MESH = pl.DeviceIdType.MESH


def split_bf16(value):
    high = value.astype(BF16)
    return high, (value - high.astype(F32)).astype(BF16)


def dot3(lhs, rhs):
    def dot(a, b):
        return jnp.dot(a, b, preferred_element_type=F32)
    return dot(lhs[0], rhs[0]) + dot(lhs[1], rhs[0]) + dot(lhs[0], rhs[1])


def np_split(value):
    value = np.asarray(value, np.float32)
    high = value.astype(BF16)
    return np.stack([high, (value - high.astype(np.float32)).astype(BF16)])


def dft_tables(grid_n, y_devs, z_devs):
    turn = 2.0 * np.pi / grid_n
    len_y, len_z = grid_n // y_devs, grid_n // z_devs
    x = np.arange(grid_n)
    freq = np.arange(grid_n)
    phase_x = (np.outer(x, freq) % grid_n) * turn
    table_x = np.stack([np_split(np.concatenate([np.cos(phase_x[:, i * len_y:(i + 1) * len_y]), -np.sin(phase_x[:, i * len_y:(i + 1) * len_y])], axis=1)) for i in range(y_devs)])
    phase_y = (np.outer(freq, x) % grid_n) * turn
    real = np.concatenate([np.cos(phase_y), np.sin(phase_y)], axis=1)
    imag = np.concatenate([-np.sin(phase_y), np.cos(phase_y)], axis=1)
    rows = np.stack([real.reshape(z_devs, len_z, 2 * grid_n), imag.reshape(z_devs, len_z, 2 * grid_n)], axis=1)
    table_y = np_split(rows.reshape(2 * grid_n, 2 * grid_n))
    table_z = []
    for first in (0, 2):
        pos = np.arange(z_devs)[:, None] * len_z + first + np.arange(2)[None, :]
        phase_z = ((freq[:, None, None] * pos[None]) % grid_n) * turn
        real = np.stack([np.cos(phase_z), np.sin(phase_z)], axis=3).reshape(grid_n, -1)
        imag = np.stack([-np.sin(phase_z), np.cos(phase_z)], axis=3).reshape(grid_n, -1)
        table_z.append(np_split(np.concatenate([real, imag], axis=0)))
    return table_x, table_y, np.stack(table_z)


def ghost_rows(group):
    return -(-8 * len(GROUPS[group]) // 16) * 16


def energy_kernel(y_devs, z_devs, q_hbm, m_hbm, idx_hbm, w_hbm, bc_hbm, tx_hbm, ty_hbm, tz_hbm, ek_hbm, sum_ref,
                  q_ref, m_ref, idx_ref, w_ref, line_ref, xh_ref, xl_ref, ph_ref, pl_ref, acc_refs, got_refs, grid_ref, mid_ref, mode_ref,
                  code_refs, recv_refs, scale_ref, rscale_ref,
                  deq_ref, zed_ref, bc_ref, ek_ref, tx_ref, ty_ref, tz_ref, row_ref, rrow_ref,
                  early_sem, load_sem, swap_sem, send_sem, recv_sem, ssend_sem, srecv_sem, row_sem):
    my_y = lax.axis_index('ydom')
    my_z = lax.axis_index('zdom')
    grid_n = xh_ref.shape[1]
    slots = q_ref.shape[1]
    len_y = grid_n // y_devs
    half = grid_n // 2
    n_groups = len(GROUPS)
    barrier = pltpu.get_barrier_semaphore()
    partner = {'ydom': 1 - my_y}

    def chip(step):
        return (my_z + step) & (z_devs - 1)

    def slot_loads(piece):
        cols = pl.ds(0, EARLY) if piece == 0 else pl.ds(EARLY, slots - EARLY)
        return [pltpu.make_async_copy(hbm.at[lead + (cols,)], ref.at[lead + (cols,)], early_sem.at[piece, k])
                for k, (hbm, ref, lead) in enumerate(((q_hbm, q_ref, (slice(None),)), (m_hbm, m_ref, (slice(None),)), (idx_hbm, idx_ref, (slice(None),)), (w_hbm, w_ref, (slice(None), slice(None)))))]

    for piece in range(2):
        for load in slot_loads(piece):
            load.start()

    @pl.loop(1, z_devs)
    def _(step):
        pl.semaphore_signal(barrier, inc=1, device_id={'zdom': chip(step)}, device_id_type=MESH)

    pl.semaphore_signal(barrier, inc=1, device_id=partner, device_id_type=MESH)

    loads = [pltpu.make_async_copy(tx_hbm.at[my_y], tx_ref, load_sem.at[0]), pltpu.make_async_copy(ty_hbm, ty_ref, load_sem.at[1]),
             pltpu.make_async_copy(tz_hbm, tz_ref, load_sem.at[2]), pltpu.make_async_copy(bc_hbm, bc_ref, load_sem.at[3])]
    for load in loads:
        load.start()

    def swap(group):
        return pltpu.make_async_remote_copy(src_ref=acc_refs[group], dst_ref=got_refs[group], send_sem=swap_sem.at[0, group], recv_sem=swap_sem.at[1, group], device_id=partner, device_id_type=MESH)

    def send(group, step):
        other = chip(step)
        return pltpu.make_async_remote_copy(src_ref=code_refs[group].at[other], dst_ref=recv_refs[group].at[my_z], send_sem=send_sem.at[group], recv_sem=recv_sem.at[group], device_id={'zdom': other}, device_id_type=MESH)

    def send_scale(last, step):
        return pltpu.make_async_remote_copy(src_ref=scale_ref.at[last, pl.ds(0, 2 - last)], dst_ref=rscale_ref.at[last, my_z, pl.ds(0, 2 - last)], send_sem=ssend_sem.at[last], recv_sem=srecv_sem.at[last], device_id={'zdom': chip(step)}, device_id_type=MESH)

    def spread(group, base):
        planes = GROUPS[group]
        total = None
        for sub in range(CHUNK // SUB):
            slot = sub % 2
            cols = pl.ds(pl.multiple_of(base + sub * SUB, SUB), SUB)
            if group == 0:
                tap = lax.broadcasted_iota(jnp.int32, (4, SUB), 0)
                weight = q_ref[:, cols] * m_ref[:, cols].astype(F32)
                pos_x = ((idx_ref[0:1, cols] + tap) & (grid_n - 1)).astype(F32).astype(BF16)
                wxh, wxl = split_bf16(w_ref[0, :, cols] * weight)
                row_x = lax.broadcasted_iota(jnp.int32, (grid_n, SUB), 0).astype(F32).astype(BF16)
                line_h = jnp.zeros((grid_n, SUB), BF16)
                line_l = jnp.zeros((grid_n, SUB), BF16)
                for s in range(4):
                    hit = row_x == pos_x[s:s + 1]
                    line_h = jnp.where(hit, wxh[s:s + 1], line_h)
                    line_l = jnp.where(hit, wxl[s:s + 1], line_l)
                xh_ref[cols, :] = line_h.T
                xl_ref[cols, :] = line_l.T
                pos_y = idx_ref[1:2, cols] + tap
                pos_z = idx_ref[2:3, cols] + tap
                wy = w_ref[1, :, cols]
                wz = w_ref[2, :, cols]
                row_8 = lax.broadcasted_iota(jnp.int32, (8, SUB), 0)
                line_z = jnp.zeros((8, SUB), F32)
                ghost_y = jnp.zeros((8, SUB), F32)
                row_y = lax.broadcasted_iota(jnp.int32, (len_y, SUB), 0)
                line_y = jnp.zeros((len_y, SUB), F32)
                for t in range(4):
                    line_z = jnp.where(row_8 == pos_z[t:t + 1], wz[t:t + 1], line_z)
                    ghost_y = jnp.where(row_8 + len_y == pos_y[t:t + 1], wy[t:t + 1], ghost_y)
                    line_y = jnp.where(row_y == pos_y[t:t + 1], wy[t:t + 1], line_y)
                line_ref[pl.ds(0, len_y), cols] = line_y
                line_ref[pl.ds(len_y, 8), cols] = ghost_y
                line_ref[pl.ds(len_y + 8, 8), cols] = line_z
            else:
                line_y = line_ref[pl.ds(0, len_y), cols]
                ghost_y = line_ref[pl.ds(len_y, 8), cols]
                line_z = line_ref[pl.ds(len_y + 8, 8), cols]
            for k, z in enumerate(planes):
                high, low = split_bf16(line_y * line_z[z:z + 1])
                ph_ref[slot, k * len_y:(k + 1) * len_y, :] = high
                pl_ref[slot, k * len_y:(k + 1) * len_y, :] = low
            ghosts = [ghost_y * line_z[z:z + 1] for z in planes]
            if len(planes) % 2:
                ghosts.append(jnp.zeros((8, SUB), F32))
            high, low = split_bf16(jnp.concatenate(ghosts, axis=0))
            top = len(planes) * len_y
            rows = pl.ds(0, top + ghost_rows(group))
            ph_ref[slot, top:top + ghost_rows(group), :] = high
            pl_ref[slot, top:top + ghost_rows(group), :] = low
            part = dot3((ph_ref[slot, rows, :], pl_ref[slot, rows, :]), (xh_ref[cols, :], xl_ref[cols, :]))
            total = part if total is None else total + part
        acc_refs[group][...] += total

    def transform_send(group):
        planes = GROUPS[group]
        acc_ref, got_ref = acc_refs[group], got_refs[group]
        swap(group).wait()
        mine, theirs = my_y * len_y, (1 - my_y) * len_y
        peak = jnp.full((1, 1), 1e-30, F32)
        for first in range(0, len(planes), 2):
            count = min(2, len(planes) - first)
            for k in range(count):
                block = pl.ds((first + k) * len_y, len_y)
                grid_ref[pl.ds(pl.multiple_of(k * grid_n + mine, len_y), len_y), :] = acc_ref[block, :]
                grid_ref[pl.ds(pl.multiple_of(k * grid_n + theirs, len_y), len_y), :] = got_ref[block, :]
            for k in range(count):
                ghost = pl.ds(len(planes) * len_y + 8 * (first + k), 8)
                grid_ref[pl.ds(pl.multiple_of(k * grid_n + theirs, len_y), 8), :] += acc_ref[ghost, :]
                grid_ref[pl.ds(pl.multiple_of(k * grid_n + mine, len_y), 8), :] += got_ref[ghost, :]
            size = count * grid_n
            mid_ref[pl.ds(0, size), :] = dot3(split_bf16(grid_ref[pl.ds(0, size), :]), (tx_ref[0], tx_ref[1]))
            columns = [jnp.concatenate([mid_ref[pl.ds(k * grid_n, grid_n), pl.ds(c * half, half)] for c in range(2)], axis=0) for k in range(count)]
            modes = dot3((ty_ref[0], ty_ref[1]), split_bf16(jnp.concatenate(columns, axis=1)))
            mode_ref[:, pl.ds(first * half, count * half)] = modes
            peak = jnp.maximum(peak, jnp.max(jnp.abs(modes), keepdims=True))
        gain = CODE_MAX / peak
        for k in range(len(planes)):
            codes = jnp.round(mode_ref[:, pl.ds(k * half, half)] * gain).astype(jnp.int32).astype(jnp.int16)
            code_refs[group][:, k] = codes.reshape(z_devs, 8, half)
        last = group // 2
        scale_ref[last, pl.ds(group % 2, 1)] = jnp.broadcast_to(peak * (1.0 / CODE_MAX), (1, 128))

        @pl.loop(1, z_devs)
        def _(step):
            send(group, step).start()
            if group:
                send_scale(last, step).start()

        recv_refs[group][my_z] = code_refs[group][my_z]
        if group:
            rscale_ref[last, my_z] = scale_ref[last]

    def await_all(ref, sem):
        pltpu.make_async_copy(ref, ref, sem).wait()

    def await_codes(group):
        await_all(recv_refs[group].at[pl.ds(0, z_devs - 1)], recv_sem.at[group])

    def await_scale(last):
        await_all(rscale_ref.at[last, pl.ds(0, z_devs - 1), pl.ds(0, 2 - last)], srecv_sem.at[last])

    def decode(group, planes):
        codes = recv_refs[group][:, planes].astype(jnp.int32).astype(F32)
        return codes * rscale_ref[group // 2, :, pl.ds(group % 2, 1), :].reshape(z_devs, 1, 1, half)

    def fold(part, planes):
        rows = z_devs * 16
        flat = planes.reshape(rows, half)
        deq_ref[part, pl.ds(16, rows - 16), :] += flat[:rows - 16]
        deq_ref[part, pl.ds(0, 16), :] += flat[rows - 16:]

    def transform_z(part):
        flat = deq_ref.at[part]
        columns = [flat[pl.ds(ky, grid_n, stride=4), :] for ky in range(4)]
        zed = dot3((tz_ref[part, 0], tz_ref[part, 1]), split_bf16(jnp.concatenate(columns, axis=1)))
        if part == 0:
            zed_ref[...] = zed
        else:
            zed_ref[...] += zed

    for acc_ref in acc_refs:
        acc_ref[...] = jnp.zeros_like(acc_ref)
    for load in slot_loads(0):
        load.wait()
    for group in range(n_groups):
        @pl.loop(0, slots // CHUNK)
        def _(i):
            if group == 0:
                @pl.when(i == EARLY // CHUNK)
                def _():
                    for load in slot_loads(1):
                        load.wait()

            spread(group, i * CHUNK)
            if group:
                @pl.when(i == STEP_AT[group])
                def _():
                    transform_send(group - 1)

        if group == 0:
            pl.semaphore_wait(barrier, z_devs)
            for load in loads:
                load.wait()
        swap(group).start()
    transform_send(n_groups - 1)

    rows = z_devs * 16
    await_codes(0)
    await_scale(0)
    for part in range(2):
        deq_ref[part] = decode(0, slice(2 * part, 2 * part + 2)).reshape(rows, half)
    await_codes(1)
    fold(0, decode(1, slice(0, 2)))
    transform_z(0)
    await_codes(2)
    await_scale(1)
    late = decode(2, slice(0, 1))
    fold(1, jnp.concatenate([late, jnp.zeros_like(late)], axis=1))
    transform_z(1)

    row = jnp.zeros((8, grid_n), F32)
    for ky in range(4):
        cols = pl.ds(ky * half, half)
        real, imag = zed_ref[pl.ds(0, grid_n), cols], zed_ref[pl.ds(grid_n, grid_n), cols]
        value = 0.5 * bc_ref[:, ky, :] * (real * real + imag * imag).T
        ek_ref[:, ky, :] = value
        row += jnp.sum(value.reshape(half // 8, 8, grid_n), axis=0)
    store = pltpu.make_async_copy(ek_ref, ek_hbm, load_sem.at[0])
    store.start()
    row_ref[0] = jnp.broadcast_to(jnp.sum(row[:, :half] + row[:, half:], axis=0, keepdims=True), (8, half))

    def pair_copy():
        return pltpu.make_async_remote_copy(src_ref=row_ref.at[0], dst_ref=row_ref.at[1], send_sem=row_sem.at[0], recv_sem=row_sem.at[1], device_id=partner, device_id_type=MESH)

    def row_copy(step):
        return pltpu.make_async_remote_copy(src_ref=row_ref.at[2, pl.ds(0, 1)], dst_ref=rrow_ref.at[my_z, pl.ds(0, 1)], send_sem=row_sem.at[2], recv_sem=row_sem.at[3], device_id={'zdom': chip(step)}, device_id_type=MESH)

    pair_copy().start()
    pair_copy().wait()
    row_ref[2] = row_ref[0] + row_ref[1]

    @pl.loop(1, z_devs)
    def _(step):
        row_copy(step).start()

    rrow_ref[my_z, pl.ds(0, 1)] = row_ref[2, pl.ds(0, 1)]
    others = rrow_ref.at[pl.ds(0, z_devs - 1), pl.ds(0, 1)]
    pltpu.make_async_copy(others, others, row_sem.at[3]).wait()
    sum_ref[0] = jnp.sum(rrow_ref[:, pl.ds(0, 1), :]) * (1.0 / (grid_n * grid_n * grid_n))
    await_all(others, row_sem.at[2])
    for group in range(n_groups):
        await_all(code_refs[group].at[pl.ds(0, z_devs - 1)], send_sem.at[group])
    for last in range(2):
        await_all(rscale_ref.at[last, pl.ds(0, z_devs - 1), pl.ds(0, 2 - last)], ssend_sem.at[last])
    store.wait()


def solution(mesh):
    y_devs = mesh.shape['ydom']
    z_devs = mesh.shape['zdom']
    slot_spec = P(('sys', 'ydom', 'zdom'))
    mode_spec = P(('sys', 'ydom'), 'zdom', None)

    def local_energy(charge, real_mask, grid_idx, spline_w, influence):
        grid_n = influence.shape[2]
        slots = charge.shape[0]
        half = grid_n // 2
        n_groups = len(GROUPS)
        table_x, table_y, table_z = dft_tables(grid_n, y_devs, z_devs)
        any_spec = pl.BlockSpec(memory_space=pl.ANY)
        rows = [len(GROUPS[g]) * (grid_n // y_devs) + ghost_rows(g) for g in range(n_groups)]
        codes = [pltpu.VMEM((z_devs, len(planes), 8, half), jnp.int16) for planes in GROUPS]
        mode_energy, energy = pl.pallas_call(
            functools.partial(energy_kernel, y_devs, z_devs),
            in_specs=[any_spec] * 8,
            out_specs=[any_spec, pl.BlockSpec(memory_space=pltpu.SMEM)],
            out_shape=[jax.ShapeDtypeStruct(influence.shape, F32), jax.ShapeDtypeStruct((1,), F32)],
            scratch_shapes=[
                pltpu.VMEM((1, slots), F32), pltpu.VMEM((1, slots), jnp.int32), pltpu.VMEM((3, slots), jnp.int32), pltpu.VMEM((3, 4, slots), F32),
                pltpu.VMEM((grid_n // y_devs + 16, slots), F32),
                pltpu.VMEM((slots, grid_n), BF16), pltpu.VMEM((slots, grid_n), BF16),
                pltpu.VMEM((2, rows[0], SUB), BF16), pltpu.VMEM((2, rows[0], SUB), BF16),
                [pltpu.VMEM((r, grid_n), F32) for r in rows], [pltpu.VMEM((r, grid_n), F32) for r in rows],
                pltpu.VMEM((2 * grid_n, grid_n), F32), pltpu.VMEM((2 * grid_n, grid_n), F32), pltpu.VMEM((2 * grid_n, 4 * half), F32),
                codes, codes,
                pltpu.VMEM((2, 2, 128), F32), pltpu.VMEM((2, z_devs, 2, 128), F32),
                pltpu.VMEM((2, z_devs * 16, half), F32), pltpu.VMEM((2 * grid_n, 4 * half), F32),
                pltpu.VMEM(influence.shape, F32), pltpu.VMEM(influence.shape, F32),
                pltpu.VMEM(table_x.shape[1:], BF16), pltpu.VMEM(table_y.shape, BF16), pltpu.VMEM(table_z.shape, BF16),
                pltpu.VMEM((3, 8, 128), F32), pltpu.VMEM((z_devs, 8, 128), F32),
                pltpu.SemaphoreType.DMA((2, 4)), pltpu.SemaphoreType.DMA((4,)), pltpu.SemaphoreType.DMA((2, n_groups)),
                pltpu.SemaphoreType.DMA((n_groups,)), pltpu.SemaphoreType.DMA((n_groups,)),
                pltpu.SemaphoreType.DMA((2,)), pltpu.SemaphoreType.DMA((2,)),
                pltpu.SemaphoreType.DMA((4,)),
            ],
            compiler_params=pltpu.CompilerParams(collective_id=0, has_side_effects=True, vmem_limit_bytes=60 * 1024 * 1024),
            name="energy",
        )(charge.reshape(1, slots), real_mask.reshape(1, slots), grid_idx.T, jnp.transpose(spline_w, (1, 2, 0)), influence, jnp.asarray(table_x), jnp.asarray(table_y), jnp.asarray(table_z))
        return mode_energy, energy

    return jax.shard_map(local_energy, mesh=mesh, in_specs=(slot_spec, slot_spec, P(('sys', 'ydom', 'zdom'), None), P(('sys', 'ydom', 'zdom'), None, None), mode_spec), out_specs=(mode_spec, P('sys')), check_vma=False)
```

```python
import functools
import math
import jax
import jax.numpy as jnp
import numpy as np
from jax import lax
from jax.experimental import pallas as pl
from jax.experimental.pallas import tpu as pltpu
from jax.sharding import PartitionSpec as P

F32 = jnp.float32
BF16 = jnp.bfloat16
SUB = 256
CHUNK = 1024
GROUPS = ((0, 1, 2, 3), (4, 5), (6,))
STEP_AT = (0, 5, 7)
EARLY = 2048
CODE_MAX = 32767.0
MESH = pl.DeviceIdType.MESH


def split_bf16(value):
    high = value.astype(BF16)
    return high, (value - high.astype(F32)).astype(BF16)


def dot3(lhs, rhs, rhs_dim=0):
    def dot(a, b):
        return lax.dot_general(a, b, (((1,), (rhs_dim,)), ((), ())), preferred_element_type=F32)
    return dot(lhs[0], rhs[0]) + dot(lhs[1], rhs[0]) + dot(lhs[0], rhs[1])


def pick(ahead, taps, wrap=True):
    place = ahead & 15 if wrap else ahead
    value = jnp.zeros(ahead.shape, F32)
    for t in range(4):
        value = jnp.where(place == t, taps[t:t + 1], value)
    return value


def np_split(value):
    value = np.asarray(value, np.float32)
    high = value.astype(BF16)
    return np.stack([high, (value - high.astype(np.float32)).astype(BF16)])


def dft_tables(grid_n, y_devs, z_devs):
    turn = 2.0 * np.pi / grid_n
    len_y, len_z = grid_n // y_devs, grid_n // z_devs
    x = np.arange(grid_n)
    freq = np.arange(grid_n)
    phase_x = (np.outer(x, freq) % grid_n) * turn
    table_x = np.stack([np_split(np.concatenate([np.cos(phase_x[:, i * len_y:(i + 1) * len_y]), -np.sin(phase_x[:, i * len_y:(i + 1) * len_y])], axis=1)) for i in range(y_devs)])
    phase_y = (np.outer(freq, x) % grid_n) * turn
    real = np.concatenate([np.cos(phase_y), np.sin(phase_y)], axis=1)
    imag = np.concatenate([-np.sin(phase_y), np.cos(phase_y)], axis=1)
    rows = np.stack([real.reshape(z_devs, len_z, 2 * grid_n), imag.reshape(z_devs, len_z, 2 * grid_n)], axis=1)
    table_y = np_split(rows.reshape(2 * grid_n, 2 * grid_n))
    table_z = []
    for first in (0, 2):
        pos = np.arange(z_devs)[:, None] * len_z + first + np.arange(2)[None, :]
        phase_z = ((freq[:, None, None] * pos[None]) % grid_n) * turn
        real = np.stack([np.cos(phase_z), np.sin(phase_z)], axis=3).reshape(grid_n, -1)
        imag = np.stack([-np.sin(phase_z), np.cos(phase_z)], axis=3).reshape(grid_n, -1)
        table_z.append(np_split(np.concatenate([real, imag], axis=0)))
    return table_x, table_y, np.stack(table_z)


def ghost_rows(group):
    return -(-8 * len(GROUPS[group]) // 16) * 16


def energy_kernel(y_devs, z_devs, q_hbm, m_hbm, idx_hbm, w_hbm, bc_hbm, tx_hbm, ty_hbm, tz_hbm, ek_hbm, sum_ref,
                  q_ref, m_ref, idx_ref, w_ref, near_ref, xh_ref, xl_ref, ph_ref, pl_ref, acc_refs, got_refs, grid_ref, mid_ref, mode_ref,
                  code_refs, recv_refs, scale_ref, rscale_ref,
                  deq_ref, zed_ref, bc_ref, ek_ref, tx_ref, ty_ref, tz_ref, row_ref, rrow_ref,
                  early_sem, load_sem, swap_sem, send_sem, recv_sem, ssend_sem, srecv_sem, row_sem):
    my_y = lax.axis_index('ydom')
    my_z = lax.axis_index('zdom')
    grid_n = xh_ref.shape[1]
    slots = q_ref.shape[1]
    len_y = grid_n // y_devs
    half = grid_n // 2
    n_groups = len(GROUPS)
    barrier = pltpu.get_barrier_semaphore()
    partner = {'ydom': 1 - my_y}

    def chip(step):
        return (my_z + step) & (z_devs - 1)

    def slot_loads(piece):
        cols = pl.ds(0, EARLY) if piece == 0 else pl.ds(EARLY, slots - EARLY)
        return [pltpu.make_async_copy(hbm.at[lead + (cols,)], ref.at[lead + (cols,)], early_sem.at[piece, k])
                for k, (hbm, ref, lead) in enumerate(((q_hbm, q_ref, (slice(None),)), (m_hbm, m_ref, (slice(None),)), (idx_hbm, idx_ref, (slice(None),)), (w_hbm, w_ref, (slice(None), slice(None)))))]

    for piece in range(2):
        for load in slot_loads(piece):
            load.start()

    @pl.loop(1, z_devs)
    def _(step):
        pl.semaphore_signal(barrier, inc=1, device_id={'zdom': chip(step)}, device_id_type=MESH)

    pl.semaphore_signal(barrier, inc=1, device_id=partner, device_id_type=MESH)

    loads = [pltpu.make_async_copy(tx_hbm.at[my_y], tx_ref, load_sem.at[0]), pltpu.make_async_copy(ty_hbm, ty_ref, load_sem.at[1]),
             pltpu.make_async_copy(tz_hbm, tz_ref, load_sem.at[2]), pltpu.make_async_copy(bc_hbm, bc_ref, load_sem.at[3])]
    for load in loads:
        load.start()

    def swap(group):
        return pltpu.make_async_remote_copy(src_ref=acc_refs[group], dst_ref=got_refs[group], send_sem=swap_sem.at[0, group], recv_sem=swap_sem.at[1, group], device_id=partner, device_id_type=MESH)

    def send(group, step):
        other = chip(step)
        return pltpu.make_async_remote_copy(src_ref=code_refs[group].at[other], dst_ref=recv_refs[group].at[my_z], send_sem=send_sem.at[group], recv_sem=recv_sem.at[group], device_id={'zdom': other}, device_id_type=MESH)

    def send_scale(last, step):
        return pltpu.make_async_remote_copy(src_ref=scale_ref.at[last, pl.ds(0, 2 - last)], dst_ref=rscale_ref.at[last, my_z, pl.ds(0, 2 - last)], send_sem=ssend_sem.at[last], recv_sem=srecv_sem.at[last], device_id={'zdom': chip(step)}, device_id_type=MESH)

    def spread(group, base):
        planes = GROUPS[group]
        zero_16 = jnp.zeros((16, SUB), BF16)
        total = None
        for sub in range(CHUNK // SUB):
            slot = sub % 2
            cols = pl.ds(pl.multiple_of(base + sub * SUB, SUB), SUB)
            row_16 = lax.broadcasted_iota(jnp.int32, (16, SUB), 0)
            if group == 0:
                weight = q_ref[:, cols] * m_ref[:, cols].astype(F32)
                ahead = row_16 - idx_ref[0:1, cols]
                taps = w_ref[0, :, cols] * weight
                high, low = split_bf16(pick(ahead, taps))
                tile_x = (-(ahead >> 4) & 15).astype(F32).astype(BF16)
                for r in range(grid_n // 16):
                    hit = tile_x == r
                    near_ref[slot, 0, 16 * r:16 * r + 16, :] = jnp.where(hit, high, zero_16)
                    near_ref[slot, 1, 16 * r:16 * r + 16, :] = jnp.where(hit, low, zero_16)
                xh_ref[cols, :] = near_ref[slot, 0].T
                xl_ref[cols, :] = near_ref[slot, 1].T
            ahead = row_16 - idx_ref[1:2, cols]
            line_y = pick(ahead, w_ref[1, :, cols])
            tile = -(ahead >> 4)
            ghost_y = jnp.where(tile[:8] == len_y // 16, line_y[:8], 0.0)
            tile_y = tile.astype(F32).astype(BF16)
            line_z = pick(row_16[:8] - idx_ref[2:3, cols], w_ref[2, :, cols], False)
            sides = [split_bf16(line_y * line_z[z:z + 1]) for z in planes]
            for r in range(len_y // 16):
                hit = tile_y == r
                for k, side in enumerate(sides):
                    first = k * len_y + 16 * r
                    ph_ref[slot, first:first + 16, :] = jnp.where(hit, side[0], zero_16)
                    pl_ref[slot, first:first + 16, :] = jnp.where(hit, side[1], zero_16)
            ghosts = [ghost_y * line_z[z:z + 1] for z in planes]
            if len(planes) % 2:
                ghosts.append(jnp.zeros((8, SUB), F32))
            high, low = split_bf16(jnp.concatenate(ghosts, axis=0))
            top = len(planes) * len_y
            rows = pl.ds(0, top + ghost_rows(group))
            ph_ref[slot, top:top + ghost_rows(group), :] = high
            pl_ref[slot, top:top + ghost_rows(group), :] = low
            if group == 0:
                part = dot3((ph_ref[slot, rows, :], pl_ref[slot, rows, :]), (near_ref[slot, 0], near_ref[slot, 1]), 1)
            else:
                part = dot3((ph_ref[slot, rows, :], pl_ref[slot, rows, :]), (xh_ref[cols, :], xl_ref[cols, :]))
            total = part if total is None else total + part
        acc_refs[group][...] += total

    def transform_send(group):
        planes = GROUPS[group]
        acc_ref, got_ref = acc_refs[group], got_refs[group]
        swap(group).wait()
        mine, theirs = my_y * len_y, (1 - my_y) * len_y
        peak = jnp.full((1, 1), 1e-30, F32)
        for first in range(0, len(planes), 2):
            count = min(2, len(planes) - first)
            for k in range(count):
                block = pl.ds((first + k) * len_y, len_y)
                grid_ref[pl.ds(pl.multiple_of(k * grid_n + mine, len_y), len_y), :] = acc_ref[block, :]
                grid_ref[pl.ds(pl.multiple_of(k * grid_n + theirs, len_y), len_y), :] = got_ref[block, :]
            for k in range(count):
                ghost = pl.ds(len(planes) * len_y + 8 * (first + k), 8)
                grid_ref[pl.ds(pl.multiple_of(k * grid_n + theirs, len_y), 8), :] += acc_ref[ghost, :]
                grid_ref[pl.ds(pl.multiple_of(k * grid_n + mine, len_y), 8), :] += got_ref[ghost, :]
            size = count * grid_n
            mid_ref[pl.ds(0, size), :] = dot3(split_bf16(grid_ref[pl.ds(0, size), :]), (tx_ref[0], tx_ref[1]))
            columns = [jnp.concatenate([mid_ref[pl.ds(k * grid_n, grid_n), pl.ds(c * half, half)] for c in range(2)], axis=0) for k in range(count)]
            modes = dot3((ty_ref[0], ty_ref[1]), split_bf16(jnp.concatenate(columns, axis=1)))
            mode_ref[:, pl.ds(first * half, count * half)] = modes
            peak = jnp.maximum(peak, jnp.max(jnp.abs(modes), keepdims=True))
        gain = CODE_MAX / peak
        for k in range(len(planes)):
            codes = jnp.round(mode_ref[:, pl.ds(k * half, half)] * gain).astype(jnp.int32).astype(jnp.int16)
            code_refs[group][:, k] = codes.reshape(z_devs, 8, half)
        last = group // 2
        scale_ref[last, pl.ds(group % 2, 1)] = jnp.broadcast_to(peak * (1.0 / CODE_MAX), (1, 128))

        @pl.loop(1, z_devs)
        def _(step):
            send(group, step).start()
            if group:
                send_scale(last, step).start()

        recv_refs[group][my_z] = code_refs[group][my_z]
        if group:
            rscale_ref[last, my_z] = scale_ref[last]

    def await_all(ref, sem):
        pltpu.make_async_copy(ref, ref, sem).wait()

    def await_codes(group):
        await_all(recv_refs[group].at[pl.ds(0, z_devs - 1)], recv_sem.at[group])

    def await_scale(last):
        await_all(rscale_ref.at[last, pl.ds(0, z_devs - 1), pl.ds(0, 2 - last)], srecv_sem.at[last])

    def decode(group, planes):
        codes = recv_refs[group][:, planes].astype(jnp.int32).astype(F32)
        return codes * rscale_ref[group // 2, :, pl.ds(group % 2, 1), :].reshape(z_devs, 1, 1, half)

    def fold(part, planes):
        rows = z_devs * 16
        flat = planes.reshape(rows, half)
        deq_ref[part, pl.ds(16, rows - 16), :] += flat[:rows - 16]
        deq_ref[part, pl.ds(0, 16), :] += flat[rows - 16:]

    def transform_z(part):
        flat = deq_ref.at[part]
        columns = [flat[pl.ds(ky, grid_n, stride=4), :] for ky in range(4)]
        zed = dot3((tz_ref[part, 0], tz_ref[part, 1]), split_bf16(jnp.concatenate(columns, axis=1)))
        if part == 0:
            zed_ref[...] = zed
        else:
            zed_ref[...] += zed

    for acc_ref in acc_refs:
        acc_ref[...] = jnp.zeros_like(acc_ref)
    for load in slot_loads(0):
        load.wait()
    for group in range(n_groups):
        @pl.loop(0, slots // CHUNK)
        def _(i):
            if group == 0:
                @pl.when(i == EARLY // CHUNK)
                def _():
                    for load in slot_loads(1):
                        load.wait()

            spread(group, i * CHUNK)
            if group:
                @pl.when(i == STEP_AT[group])
                def _():
                    transform_send(group - 1)

        if group == 0:
            pl.semaphore_wait(barrier, z_devs)
            for load in loads:
                load.wait()
        swap(group).start()
    transform_send(n_groups - 1)

    rows = z_devs * 16
    await_codes(0)
    await_scale(0)
    for part in range(2):
        deq_ref[part] = decode(0, slice(2 * part, 2 * part + 2)).reshape(rows, half)
    await_codes(1)
    fold(0, decode(1, slice(0, 2)))
    transform_z(0)
    await_codes(2)
    await_scale(1)
    late = decode(2, slice(0, 1))
    fold(1, jnp.concatenate([late, jnp.zeros_like(late)], axis=1))
    transform_z(1)

    row = jnp.zeros((8, grid_n), F32)
    for ky in range(4):
        cols = pl.ds(ky * half, half)
        real, imag = zed_ref[pl.ds(0, grid_n), cols], zed_ref[pl.ds(grid_n, grid_n), cols]
        value = 0.5 * bc_ref[:, ky, :] * (real * real + imag * imag).T
        ek_ref[:, ky, :] = value
        row += jnp.sum(value.reshape(half // 8, 8, grid_n), axis=0)
    store = pltpu.make_async_copy(ek_ref, ek_hbm, load_sem.at[0])
    store.start()
    row_ref[0] = jnp.broadcast_to(jnp.sum(row[:, :half] + row[:, half:], axis=0, keepdims=True), (8, half))

    def pair_copy():
        return pltpu.make_async_remote_copy(src_ref=row_ref.at[0], dst_ref=row_ref.at[1], send_sem=row_sem.at[0], recv_sem=row_sem.at[1], device_id=partner, device_id_type=MESH)

    def row_copy(step):
        return pltpu.make_async_remote_copy(src_ref=row_ref.at[2, pl.ds(0, 1)], dst_ref=rrow_ref.at[my_z, pl.ds(0, 1)], send_sem=row_sem.at[2], recv_sem=row_sem.at[3], device_id={'zdom': chip(step)}, device_id_type=MESH)

    pair_copy().start()
    pair_copy().wait()
    row_ref[2] = row_ref[0] + row_ref[1]

    @pl.loop(1, z_devs)
    def _(step):
        row_copy(step).start()

    rrow_ref[my_z, pl.ds(0, 1)] = row_ref[2, pl.ds(0, 1)]
    others = rrow_ref.at[pl.ds(0, z_devs - 1), pl.ds(0, 1)]
    pltpu.make_async_copy(others, others, row_sem.at[3]).wait()
    sum_ref[0] = jnp.sum(rrow_ref[:, pl.ds(0, 1), :]) * (1.0 / (grid_n * grid_n * grid_n))
    await_all(others, row_sem.at[2])
    for group in range(n_groups):
        await_all(code_refs[group].at[pl.ds(0, z_devs - 1)], send_sem.at[group])
    for last in range(2):
        await_all(rscale_ref.at[last, pl.ds(0, z_devs - 1), pl.ds(0, 2 - last)], ssend_sem.at[last])
    store.wait()


def solution(mesh):
    y_devs = mesh.shape['ydom']
    z_devs = mesh.shape['zdom']
    slot_spec = P(('sys', 'ydom', 'zdom'))
    mode_spec = P(('sys', 'ydom'), 'zdom', None)

    def local_energy(charge, real_mask, grid_idx, spline_w, influence):
        grid_n = influence.shape[2]
        slots = charge.shape[0]
        half = grid_n // 2
        n_groups = len(GROUPS)
        table_x, table_y, table_z = dft_tables(grid_n, y_devs, z_devs)
        any_spec = pl.BlockSpec(memory_space=pl.ANY)
        rows = [len(GROUPS[g]) * (grid_n // y_devs) + ghost_rows(g) for g in range(n_groups)]
        codes = [pltpu.VMEM((z_devs, len(planes), 8, half), jnp.int16) for planes in GROUPS]
        mode_energy, energy = pl.pallas_call(
            functools.partial(energy_kernel, y_devs, z_devs),
            in_specs=[any_spec] * 8,
            out_specs=[any_spec, pl.BlockSpec(memory_space=pltpu.SMEM)],
            out_shape=[jax.ShapeDtypeStruct(influence.shape, F32), jax.ShapeDtypeStruct((1,), F32)],
            scratch_shapes=[
                pltpu.VMEM((1, slots), F32), pltpu.VMEM((1, slots), jnp.int32), pltpu.VMEM((3, slots), jnp.int32), pltpu.VMEM((3, 4, slots), F32),
                pltpu.VMEM((2, 2, grid_n, SUB), BF16), pltpu.VMEM((slots, grid_n), BF16), pltpu.VMEM((slots, grid_n), BF16),
                pltpu.VMEM((2, rows[0], SUB), BF16), pltpu.VMEM((2, rows[0], SUB), BF16),
                [pltpu.VMEM((r, grid_n), F32) for r in rows], [pltpu.VMEM((r, grid_n), F32) for r in rows],
                pltpu.VMEM((2 * grid_n, grid_n), F32), pltpu.VMEM((2 * grid_n, grid_n), F32), pltpu.VMEM((2 * grid_n, 4 * half), F32),
                codes, codes,
                pltpu.VMEM((2, 2, 128), F32), pltpu.VMEM((2, z_devs, 2, 128), F32),
                pltpu.VMEM((2, z_devs * 16, half), F32), pltpu.VMEM((2 * grid_n, 4 * half), F32),
                pltpu.VMEM(influence.shape, F32), pltpu.VMEM(influence.shape, F32),
                pltpu.VMEM(table_x.shape[1:], BF16), pltpu.VMEM(table_y.shape, BF16), pltpu.VMEM(table_z.shape, BF16),
                pltpu.VMEM((3, 8, 128), F32), pltpu.VMEM((z_devs, 8, 128), F32),
                pltpu.SemaphoreType.DMA((2, 4)), pltpu.SemaphoreType.DMA((4,)), pltpu.SemaphoreType.DMA((2, n_groups)),
                pltpu.SemaphoreType.DMA((n_groups,)), pltpu.SemaphoreType.DMA((n_groups,)),
                pltpu.SemaphoreType.DMA((2,)), pltpu.SemaphoreType.DMA((2,)),
                pltpu.SemaphoreType.DMA((4,)),
            ],
            compiler_params=pltpu.CompilerParams(collective_id=0, has_side_effects=True, vmem_limit_bytes=60 * 1024 * 1024),
            name="energy",
        )(charge.reshape(1, slots), real_mask.reshape(1, slots), grid_idx.T, jnp.transpose(spline_w, (1, 2, 0)), influence, jnp.asarray(table_x), jnp.asarray(table_y), jnp.asarray(table_z))
        return mode_energy, energy

    return jax.shard_map(local_energy, mesh=mesh, in_specs=(slot_spec, slot_spec, P(('sys', 'ydom', 'zdom'), None), P(('sys', 'ydom', 'zdom'), None, None), mode_spec), out_specs=(mode_spec, P('sys')), check_vma=False)
```

```python
import functools
import math
import jax
import jax.numpy as jnp
import numpy as np
from jax import lax
from jax.experimental import pallas as pl
from jax.experimental.pallas import tpu as pltpu
from jax.sharding import PartitionSpec as P

F32 = jnp.float32
BF16 = jnp.bfloat16
SUB = 256
CHUNK = 1024
GROUPS = ((0, 1, 2, 3), (4, 5), (6,))
STEP_AT = (0, 5, 7)
EARLY = 2048
CODE_MAX = 32767.0
MESH = pl.DeviceIdType.MESH


def split_bf16(value):
    high = value.astype(BF16)
    return high, (value - high.astype(F32)).astype(BF16)


def dot3(lhs, rhs, rhs_dim=0):
    def dot(a, b):
        return lax.dot_general(a, b, (((1,), (rhs_dim,)), ((), ())), preferred_element_type=F32)
    return dot(lhs[0], rhs[0]) + dot(lhs[1], rhs[0]) + dot(lhs[0], rhs[1])


def pick(ahead, taps, wrap=True):
    place = ahead & 15 if wrap else ahead
    value = jnp.zeros(ahead.shape, F32)
    for t in range(4):
        value = jnp.where(place == t, taps[t:t + 1], value)
    return value


def np_split(value):
    value = np.asarray(value, np.float32)
    high = value.astype(BF16)
    return np.stack([high, (value - high.astype(np.float32)).astype(BF16)])


def dft_tables(grid_n, y_devs, z_devs):
    turn = 2.0 * np.pi / grid_n
    len_y, len_z = grid_n // y_devs, grid_n // z_devs
    x = np.arange(grid_n)
    freq = np.arange(grid_n)
    phase_x = (np.outer(x, freq) % grid_n) * turn
    table_x = np.stack([np_split(np.concatenate([np.cos(phase_x[:, i * len_y:(i + 1) * len_y]), -np.sin(phase_x[:, i * len_y:(i + 1) * len_y])], axis=1)) for i in range(y_devs)])
    phase_y = (np.outer(freq, x) % grid_n) * turn
    real = np.concatenate([np.cos(phase_y), np.sin(phase_y)], axis=1)
    imag = np.concatenate([-np.sin(phase_y), np.cos(phase_y)], axis=1)
    rows = np.stack([real.reshape(z_devs, len_z, 2 * grid_n), imag.reshape(z_devs, len_z, 2 * grid_n)], axis=1)
    table_y = np_split(rows.reshape(2 * grid_n, 2 * grid_n))
    table_z = []
    for first in (0, 2):
        pos = np.arange(z_devs)[:, None] * len_z + first + np.arange(2)[None, :]
        phase_z = ((freq[:, None, None] * pos[None]) % grid_n) * turn
        real = np.stack([np.cos(phase_z), np.sin(phase_z)], axis=3).reshape(grid_n, -1)
        imag = np.stack([-np.sin(phase_z), np.cos(phase_z)], axis=3).reshape(grid_n, -1)
        table_z.append(np_split(np.concatenate([real, imag], axis=0)))
    return table_x, table_y, np.stack(table_z)


def ghost_rows(group):
    return -(-8 * len(GROUPS[group]) // 16) * 16


def energy_kernel(y_devs, z_devs, q_hbm, m_hbm, idx_hbm, w_hbm, bc_hbm, tx_hbm, ty_hbm, tz_hbm, ek_hbm, sum_ref,
                  q_ref, m_ref, idx_ref, w_ref, near_ref, xh_ref, xl_ref, ph_ref, pl_ref, acc_refs, got_refs, grid_ref, mid_ref, mode_ref,
                  code_refs, recv_refs, scale_ref, rscale_ref,
                  deq_ref, zed_ref, bc_ref, ek_ref, tx_ref, ty_ref, tz_ref, row_ref, rrow_ref,
                  early_sem, load_sem, swap_sem, send_sem, recv_sem, ssend_sem, srecv_sem, row_sem):
    my_y = lax.axis_index('ydom')
    my_z = lax.axis_index('zdom')
    grid_n = xh_ref.shape[1]
    slots = q_ref.shape[1]
    len_y = grid_n // y_devs
    half = grid_n // 2
    n_groups = len(GROUPS)
    barrier = pltpu.get_barrier_semaphore()
    partner = {'ydom': 1 - my_y}

    def chip(step):
        return (my_z + step) & (z_devs - 1)

    def far_first(start):
        pl.loop(z_devs // 2, z_devs)(start)
        pl.loop(1, z_devs // 2)(start)

    def slot_loads(piece):
        cols = pl.ds(0, EARLY) if piece == 0 else pl.ds(EARLY, slots - EARLY)
        return [pltpu.make_async_copy(hbm.at[lead + (cols,)], ref.at[lead + (cols,)], early_sem.at[piece, k])
                for k, (hbm, ref, lead) in enumerate(((q_hbm, q_ref, (slice(None),)), (m_hbm, m_ref, (slice(None),)), (idx_hbm, idx_ref, (slice(None),)), (w_hbm, w_ref, (slice(None), slice(None)))))]

    for piece in range(2):
        for load in slot_loads(piece):
            load.start()

    @pl.loop(1, z_devs)
    def _(step):
        for core in range(y_devs):
            pl.semaphore_signal(barrier, inc=1, device_id={'zdom': chip(step), 'ydom': core}, device_id_type=MESH)

    pl.semaphore_signal(barrier, inc=1, device_id=partner, device_id_type=MESH)

    loads = [pltpu.make_async_copy(tx_hbm.at[my_y], tx_ref, load_sem.at[0]), pltpu.make_async_copy(ty_hbm, ty_ref, load_sem.at[1]),
             pltpu.make_async_copy(tz_hbm, tz_ref, load_sem.at[2]), pltpu.make_async_copy(bc_hbm, bc_ref, load_sem.at[3])]
    for load in loads:
        load.start()

    def swap(group):
        return pltpu.make_async_remote_copy(src_ref=acc_refs[group], dst_ref=got_refs[group], send_sem=swap_sem.at[0, group], recv_sem=swap_sem.at[1, group], device_id=partner, device_id_type=MESH)

    def send(group, step):
        other = chip(step)
        return pltpu.make_async_remote_copy(src_ref=code_refs[group].at[other], dst_ref=recv_refs[group].at[my_z], send_sem=send_sem.at[group], recv_sem=recv_sem.at[group], device_id={'zdom': other}, device_id_type=MESH)

    def send_scale(last, step):
        return pltpu.make_async_remote_copy(src_ref=scale_ref.at[last, pl.ds(0, 2 - last)], dst_ref=rscale_ref.at[last, my_z, pl.ds(0, 2 - last)], send_sem=ssend_sem.at[last], recv_sem=srecv_sem.at[last], device_id={'zdom': chip(step)}, device_id_type=MESH)

    def spread(group, base):
        planes = GROUPS[group]
        zero_16 = jnp.zeros((16, SUB), BF16)
        total = None
        for sub in range(CHUNK // SUB):
            slot = sub % 2
            cols = pl.ds(pl.multiple_of(base + sub * SUB, SUB), SUB)
            row_16 = lax.broadcasted_iota(jnp.int32, (16, SUB), 0)
            if group == 0:
                weight = q_ref[:, cols] * m_ref[:, cols].astype(F32)
                ahead = row_16 - idx_ref[0:1, cols]
                taps = w_ref[0, :, cols] * weight
                high, low = split_bf16(pick(ahead, taps))
                tile_x = (-(ahead >> 4) & 15).astype(F32).astype(BF16)
                for r in range(grid_n // 16):
                    hit = tile_x == r
                    near_ref[slot, 0, 16 * r:16 * r + 16, :] = jnp.where(hit, high, zero_16)
                    near_ref[slot, 1, 16 * r:16 * r + 16, :] = jnp.where(hit, low, zero_16)
                xh_ref[cols, :] = near_ref[slot, 0].T
                xl_ref[cols, :] = near_ref[slot, 1].T
            ahead = row_16 - idx_ref[1:2, cols]
            line_y = pick(ahead, w_ref[1, :, cols])
            tile = -(ahead >> 4)
            ghost_y = jnp.where(tile[:8] == len_y // 16, line_y[:8], 0.0)
            tile_y = tile.astype(F32).astype(BF16)
            line_z = pick(row_16[:8] - idx_ref[2:3, cols], w_ref[2, :, cols], False)
            sides = [split_bf16(line_y * line_z[z:z + 1]) for z in planes]
            for r in range(len_y // 16):
                hit = tile_y == r
                for k, side in enumerate(sides):
                    first = k * len_y + 16 * r
                    ph_ref[slot, first:first + 16, :] = jnp.where(hit, side[0], zero_16)
                    pl_ref[slot, first:first + 16, :] = jnp.where(hit, side[1], zero_16)
            ghosts = [ghost_y * line_z[z:z + 1] for z in planes]
            if len(planes) % 2:
                ghosts.append(jnp.zeros((8, SUB), F32))
            high, low = split_bf16(jnp.concatenate(ghosts, axis=0))
            top = len(planes) * len_y
            rows = pl.ds(0, top + ghost_rows(group))
            ph_ref[slot, top:top + ghost_rows(group), :] = high
            pl_ref[slot, top:top + ghost_rows(group), :] = low
            if group == 0:
                part = dot3((ph_ref[slot, rows, :], pl_ref[slot, rows, :]), (near_ref[slot, 0], near_ref[slot, 1]), 1)
            else:
                part = dot3((ph_ref[slot, rows, :], pl_ref[slot, rows, :]), (xh_ref[cols, :], xl_ref[cols, :]))
            total = part if total is None else total + part
        acc_refs[group][...] += total

    def transform_send(group):
        planes = GROUPS[group]
        acc_ref, got_ref = acc_refs[group], got_refs[group]
        swap(group).wait()
        mine, theirs = my_y * len_y, (1 - my_y) * len_y
        peak = jnp.full((1, 1), 1e-30, F32)
        for first in range(0, len(planes), 2):
            count = min(2, len(planes) - first)
            for k in range(count):
                block = pl.ds((first + k) * len_y, len_y)
                grid_ref[pl.ds(pl.multiple_of(k * grid_n + mine, len_y), len_y), :] = acc_ref[block, :]
                grid_ref[pl.ds(pl.multiple_of(k * grid_n + theirs, len_y), len_y), :] = got_ref[block, :]
            for k in range(count):
                ghost = pl.ds(len(planes) * len_y + 8 * (first + k), 8)
                grid_ref[pl.ds(pl.multiple_of(k * grid_n + theirs, len_y), 8), :] += acc_ref[ghost, :]
                grid_ref[pl.ds(pl.multiple_of(k * grid_n + mine, len_y), 8), :] += got_ref[ghost, :]
            size = count * grid_n
            mid_ref[pl.ds(0, size), :] = dot3(split_bf16(grid_ref[pl.ds(0, size), :]), (tx_ref[0], tx_ref[1]))
            columns = [jnp.concatenate([mid_ref[pl.ds(k * grid_n, grid_n), pl.ds(c * half, half)] for c in range(2)], axis=0) for k in range(count)]
            modes = dot3((ty_ref[0], ty_ref[1]), split_bf16(jnp.concatenate(columns, axis=1)))
            mode_ref[:, pl.ds(first * half, count * half)] = modes
            peak = jnp.maximum(peak, jnp.max(jnp.abs(modes), keepdims=True))
        gain = CODE_MAX / peak
        for k in range(len(planes)):
            codes = jnp.round(mode_ref[:, pl.ds(k * half, half)] * gain).astype(jnp.int32).astype(jnp.int16)
            code_refs[group][:, k] = codes.reshape(z_devs, 8, half)
        last = group // 2
        scale_ref[last, pl.ds(group % 2, 1)] = jnp.broadcast_to(peak * (1.0 / CODE_MAX), (1, 128))

        def start(step):
            send(group, step).start()
            if group:
                send_scale(last, step).start()

        far_first(start)

        recv_refs[group][my_z] = code_refs[group][my_z]
        if group:
            rscale_ref[last, my_z] = scale_ref[last]

    def await_all(ref, sem):
        pltpu.make_async_copy(ref, ref, sem).wait()

    def await_codes(group):
        await_all(recv_refs[group].at[pl.ds(0, z_devs - 1)], recv_sem.at[group])

    def await_scale(last):
        await_all(rscale_ref.at[last, pl.ds(0, z_devs - 1), pl.ds(0, 2 - last)], srecv_sem.at[last])

    def decode(group, planes):
        codes = recv_refs[group][:, planes].astype(jnp.int32).astype(F32)
        return codes * rscale_ref[group // 2, :, pl.ds(group % 2, 1), :].reshape(z_devs, 1, 1, half)

    def fold(part, planes):
        rows = z_devs * 16
        flat = planes.reshape(rows, half)
        deq_ref[part, pl.ds(16, rows - 16), :] += flat[:rows - 16]
        deq_ref[part, pl.ds(0, 16), :] += flat[rows - 16:]

    def transform_z(part):
        flat = deq_ref.at[part]
        columns = [flat[pl.ds(ky, grid_n, stride=4), :] for ky in range(4)]
        zed = dot3((tz_ref[part, 0], tz_ref[part, 1]), split_bf16(jnp.concatenate(columns, axis=1)))
        if part == 0:
            zed_ref[...] = zed
        else:
            zed_ref[...] += zed

    for acc_ref in acc_refs:
        acc_ref[...] = jnp.zeros_like(acc_ref)
    for load in slot_loads(0):
        load.wait()
    for group in range(n_groups):
        @pl.loop(0, slots // CHUNK)
        def _(i):
            if group == 0:
                @pl.when(i == EARLY // CHUNK)
                def _():
                    for load in slot_loads(1):
                        load.wait()

            spread(group, i * CHUNK)
            if group:
                @pl.when(i == STEP_AT[group])
                def _():
                    transform_send(group - 1)

        if group == 0:
            pl.semaphore_wait(barrier, y_devs * z_devs - 1)
            for load in loads:
                load.wait()
        swap(group).start()
    transform_send(n_groups - 1)

    rows = z_devs * 16
    await_codes(0)
    await_scale(0)
    for part in range(2):
        deq_ref[part] = decode(0, slice(2 * part, 2 * part + 2)).reshape(rows, half)
    await_codes(1)
    fold(0, decode(1, slice(0, 2)))
    transform_z(0)
    await_codes(2)
    await_scale(1)
    late = decode(2, slice(0, 1))
    fold(1, jnp.concatenate([late, jnp.zeros_like(late)], axis=1))
    transform_z(1)

    row = jnp.zeros((8, half), F32)
    for ky in range(4):
        cols = pl.ds(ky * half, half)
        real, imag = zed_ref[pl.ds(0, grid_n), cols], zed_ref[pl.ds(grid_n, grid_n), cols]
        power = real * real + imag * imag
        for part in range(2):
            place = pl.ds(4 * part + ky, half, stride=8)
            value = bc_ref[place, :] * power[part * half:(part + 1) * half].T
            ek_ref[place, :] = value
            row += jnp.sum(value.reshape(half // 8, 8, half), axis=0)
    store = pltpu.make_async_copy(ek_ref, ek_hbm, load_sem.at[0])
    store.start()
    row_ref[...] = jnp.broadcast_to(jnp.sum(row, axis=0, keepdims=True), (8, half))

    me = my_z * y_devs + my_y
    others = rrow_ref.at[pl.ds(0, y_devs * z_devs - 1), pl.ds(0, 1)]

    def row_copy(device):
        return pltpu.make_async_remote_copy(src_ref=row_ref.at[pl.ds(0, 1)], dst_ref=rrow_ref.at[me, pl.ds(0, 1)], send_sem=row_sem.at[0], recv_sem=row_sem.at[1], device_id=device, device_id_type=MESH)

    def start(step):
        for core in range(y_devs):
            row_copy({'zdom': chip(step), 'ydom': core}).start()

    far_first(start)
    row_copy(partner).start()
    rrow_ref[me, pl.ds(0, 1)] = row_ref[pl.ds(0, 1)]
    await_all(others, row_sem.at[1])
    sum_ref[0] = jnp.sum(rrow_ref[:, pl.ds(0, 1), :]) * (0.5 / (grid_n * grid_n * grid_n))
    await_all(others, row_sem.at[0])
    for group in range(n_groups):
        await_all(code_refs[group].at[pl.ds(0, z_devs - 1)], send_sem.at[group])
    for last in range(2):
        await_all(rscale_ref.at[last, pl.ds(0, z_devs - 1), pl.ds(0, 2 - last)], ssend_sem.at[last])
    store.wait()


def solution(mesh):
    y_devs = mesh.shape['ydom']
    z_devs = mesh.shape['zdom']
    slot_spec = P(('sys', 'ydom', 'zdom'))
    mode_spec = P(('sys', 'ydom'), 'zdom', None)

    def local_energy(charge, real_mask, grid_idx, spline_w, influence):
        grid_n = influence.shape[2]
        slots = charge.shape[0]
        half = grid_n // 2
        n_groups = len(GROUPS)
        table_x, table_y, table_z = dft_tables(grid_n, y_devs, z_devs)
        any_spec = pl.BlockSpec(memory_space=pl.ANY)
        rows = [len(GROUPS[g]) * (grid_n // y_devs) + ghost_rows(g) for g in range(n_groups)]
        codes = [pltpu.VMEM((z_devs, len(planes), 8, half), jnp.int16) for planes in GROUPS]
        tiles = jnp.swapaxes(influence.reshape(half, 4, 2, half), 1, 2).reshape(8 * half, half)
        mode_energy, energy = pl.pallas_call(
            functools.partial(energy_kernel, y_devs, z_devs),
            in_specs=[any_spec] * 8,
            out_specs=[any_spec, pl.BlockSpec(memory_space=pltpu.SMEM)],
            out_shape=[jax.ShapeDtypeStruct((8 * half, half), F32), jax.ShapeDtypeStruct((1,), F32)],
            scratch_shapes=[
                pltpu.VMEM((1, slots), F32), pltpu.VMEM((1, slots), jnp.int32), pltpu.VMEM((3, slots), jnp.int32), pltpu.VMEM((3, 4, slots), F32),
                pltpu.VMEM((2, 2, grid_n, SUB), BF16), pltpu.VMEM((slots, grid_n), BF16), pltpu.VMEM((slots, grid_n), BF16),
                pltpu.VMEM((2, rows[0], SUB), BF16), pltpu.VMEM((2, rows[0], SUB), BF16),
                [pltpu.VMEM((r, grid_n), F32) for r in rows], [pltpu.VMEM((r, grid_n), F32) for r in rows],
                pltpu.VMEM((2 * grid_n, grid_n), F32), pltpu.VMEM((2 * grid_n, grid_n), F32), pltpu.VMEM((2 * grid_n, 4 * half), F32),
                codes, codes,
                pltpu.VMEM((2, 2, 128), F32), pltpu.VMEM((2, z_devs, 2, 128), F32),
                pltpu.VMEM((2, z_devs * 16, half), F32), pltpu.VMEM((2 * grid_n, 4 * half), F32),
                pltpu.VMEM((8 * half, half), F32), pltpu.VMEM((8 * half, half), F32),
                pltpu.VMEM(table_x.shape[1:], BF16), pltpu.VMEM(table_y.shape, BF16), pltpu.VMEM(table_z.shape, BF16),
                pltpu.VMEM((8, 128), F32), pltpu.VMEM((y_devs * z_devs, 8, 128), F32),
                pltpu.SemaphoreType.DMA((2, 4)), pltpu.SemaphoreType.DMA((4,)), pltpu.SemaphoreType.DMA((2, n_groups)),
                pltpu.SemaphoreType.DMA((n_groups,)), pltpu.SemaphoreType.DMA((n_groups,)),
                pltpu.SemaphoreType.DMA((2,)), pltpu.SemaphoreType.DMA((2,)),
                pltpu.SemaphoreType.DMA((2,)),
            ],
            compiler_params=pltpu.CompilerParams(collective_id=0, has_side_effects=True, vmem_limit_bytes=60 * 1024 * 1024),
            name="energy",
        )(charge.reshape(1, slots), real_mask.reshape(1, slots), grid_idx.T, jnp.transpose(spline_w, (1, 2, 0)), tiles, jnp.asarray(table_x), jnp.asarray(table_y), jnp.asarray(table_z))
        mode_energy = lax.optimization_barrier(0.5 * mode_energy)
        return jnp.swapaxes(mode_energy.reshape(half, 2, 4, half), 1, 2).reshape(influence.shape), energy

    return jax.shard_map(local_energy, mesh=mesh, in_specs=(slot_spec, slot_spec, P(('sys', 'ydom', 'zdom'), None), P(('sys', 'ydom', 'zdom'), None, None), mode_spec), out_specs=(mode_spec, P('sys')), check_vma=False)
```

```python
import functools
import math
import jax
import jax.numpy as jnp
import numpy as np
from jax import lax
from jax.experimental import pallas as pl
from jax.experimental.pallas import tpu as pltpu
from jax.sharding import PartitionSpec as P

F32 = jnp.float32
BF16 = jnp.bfloat16
SUB = 256
CHUNK = 2048
GROUPS = ((0, 1, 2, 3), (4, 5), (6,))
STEP_AT = (0, 2, 3)
EARLY = 2048
CODE_MAX = 32767.0
MESH = pl.DeviceIdType.MESH


def split_bf16(value):
    high = value.astype(BF16)
    return high, (value - high.astype(F32)).astype(BF16)


def dot3(lhs, rhs, rhs_dim=0):
    def dot(a, b):
        return lax.dot_general(a, b, (((1,), (rhs_dim,)), ((), ())), preferred_element_type=F32)
    return dot(lhs[0], rhs[0]) + dot(lhs[1], rhs[0]) + dot(lhs[0], rhs[1])


def pick(ahead, taps, wrap=True):
    place = ahead & 15 if wrap else ahead
    value = jnp.zeros(ahead.shape, F32)
    for t in range(4):
        value = jnp.where(place == t, taps[t:t + 1], value)
    return value


def np_split(value):
    value = np.asarray(value, np.float32)
    high = value.astype(BF16)
    return np.stack([high, (value - high.astype(np.float32)).astype(BF16)])


def dft_tables(grid_n, y_devs, z_devs):
    turn = 2.0 * np.pi / grid_n
    len_y, len_z = grid_n // y_devs, grid_n // z_devs
    x = np.arange(grid_n)
    freq = np.arange(grid_n)
    phase_x = (np.outer(x, freq) % grid_n) * turn
    table_x = np.stack([np_split(np.concatenate([np.cos(phase_x[:, i * len_y:(i + 1) * len_y]), -np.sin(phase_x[:, i * len_y:(i + 1) * len_y])], axis=1)) for i in range(y_devs)])
    phase_y = (np.outer(freq, x) % grid_n) * turn
    real = np.concatenate([np.cos(phase_y), np.sin(phase_y)], axis=1)
    imag = np.concatenate([-np.sin(phase_y), np.cos(phase_y)], axis=1)
    rows = np.stack([real.reshape(z_devs, len_z, 2 * grid_n), imag.reshape(z_devs, len_z, 2 * grid_n)], axis=1)
    table_y = np_split(rows.reshape(2 * grid_n, 2 * grid_n))
    table_z = []
    for first in (0, 2):
        pos = np.arange(z_devs)[:, None] * len_z + first + np.arange(2)[None, :]
        phase_z = ((freq[:, None, None] * pos[None]) % grid_n) * turn
        real = np.stack([np.cos(phase_z), np.sin(phase_z)], axis=3).reshape(grid_n, -1)
        imag = np.stack([-np.sin(phase_z), np.cos(phase_z)], axis=3).reshape(grid_n, -1)
        table_z.append(np_split(np.concatenate([real, imag], axis=0)))
    return table_x, table_y, np.stack(table_z)


def ghost_rows(group):
    return -(-8 * len(GROUPS[group]) // 16) * 16


def energy_kernel(y_devs, z_devs, q_hbm, m_hbm, idx_hbm, w_hbm, bc_hbm, tx_hbm, ty_hbm, tz_hbm, ek_ref, sum_ref,
                  q_ref, m_ref, idx_ref, w_ref, near_ref, xh_ref, xl_ref, ph_ref, pl_ref, acc_refs, got_refs, grid_ref, mid_ref, mode_ref,
                  code_refs, recv_refs, scale_ref, rscale_ref,
                  deq_ref, zed_ref, bc_ref, tx_ref, ty_ref, tz_ref, row_ref, rrow_ref,
                  early_sem, load_sem, swap_sem, send_sem, recv_sem, ssend_sem, srecv_sem, row_sem):
    my_y = lax.axis_index('ydom')
    my_z = lax.axis_index('zdom')
    grid_n = xh_ref.shape[1]
    slots = q_ref.shape[1]
    len_y = grid_n // y_devs
    half = grid_n // 2
    n_groups = len(GROUPS)
    barrier = pltpu.get_barrier_semaphore()
    partner = {'ydom': 1 - my_y}

    def chip(step):
        return (my_z + step) & (z_devs - 1)

    def far_first(start):
        pl.loop(z_devs // 2, z_devs)(start)
        pl.loop(1, z_devs // 2)(start)

    def slot_loads(piece):
        cols = pl.ds(0, EARLY) if piece == 0 else pl.ds(EARLY, slots - EARLY)
        return [pltpu.make_async_copy(hbm.at[lead + (cols,)], ref.at[lead + (cols,)], early_sem.at[piece, k])
                for k, (hbm, ref, lead) in enumerate(((q_hbm, q_ref, (slice(None),)), (m_hbm, m_ref, (slice(None),)), (idx_hbm, idx_ref, (slice(None),)), (w_hbm, w_ref, (slice(None), slice(None)))))]

    for piece in range(2):
        for load in slot_loads(piece):
            load.start()

    @pl.loop(1, z_devs)
    def _(step):
        pl.semaphore_signal(barrier, inc=1, device_id={'zdom': chip(step)}, device_id_type=MESH)

    pl.semaphore_signal(barrier, inc=1, device_id=partner, device_id_type=MESH)

    loads = [pltpu.make_async_copy(tx_hbm.at[my_y], tx_ref, load_sem.at[0]), pltpu.make_async_copy(ty_hbm, ty_ref, load_sem.at[1]),
             pltpu.make_async_copy(tz_hbm, tz_ref, load_sem.at[2]), pltpu.make_async_copy(bc_hbm, bc_ref, load_sem.at[3])]
    for load in loads:
        load.start()

    def swap(group):
        return pltpu.make_async_remote_copy(src_ref=acc_refs[group], dst_ref=got_refs[group], send_sem=swap_sem.at[0, group], recv_sem=swap_sem.at[1, group], device_id=partner, device_id_type=MESH)

    def send(group, step):
        other = chip(step)
        return pltpu.make_async_remote_copy(src_ref=code_refs[group].at[other], dst_ref=recv_refs[group].at[my_z], send_sem=send_sem.at[group], recv_sem=recv_sem.at[group], device_id={'zdom': other}, device_id_type=MESH)

    def send_scale(last, step):
        return pltpu.make_async_remote_copy(src_ref=scale_ref.at[last, pl.ds(0, 2 - last)], dst_ref=rscale_ref.at[last, my_z, pl.ds(0, 2 - last)], send_sem=ssend_sem.at[last], recv_sem=srecv_sem.at[last], device_id={'zdom': chip(step)}, device_id_type=MESH)

    def spread(group, base):
        planes = GROUPS[group]
        zero_16 = jnp.zeros((16, SUB), BF16)
        total = None
        for sub in range(CHUNK // SUB):
            slot = sub % 2
            cols = pl.ds(pl.multiple_of(base + sub * SUB, SUB), SUB)
            row_16 = lax.broadcasted_iota(jnp.int32, (16, SUB), 0)
            if group == 0:
                weight = q_ref[:, cols] * m_ref[:, cols].astype(F32)
                ahead = row_16 - idx_ref[0:1, cols]
                taps = w_ref[0, :, cols] * weight
                high, low = split_bf16(pick(ahead, taps))
                tile_x = (-(ahead >> 4) & 15).astype(F32).astype(BF16)
                for r in range(grid_n // 16):
                    hit = tile_x == r
                    near_ref[slot, 0, 16 * r:16 * r + 16, :] = jnp.where(hit, high, zero_16)
                    near_ref[slot, 1, 16 * r:16 * r + 16, :] = jnp.where(hit, low, zero_16)
                xh_ref[cols, :] = near_ref[slot, 0].T
                xl_ref[cols, :] = near_ref[slot, 1].T
            ahead = row_16 - idx_ref[1:2, cols]
            line_y = pick(ahead, w_ref[1, :, cols])
            tile = -(ahead >> 4)
            ghost_y = jnp.where(tile[:8] == len_y // 16, line_y[:8], 0.0)
            tile_y = tile.astype(F32).astype(BF16)
            line_z = pick(row_16[:8] - idx_ref[2:3, cols], w_ref[2, :, cols], False)
            sides = [split_bf16(line_y * line_z[z:z + 1]) for z in planes]
            for r in range(len_y // 16):
                hit = tile_y == r
                for k, side in enumerate(sides):
                    first = k * len_y + 16 * r
                    ph_ref[slot, first:first + 16, :] = jnp.where(hit, side[0], zero_16)
                    pl_ref[slot, first:first + 16, :] = jnp.where(hit, side[1], zero_16)
            ghosts = [ghost_y * line_z[z:z + 1] for z in planes]
            if len(planes) % 2:
                ghosts.append(jnp.zeros((8, SUB), F32))
            high, low = split_bf16(jnp.concatenate(ghosts, axis=0))
            top = len(planes) * len_y
            rows = pl.ds(0, top + ghost_rows(group))
            ph_ref[slot, top:top + ghost_rows(group), :] = high
            pl_ref[slot, top:top + ghost_rows(group), :] = low
            if group == 0:
                part = dot3((ph_ref[slot, rows, :], pl_ref[slot, rows, :]), (near_ref[slot, 0], near_ref[slot, 1]), 1)
            else:
                part = dot3((ph_ref[slot, rows, :], pl_ref[slot, rows, :]), (xh_ref[cols, :], xl_ref[cols, :]))
            total = part if total is None else total + part
        acc_refs[group][...] += total

    def transform_send(group):
        planes = GROUPS[group]
        acc_ref, got_ref = acc_refs[group], got_refs[group]
        swap(group).wait()
        mine, theirs = my_y * len_y, (1 - my_y) * len_y
        peak = jnp.full((1, 1), 1e-30, F32)
        for first in range(0, len(planes), 2):
            count = min(2, len(planes) - first)
            for k in range(count):
                block = pl.ds((first + k) * len_y, len_y)
                grid_ref[pl.ds(pl.multiple_of(k * grid_n + mine, len_y), len_y), :] = acc_ref[block, :]
                grid_ref[pl.ds(pl.multiple_of(k * grid_n + theirs, len_y), len_y), :] = got_ref[block, :]
            for k in range(count):
                ghost = pl.ds(len(planes) * len_y + 8 * (first + k), 8)
                grid_ref[pl.ds(pl.multiple_of(k * grid_n + theirs, len_y), 8), :] += acc_ref[ghost, :]
                grid_ref[pl.ds(pl.multiple_of(k * grid_n + mine, len_y), 8), :] += got_ref[ghost, :]
            size = count * grid_n
            mid_ref[pl.ds(0, size), :] = dot3(split_bf16(grid_ref[pl.ds(0, size), :]), (tx_ref[0], tx_ref[1]))
            columns = [jnp.concatenate([mid_ref[pl.ds(k * grid_n, grid_n), pl.ds(c * half, half)] for c in range(2)], axis=0) for k in range(count)]
            modes = dot3((ty_ref[0], ty_ref[1]), split_bf16(jnp.concatenate(columns, axis=1)))
            mode_ref[:, pl.ds(first * half, count * half)] = modes
            peak = jnp.maximum(peak, jnp.max(jnp.abs(modes), keepdims=True))
        gain = CODE_MAX / peak
        for k in range(len(planes)):
            codes = jnp.round(mode_ref[:, pl.ds(k * half, half)] * gain).astype(jnp.int32).astype(jnp.int16)
            code_refs[group][:, k] = codes.reshape(z_devs, 8, half)
        last = group // 2
        scale_ref[last, pl.ds(group % 2, 1)] = jnp.broadcast_to(peak * (1.0 / CODE_MAX), (1, 128))

        def start(step):
            send(group, step).start()
            if group:
                send_scale(last, step).start()

        far_first(start)

        recv_refs[group][my_z] = code_refs[group][my_z]
        if group:
            rscale_ref[last, my_z] = scale_ref[last]

    def await_all(ref, sem):
        pltpu.make_async_copy(ref, ref, sem).wait()

    def await_codes(group):
        await_all(recv_refs[group].at[pl.ds(0, z_devs - 1)], recv_sem.at[group])

    def await_scale(last):
        await_all(rscale_ref.at[last, pl.ds(0, z_devs - 1), pl.ds(0, 2 - last)], srecv_sem.at[last])

    def decode(group, planes):
        codes = recv_refs[group][:, planes].astype(jnp.int32).astype(F32)
        return codes * rscale_ref[group // 2, :, pl.ds(group % 2, 1), :].reshape(z_devs, 1, 1, half)

    def fold(part, planes):
        rows = z_devs * 16
        flat = planes.reshape(rows, half)
        deq_ref[part, pl.ds(16, rows - 16), :] += flat[:rows - 16]
        deq_ref[part, pl.ds(0, 16), :] += flat[rows - 16:]

    def transform_z(part):
        flat = deq_ref.at[part]
        columns = [flat[pl.ds(ky, grid_n, stride=4), :] for ky in range(4)]
        zed = dot3((tz_ref[part, 0], tz_ref[part, 1]), split_bf16(jnp.concatenate(columns, axis=1)))
        if part == 0:
            zed_ref[...] = zed
        else:
            zed_ref[...] += zed

    for acc_ref in acc_refs:
        acc_ref[...] = jnp.zeros_like(acc_ref)
    for load in slot_loads(0):
        load.wait()
    for group in range(n_groups):
        @pl.loop(0, slots // CHUNK)
        def _(i):
            if group == 0:
                @pl.when(i == EARLY // CHUNK)
                def _():
                    for load in slot_loads(1):
                        load.wait()

            spread(group, i * CHUNK)
            if group:
                @pl.when(i == STEP_AT[group])
                def _():
                    transform_send(group - 1)

        if group == 0:
            pl.semaphore_wait(barrier, z_devs)
            for load in loads:
                load.wait()
        swap(group).start()
    transform_send(n_groups - 1)

    rows = z_devs * 16
    await_codes(0)
    await_scale(0)
    for part in range(2):
        deq_ref[part] = decode(0, slice(2 * part, 2 * part + 2)).reshape(rows, half)
    await_codes(1)
    fold(0, decode(1, slice(0, 2)))
    transform_z(0)
    await_codes(2)
    await_scale(1)
    late = decode(2, slice(0, 1))
    fold(1, jnp.concatenate([late, jnp.zeros_like(late)], axis=1))
    transform_z(1)

    row = jnp.zeros((8, half), F32)
    for ky in range(4):
        cols = pl.ds(ky * half, half)
        real, imag = zed_ref[pl.ds(0, grid_n), cols], zed_ref[pl.ds(grid_n, grid_n), cols]
        power = real * real + imag * imag
        for part in range(2):
            place = pl.ds(4 * part + ky, half, stride=8)
            value = bc_ref[place, :] * power[part * half:(part + 1) * half].T
            ek_ref[place, :] = value
            row += jnp.sum(value.reshape(half // 8, 8, half), axis=0)
    row_ref[0] = jnp.broadcast_to(jnp.sum(row, axis=0, keepdims=True), (8, half))

    others = rrow_ref.at[pl.ds(0, z_devs - 1), pl.ds(0, 1)]
    pair = pltpu.make_async_remote_copy(src_ref=row_ref.at[0, pl.ds(0, 1)], dst_ref=row_ref.at[1, pl.ds(0, 1)], send_sem=row_sem.at[2], recv_sem=row_sem.at[3], device_id=partner, device_id_type=MESH)
    pair.start()
    pair.wait()
    row_ref[2] = row_ref[0] + row_ref[1]

    def start(step):
        pltpu.make_async_remote_copy(src_ref=row_ref.at[2, pl.ds(0, 1)], dst_ref=rrow_ref.at[my_z, pl.ds(0, 1)], send_sem=row_sem.at[0], recv_sem=row_sem.at[1], device_id={'zdom': chip(step)}, device_id_type=MESH).start()

    far_first(start)
    rrow_ref[my_z, pl.ds(0, 1)] = row_ref[2, pl.ds(0, 1)]
    await_all(others, row_sem.at[1])
    sum_ref[0] = jnp.sum(rrow_ref[:, pl.ds(0, 1), :]) * (0.5 / (grid_n * grid_n * grid_n))
    await_all(others, row_sem.at[0])
    for group in range(n_groups):
        await_all(code_refs[group].at[pl.ds(0, z_devs - 1)], send_sem.at[group])
    for last in range(2):
        await_all(rscale_ref.at[last, pl.ds(0, z_devs - 1), pl.ds(0, 2 - last)], ssend_sem.at[last])


def solution(mesh):
    y_devs = mesh.shape['ydom']
    z_devs = mesh.shape['zdom']
    slot_spec = P(('sys', 'ydom', 'zdom'))
    mode_spec = P(('sys', 'ydom'), 'zdom', None)

    def local_energy(charge, real_mask, grid_idx, spline_w, influence):
        grid_n = influence.shape[2]
        slots = charge.shape[0]
        half = grid_n // 2
        n_groups = len(GROUPS)
        table_x, table_y, table_z = dft_tables(grid_n, y_devs, z_devs)
        any_spec = pl.BlockSpec(memory_space=pl.ANY)
        rows = [len(GROUPS[g]) * (grid_n // y_devs) + ghost_rows(g) for g in range(n_groups)]
        codes = [pltpu.VMEM((z_devs, len(planes), 8, half), jnp.int16) for planes in GROUPS]
        tiles = jnp.swapaxes(influence.reshape(half, 4, 2, half), 1, 2).reshape(8 * half, half)
        mode_energy, energy = pl.pallas_call(
            functools.partial(energy_kernel, y_devs, z_devs),
            in_specs=[any_spec] * 8,
            out_specs=[pl.BlockSpec(memory_space=pltpu.VMEM), pl.BlockSpec(memory_space=pltpu.SMEM)],
            out_shape=[pltpu.VMEM((8 * half, half), F32), jax.ShapeDtypeStruct((1,), F32)],
            scratch_shapes=[
                pltpu.VMEM((1, slots), F32), pltpu.VMEM((1, slots), jnp.int32), pltpu.VMEM((3, slots), jnp.int32), pltpu.VMEM((3, 4, slots), F32),
                pltpu.VMEM((2, 2, grid_n, SUB), BF16), pltpu.VMEM((slots, grid_n), BF16), pltpu.VMEM((slots, grid_n), BF16),
                pltpu.VMEM((2, rows[0], SUB), BF16), pltpu.VMEM((2, rows[0], SUB), BF16),
                [pltpu.VMEM((r, grid_n), F32) for r in rows], [pltpu.VMEM((r, grid_n), F32) for r in rows],
                pltpu.VMEM((2 * grid_n, grid_n), F32), pltpu.VMEM((2 * grid_n, grid_n), F32), pltpu.VMEM((2 * grid_n, 4 * half), F32),
                codes, codes,
                pltpu.VMEM((2, 2, 128), F32), pltpu.VMEM((2, z_devs, 2, 128), F32),
                pltpu.VMEM((2, z_devs * 16, half), F32), pltpu.VMEM((2 * grid_n, 4 * half), F32),
                pltpu.VMEM((8 * half, half), F32),
                pltpu.VMEM(table_x.shape[1:], BF16), pltpu.VMEM(table_y.shape, BF16), pltpu.VMEM(table_z.shape, BF16),
                pltpu.VMEM((3, 8, 128), F32), pltpu.VMEM((z_devs, 8, 128), F32),
                pltpu.SemaphoreType.DMA((2, 4)), pltpu.SemaphoreType.DMA((4,)), pltpu.SemaphoreType.DMA((2, n_groups)),
                pltpu.SemaphoreType.DMA((n_groups,)), pltpu.SemaphoreType.DMA((n_groups,)),
                pltpu.SemaphoreType.DMA((2,)), pltpu.SemaphoreType.DMA((2,)),
                pltpu.SemaphoreType.DMA((4,)),
            ],
            compiler_params=pltpu.CompilerParams(collective_id=0, has_side_effects=True, vmem_limit_bytes=60 * 1024 * 1024),
            name="energy",
        )(charge.reshape(1, slots), real_mask.reshape(1, slots), grid_idx.T, jnp.transpose(spline_w, (1, 2, 0)), tiles, jnp.asarray(table_x), jnp.asarray(table_y), jnp.asarray(table_z))
        mode_energy = lax.optimization_barrier(0.5 * mode_energy)
        return jnp.swapaxes(mode_energy.reshape(half, 2, 4, half), 1, 2).reshape(influence.shape), energy

    return jax.shard_map(local_energy, mesh=mesh, in_specs=(slot_spec, slot_spec, P(('sys', 'ydom', 'zdom'), None), P(('sys', 'ydom', 'zdom'), None, None), mode_spec), out_specs=(mode_spec, P('sys')), check_vma=False)
```

```python
import functools
import math
import jax
import jax.numpy as jnp
import numpy as np
from jax import lax
from jax.experimental import pallas as pl
from jax.experimental.pallas import tpu as pltpu
from jax.sharding import PartitionSpec as P

F32 = jnp.float32
BF16 = jnp.bfloat16
SUB = 256
CHUNK = 2048
GROUPS = ((0, 1, 2, 3), (4, 5), (6,))
STEP_AT = (0, 2, 3)
EARLY = 2048
CODE_MAX = 32767.0
MESH = pl.DeviceIdType.MESH


def split_bf16(value):
    high = value.astype(BF16)
    return high, (value - high.astype(F32)).astype(BF16)


def dot3(lhs, rhs, rhs_dim=0):
    def dot(a, b):
        return lax.dot_general(a, b, (((1,), (rhs_dim,)), ((), ())), preferred_element_type=F32)
    return dot(lhs[0], rhs[0]) + dot(lhs[1], rhs[0]) + dot(lhs[0], rhs[1])


def pick(ahead, taps, wrap=True):
    place = ahead & 15 if wrap else ahead
    value = jnp.zeros(ahead.shape, F32)
    for t in range(4):
        value = jnp.where(place == t, taps[t:t + 1], value)
    return value


def np_split(value):
    value = np.asarray(value, np.float32)
    high = value.astype(BF16)
    return np.stack([high, (value - high.astype(np.float32)).astype(BF16)])


def dft_tables(grid_n, y_devs, z_devs):
    turn = 2.0 * np.pi / grid_n
    len_y, len_z = grid_n // y_devs, grid_n // z_devs
    x = np.arange(grid_n)
    freq = np.arange(grid_n)
    phase_x = (np.outer(x, freq) % grid_n) * turn
    table_x = np.stack([np_split(np.concatenate([np.cos(phase_x[:, i * len_y:(i + 1) * len_y]), -np.sin(phase_x[:, i * len_y:(i + 1) * len_y])], axis=1)) for i in range(y_devs)])
    phase_y = (np.outer(freq, x) % grid_n) * turn
    real = np.concatenate([np.cos(phase_y), np.sin(phase_y)], axis=1)
    imag = np.concatenate([-np.sin(phase_y), np.cos(phase_y)], axis=1)
    rows = np.stack([real.reshape(z_devs, len_z, 2 * grid_n), imag.reshape(z_devs, len_z, 2 * grid_n)], axis=1)
    table_y = np_split(rows.reshape(2 * grid_n, 2 * grid_n))
    table_z = []
    for first in (0, 2):
        pos = np.arange(z_devs)[:, None] * len_z + first + np.arange(2)[None, :]
        phase_z = ((freq[:, None, None] * pos[None]) % grid_n) * turn
        real = np.stack([np.cos(phase_z), np.sin(phase_z)], axis=3).reshape(grid_n, -1)
        imag = np.stack([-np.sin(phase_z), np.cos(phase_z)], axis=3).reshape(grid_n, -1)
        table_z.append(np_split(np.concatenate([real, imag], axis=0)))
    return table_x, table_y, np.stack(table_z)


def ghost_rows(group):
    return -(-8 * len(GROUPS[group]) // 16) * 16


def energy_kernel(y_devs, z_devs, q_hbm, m_hbm, idx_hbm, w_hbm, bc_hbm, tx_hbm, ty_hbm, tz_hbm, ek_ref, sum_ref,
                  q_ref, m_ref, idx_ref, w_ref, near_ref, xh_ref, xl_ref, ph_ref, pl_ref, acc_refs, got_refs, grid_ref, mid_ref, mode_ref,
                  code_refs, recv_refs,
                  deq_ref, zed_ref, bc_ref, tx_ref, ty_ref, tz_ref, row_ref, rrow_ref,
                  early_sem, load_sem, swap_sem, send_sem, recv_sem, row_sem):
    my_y = lax.axis_index('ydom')
    my_z = lax.axis_index('zdom')
    grid_n = xh_ref.shape[1]
    slots = q_ref.shape[1]
    len_y = grid_n // y_devs
    half = grid_n // 2
    n_groups = len(GROUPS)
    barrier = pltpu.get_barrier_semaphore()
    partner = {'ydom': 1 - my_y}

    def chip(step):
        return (my_z + step) & (z_devs - 1)

    def far_first(start):
        pl.loop(z_devs // 2, z_devs)(start)
        pl.loop(1, z_devs // 2)(start)

    def slot_loads(piece):
        cols = pl.ds(0, EARLY) if piece == 0 else pl.ds(EARLY, slots - EARLY)
        return [pltpu.make_async_copy(hbm.at[lead + (cols,)], ref.at[lead + (cols,)], early_sem.at[piece, k])
                for k, (hbm, ref, lead) in enumerate(((q_hbm, q_ref, (slice(None),)), (m_hbm, m_ref, (slice(None),)), (idx_hbm, idx_ref, (slice(None),)), (w_hbm, w_ref, (slice(None), slice(None)))))]

    for piece in range(2):
        for load in slot_loads(piece):
            load.start()

    @pl.loop(1, z_devs)
    def _(step):
        pl.semaphore_signal(barrier, inc=1, device_id={'zdom': chip(step)}, device_id_type=MESH)

    pl.semaphore_signal(barrier, inc=1, device_id=partner, device_id_type=MESH)

    loads = [pltpu.make_async_copy(tx_hbm.at[my_y], tx_ref, load_sem.at[0]), pltpu.make_async_copy(ty_hbm, ty_ref, load_sem.at[1]),
             pltpu.make_async_copy(tz_hbm, tz_ref, load_sem.at[2]), pltpu.make_async_copy(bc_hbm, bc_ref, load_sem.at[3])]
    for load in loads:
        load.start()

    def swap(group):
        return pltpu.make_async_remote_copy(src_ref=acc_refs[group], dst_ref=got_refs[group], send_sem=swap_sem.at[0, group], recv_sem=swap_sem.at[1, group], device_id=partner, device_id_type=MESH)

    def used(group):
        return pl.ds(0, 8 * len(GROUPS[group]) + 2)

    def send(group, step):
        other = chip(step)
        return pltpu.make_async_remote_copy(src_ref=code_refs[group].at[other, used(group)], dst_ref=recv_refs[group].at[my_z, used(group)], send_sem=send_sem.at[group], recv_sem=recv_sem.at[group], device_id={'zdom': other}, device_id_type=MESH)

    def spread(group, base):
        planes = GROUPS[group]
        zero_16 = jnp.zeros((16, SUB), BF16)
        total = None
        for sub in range(CHUNK // SUB):
            slot = sub % 2
            cols = pl.ds(pl.multiple_of(base + sub * SUB, SUB), SUB)
            row_16 = lax.broadcasted_iota(jnp.int32, (16, SUB), 0)
            if group == 0:
                weight = q_ref[:, cols] * m_ref[:, cols].astype(F32)
                ahead = row_16 - idx_ref[0:1, cols]
                taps = w_ref[0, :, cols] * weight
                high, low = split_bf16(pick(ahead, taps))
                tile_x = (-(ahead >> 4) & 15).astype(F32).astype(BF16)
                for r in range(grid_n // 16):
                    hit = tile_x == r
                    near_ref[slot, 0, 16 * r:16 * r + 16, :] = jnp.where(hit, high, zero_16)
                    near_ref[slot, 1, 16 * r:16 * r + 16, :] = jnp.where(hit, low, zero_16)
                xh_ref[cols, :] = near_ref[slot, 0].T
                xl_ref[cols, :] = near_ref[slot, 1].T
            ahead = row_16 - idx_ref[1:2, cols]
            line_y = pick(ahead, w_ref[1, :, cols])
            tile = -(ahead >> 4)
            ghost_y = jnp.where(tile[:8] == len_y // 16, line_y[:8], 0.0)
            tile_y = tile.astype(F32).astype(BF16)
            line_z = pick(row_16[:8] - idx_ref[2:3, cols], w_ref[2, :, cols], False)
            sides = [split_bf16(line_y * line_z[z:z + 1]) for z in planes]
            for r in range(len_y // 16):
                hit = tile_y == r
                for k, side in enumerate(sides):
                    first = k * len_y + 16 * r
                    ph_ref[slot, first:first + 16, :] = jnp.where(hit, side[0], zero_16)
                    pl_ref[slot, first:first + 16, :] = jnp.where(hit, side[1], zero_16)
            ghosts = [ghost_y * line_z[z:z + 1] for z in planes]
            if len(planes) % 2:
                ghosts.append(jnp.zeros((8, SUB), F32))
            high, low = split_bf16(jnp.concatenate(ghosts, axis=0))
            top = len(planes) * len_y
            rows = pl.ds(0, top + ghost_rows(group))
            ph_ref[slot, top:top + ghost_rows(group), :] = high
            pl_ref[slot, top:top + ghost_rows(group), :] = low
            if group == 0:
                part = dot3((ph_ref[slot, rows, :], pl_ref[slot, rows, :]), (near_ref[slot, 0], near_ref[slot, 1]), 1)
            else:
                part = dot3((ph_ref[slot, rows, :], pl_ref[slot, rows, :]), (xh_ref[cols, :], xl_ref[cols, :]))
            total = part if total is None else total + part
        acc_refs[group][...] += total

    def transform_send(group):
        planes = GROUPS[group]
        acc_ref, got_ref = acc_refs[group], got_refs[group]
        swap(group).wait()
        mine, theirs = my_y * len_y, (1 - my_y) * len_y
        peak = jnp.full((1, 1), 1e-30, F32)
        for first in range(0, len(planes), 2):
            count = min(2, len(planes) - first)
            for k in range(count):
                block = pl.ds((first + k) * len_y, len_y)
                grid_ref[pl.ds(pl.multiple_of(k * grid_n + mine, len_y), len_y), :] = acc_ref[block, :]
                grid_ref[pl.ds(pl.multiple_of(k * grid_n + theirs, len_y), len_y), :] = got_ref[block, :]
            for k in range(count):
                ghost = pl.ds(len(planes) * len_y + 8 * (first + k), 8)
                grid_ref[pl.ds(pl.multiple_of(k * grid_n + theirs, len_y), 8), :] += acc_ref[ghost, :]
                grid_ref[pl.ds(pl.multiple_of(k * grid_n + mine, len_y), 8), :] += got_ref[ghost, :]
            size = count * grid_n
            mid_ref[pl.ds(0, size), :] = dot3(split_bf16(grid_ref[pl.ds(0, size), :]), (tx_ref[0], tx_ref[1]))
            columns = [jnp.concatenate([mid_ref[pl.ds(k * grid_n, grid_n), pl.ds(c * half, half)] for c in range(2)], axis=0) for k in range(count)]
            modes = dot3((ty_ref[0], ty_ref[1]), split_bf16(jnp.concatenate(columns, axis=1)))
            mode_ref[:, pl.ds(first * half, count * half)] = modes
            peak = jnp.maximum(peak, jnp.max(jnp.abs(modes), keepdims=True))
        power = jnp.ceil(jnp.log2(peak * (1.0 / CODE_MAX)) + 1e-3)
        gain = jnp.exp2(-power)
        for first in range(0, len(planes), 2):
            count = min(2, len(planes) - first)
            scaled = [(mode_ref[:, pl.ds((first + k) * half, half)] * gain).reshape(z_devs, 8, half) for k in range(count)]
            codes = jnp.round(jnp.concatenate(scaled, axis=1)).astype(jnp.int32).astype(jnp.int16)
            code_refs[group][:, pl.ds(8 * first, 8 * count), :] = codes
        code_refs[group][:, pl.ds(8 * len(planes), 2), :] = jnp.broadcast_to(power.astype(jnp.int32), (z_devs, 2, half)).astype(jnp.int16)

        def start(step):
            send(group, step).start()

        far_first(start)
        recv_refs[group][my_z] = code_refs[group][my_z]

    def await_all(ref, sem):
        pltpu.make_async_copy(ref, ref, sem).wait()

    def await_codes(group):
        await_all(recv_refs[group].at[pl.ds(0, z_devs - 1), used(group)], recv_sem.at[group])

    def decode(group, first, count):
        powers = recv_refs[group][:, pl.ds(8 * len(GROUPS[group]), 2), :].astype(jnp.int32).astype(F32)
        codes = recv_refs[group][:, pl.ds(8 * first, 8 * count), :].astype(jnp.int32).astype(F32)
        return codes * jnp.exp2(powers[:, :1, :])

    def fold(part, planes):
        rows = z_devs * 16
        flat = planes.reshape(rows, half)
        deq_ref[part, pl.ds(16, rows - 16), :] += flat[:rows - 16]
        deq_ref[part, pl.ds(0, 16), :] += flat[rows - 16:]

    def transform_z(part):
        flat = deq_ref.at[part]
        columns = [flat[pl.ds(ky, grid_n, stride=4), :] for ky in range(4)]
        zed = dot3((tz_ref[part, 0], tz_ref[part, 1]), split_bf16(jnp.concatenate(columns, axis=1)))
        if part == 0:
            zed_ref[...] = zed
        else:
            zed_ref[...] += zed

    for acc_ref in acc_refs:
        acc_ref[...] = jnp.zeros_like(acc_ref)
    for load in slot_loads(0):
        load.wait()
    for group in range(n_groups):
        @pl.loop(0, slots // CHUNK)
        def _(i):
            if group == 0:
                @pl.when(i == EARLY // CHUNK)
                def _():
                    for load in slot_loads(1):
                        load.wait()

            spread(group, i * CHUNK)
            if group:
                @pl.when(i == STEP_AT[group])
                def _():
                    transform_send(group - 1)

        if group == 0:
            pl.semaphore_wait(barrier, z_devs)
            for load in loads:
                load.wait()
        swap(group).start()
    transform_send(n_groups - 1)

    rows = z_devs * 16
    await_codes(0)
    for part in range(2):
        deq_ref[part] = decode(0, 2 * part, 2).reshape(rows, half)
    await_codes(1)
    fold(0, decode(1, 0, 2))
    transform_z(0)
    await_codes(2)
    late = decode(2, 0, 1)
    fold(1, jnp.concatenate([late, jnp.zeros_like(late)], axis=1))
    transform_z(1)

    row = jnp.zeros((8, half), F32)
    for ky in range(4):
        cols = pl.ds(ky * half, half)
        real, imag = zed_ref[pl.ds(0, grid_n), cols], zed_ref[pl.ds(grid_n, grid_n), cols]
        power = real * real + imag * imag
        for part in range(2):
            place = pl.ds(4 * part + ky, half, stride=8)
            value = bc_ref[place, :] * power[part * half:(part + 1) * half].T
            ek_ref[place, :] = value
            row += jnp.sum(value.reshape(half // 8, 8, half), axis=0)
    row_ref[0] = jnp.broadcast_to(jnp.sum(row, axis=0, keepdims=True), (8, half))

    others = rrow_ref.at[pl.ds(0, z_devs - 1), pl.ds(0, 1)]
    pair = pltpu.make_async_remote_copy(src_ref=row_ref.at[0, pl.ds(0, 1)], dst_ref=row_ref.at[1, pl.ds(0, 1)], send_sem=row_sem.at[2], recv_sem=row_sem.at[3], device_id=partner, device_id_type=MESH)
    pair.start()
    pair.wait()
    row_ref[2] = row_ref[0] + row_ref[1]

    def start(step):
        pltpu.make_async_remote_copy(src_ref=row_ref.at[2, pl.ds(0, 1)], dst_ref=rrow_ref.at[my_z, pl.ds(0, 1)], send_sem=row_sem.at[0], recv_sem=row_sem.at[1], device_id={'zdom': chip(step)}, device_id_type=MESH).start()

    far_first(start)
    rrow_ref[my_z, pl.ds(0, 1)] = row_ref[2, pl.ds(0, 1)]
    await_all(others, row_sem.at[1])
    sum_ref[0] = jnp.sum(rrow_ref[:, pl.ds(0, 1), :]) * (0.5 / (grid_n * grid_n * grid_n))
    await_all(others, row_sem.at[0])
    for group in range(n_groups):
        await_all(code_refs[group].at[pl.ds(0, z_devs - 1), used(group)], send_sem.at[group])


def solution(mesh):
    y_devs = mesh.shape['ydom']
    z_devs = mesh.shape['zdom']
    slot_spec = P(('sys', 'ydom', 'zdom'))
    mode_spec = P(('sys', 'ydom'), 'zdom', None)

    def local_energy(charge, real_mask, grid_idx, spline_w, influence):
        grid_n = influence.shape[2]
        slots = charge.shape[0]
        half = grid_n // 2
        n_groups = len(GROUPS)
        table_x, table_y, table_z = dft_tables(grid_n, y_devs, z_devs)
        any_spec = pl.BlockSpec(memory_space=pl.ANY)
        rows = [len(GROUPS[g]) * (grid_n // y_devs) + ghost_rows(g) for g in range(n_groups)]
        codes = [pltpu.VMEM((z_devs, -(-(8 * len(planes) + 2) // 16) * 16, half), jnp.int16) for planes in GROUPS]
        tiles = jnp.swapaxes(influence.reshape(half, 4, 2, half), 1, 2).reshape(8 * half, half)
        mode_energy, energy = pl.pallas_call(
            functools.partial(energy_kernel, y_devs, z_devs),
            in_specs=[any_spec] * 8,
            out_specs=[pl.BlockSpec(memory_space=pltpu.VMEM), pl.BlockSpec(memory_space=pltpu.SMEM)],
            out_shape=[pltpu.VMEM((8 * half, half), F32), jax.ShapeDtypeStruct((1,), F32)],
            scratch_shapes=[
                pltpu.VMEM((1, slots), F32), pltpu.VMEM((1, slots), jnp.int32), pltpu.VMEM((3, slots), jnp.int32), pltpu.VMEM((3, 4, slots), F32),
                pltpu.VMEM((2, 2, grid_n, SUB), BF16), pltpu.VMEM((slots, grid_n), BF16), pltpu.VMEM((slots, grid_n), BF16),
                pltpu.VMEM((2, rows[0], SUB), BF16), pltpu.VMEM((2, rows[0], SUB), BF16),
                [pltpu.VMEM((r, grid_n), F32) for r in rows], [pltpu.VMEM((r, grid_n), F32) for r in rows],
                pltpu.VMEM((2 * grid_n, grid_n), F32), pltpu.VMEM((2 * grid_n, grid_n), F32), pltpu.VMEM((2 * grid_n, 4 * half), F32),
                codes, codes,
                pltpu.VMEM((2, z_devs * 16, half), F32), pltpu.VMEM((2 * grid_n, 4 * half), F32),
                pltpu.VMEM((8 * half, half), F32),
                pltpu.VMEM(table_x.shape[1:], BF16), pltpu.VMEM(table_y.shape, BF16), pltpu.VMEM(table_z.shape, BF16),
                pltpu.VMEM((3, 8, 128), F32), pltpu.VMEM((z_devs, 8, 128), F32),
                pltpu.SemaphoreType.DMA((2, 4)), pltpu.SemaphoreType.DMA((4,)), pltpu.SemaphoreType.DMA((2, n_groups)),
                pltpu.SemaphoreType.DMA((n_groups,)), pltpu.SemaphoreType.DMA((n_groups,)),
                pltpu.SemaphoreType.DMA((4,)),
            ],
            compiler_params=pltpu.CompilerParams(collective_id=0, has_side_effects=True, vmem_limit_bytes=60 * 1024 * 1024),
            name="energy",
        )(charge.reshape(1, slots), real_mask.reshape(1, slots), grid_idx.T, jnp.transpose(spline_w, (1, 2, 0)), tiles, jnp.asarray(table_x), jnp.asarray(table_y), jnp.asarray(table_z))
        mode_energy = lax.optimization_barrier(0.5 * mode_energy)
        return jnp.swapaxes(mode_energy.reshape(half, 2, 4, half), 1, 2).reshape(influence.shape), energy

    return jax.shard_map(local_energy, mesh=mesh, in_specs=(slot_spec, slot_spec, P(('sys', 'ydom', 'zdom'), None), P(('sys', 'ydom', 'zdom'), None, None), mode_spec), out_specs=(mode_spec, P('sys')), check_vma=False)
```

```python
import functools
import math
import jax
import jax.numpy as jnp
import numpy as np
from jax import lax
from jax.experimental import pallas as pl
from jax.experimental.pallas import tpu as pltpu
from jax.sharding import PartitionSpec as P

F32 = jnp.float32
BF16 = jnp.bfloat16
SUB = 512
CHUNK = 2048
GROUPS = ((0, 1, 2, 3), (4, 5), (6,))
STEP_AT = (0, 2, 3)
EARLY = 2048
CODE_MAX = 32767.0
MESH = pl.DeviceIdType.MESH


def split_bf16(value):
    high = value.astype(BF16)
    return high, (value - high.astype(F32)).astype(BF16)


def dot3(lhs, rhs, rhs_dim=0):
    def dot(a, b):
        return lax.dot_general(a, b, (((1,), (rhs_dim,)), ((), ())), preferred_element_type=F32)
    return dot(lhs[0], rhs[0]) + dot(lhs[1], rhs[0]) + dot(lhs[0], rhs[1])


def pick(ahead, taps, wrap=True):
    place = ahead & 15 if wrap else ahead
    value = jnp.zeros(ahead.shape, F32)
    for t in range(4):
        value = jnp.where(place == t, taps[t:t + 1], value)
    return value


def np_split(value):
    value = np.asarray(value, np.float32)
    high = value.astype(BF16)
    return np.stack([high, (value - high.astype(np.float32)).astype(BF16)])


def dft_tables(grid_n, y_devs, z_devs):
    turn = 2.0 * np.pi / grid_n
    len_y, len_z = grid_n // y_devs, grid_n // z_devs
    x = np.arange(grid_n)
    freq = np.arange(grid_n)
    phase_x = (np.outer(x, freq) % grid_n) * turn
    table_x = np.stack([np_split(np.concatenate([np.cos(phase_x[:, i * len_y:(i + 1) * len_y]), -np.sin(phase_x[:, i * len_y:(i + 1) * len_y])], axis=1)) for i in range(y_devs)])
    table_y = []
    for parity in range(2):
        ky = (np.arange(z_devs)[None, :] * len_z + 2 * np.arange(2)[:, None] + parity).reshape(-1)
        phase_y = (np.outer(ky, np.arange(grid_n // 2)) % grid_n) * turn
        real = np.concatenate([np.cos(phase_y), np.sin(phase_y)], axis=1)
        imag = np.concatenate([-np.sin(phase_y), np.cos(phase_y)], axis=1)
        table_y.append(np_split(np.concatenate([real, imag], axis=0)))

    def z_table(first, count):
        pos = np.arange(z_devs)[:, None] * len_z + first + np.arange(count)[None, :]
        phase_z = ((freq[:, None, None] * pos[None]) % grid_n) * turn
        real = np.stack([np.cos(phase_z), np.sin(phase_z)], axis=3).reshape(grid_n, -1)
        imag = np.stack([-np.sin(phase_z), np.cos(phase_z)], axis=3).reshape(grid_n, -1)
        return np_split(np.concatenate([real, imag], axis=0))

    high, low = z_table(6, 1)
    late_z = np.concatenate([high, high, low], axis=1)
    return table_x, np.stack(table_y), np.stack([z_table(0, 2), z_table(2, 2)]), late_z


def ghost_rows(group):
    return -(-8 * len(GROUPS[group]) // 16) * 16


def energy_kernel(y_devs, z_devs, q_hbm, m_hbm, idx_hbm, w_hbm, bc_hbm, tx_hbm, ty_hbm, tz_hbm, tl_hbm, ek_ref, sum_ref,
                  q_ref, m_ref, idx_ref, w_ref, near_ref, xh_ref, xl_ref, ph_ref, pl_ref, acc_refs, got_refs, grid_ref, mid_ref, mode_ref,
                  code_refs, recv_refs,
                  deq_ref, zed_ref, bc_ref, tx_ref, ty_ref, tz_ref, tl_ref, late_ref, row_ref, rrow_ref,
                  early_sem, load_sem, swap_sem, send_sem, recv_sem, row_sem):
    my_y = lax.axis_index('ydom')
    my_z = lax.axis_index('zdom')
    grid_n = xh_ref.shape[1]
    slots = q_ref.shape[1]
    len_y = grid_n // y_devs
    half = grid_n // 2
    n_groups = len(GROUPS)
    barrier = pltpu.get_barrier_semaphore()
    partner = {'ydom': 1 - my_y}

    def chip(step):
        return (my_z + step) & (z_devs - 1)

    def far_first(start):
        pl.loop(z_devs // 2, z_devs)(start)
        pl.loop(1, z_devs // 2)(start)

    def slot_loads(piece):
        cols = pl.ds(0, EARLY) if piece == 0 else pl.ds(EARLY, slots - EARLY)
        return [pltpu.make_async_copy(hbm.at[lead + (cols,)], ref.at[lead + (cols,)], early_sem.at[piece, k])
                for k, (hbm, ref, lead) in enumerate(((q_hbm, q_ref, (slice(None),)), (m_hbm, m_ref, (slice(None),)), (idx_hbm, idx_ref, (slice(None),)), (w_hbm, w_ref, (slice(None), slice(None)))))]

    for piece in range(2):
        for load in slot_loads(piece):
            load.start()

    @pl.loop(1, z_devs)
    def _(step):
        pl.semaphore_signal(barrier, inc=1, device_id={'zdom': chip(step)}, device_id_type=MESH)

    pl.semaphore_signal(barrier, inc=1, device_id=partner, device_id_type=MESH)

    loads = [pltpu.make_async_copy(tx_hbm.at[my_y], tx_ref, load_sem.at[0]), pltpu.make_async_copy(ty_hbm, ty_ref, load_sem.at[1]),
             pltpu.make_async_copy(tz_hbm, tz_ref, load_sem.at[2]), pltpu.make_async_copy(bc_hbm, bc_ref, load_sem.at[3]), pltpu.make_async_copy(tl_hbm, tl_ref, load_sem.at[4])]
    for load in loads:
        load.start()

    def swap(group):
        return pltpu.make_async_remote_copy(src_ref=acc_refs[group], dst_ref=got_refs[group], send_sem=swap_sem.at[0, group], recv_sem=swap_sem.at[1, group], device_id=partner, device_id_type=MESH)

    def used(group):
        return pl.ds(0, 8 * len(GROUPS[group]) + 2)

    def send(group, step):
        other = chip(step)
        return pltpu.make_async_remote_copy(src_ref=code_refs[group].at[other, used(group)], dst_ref=recv_refs[group].at[my_z, used(group)], send_sem=send_sem.at[group], recv_sem=recv_sem.at[group], device_id={'zdom': other}, device_id_type=MESH)

    def spread(group, base):
        planes = GROUPS[group]
        zero_16 = jnp.zeros((16, SUB), BF16)
        total = None
        for sub in range(CHUNK // SUB):
            slot = sub % 2
            cols = pl.ds(pl.multiple_of(base + sub * SUB, SUB), SUB)
            row_16 = lax.broadcasted_iota(jnp.int32, (16, SUB), 0)
            if group == 0:
                weight = q_ref[:, cols] * m_ref[:, cols].astype(F32)
                ahead = row_16 - idx_ref[0:1, cols]
                taps = w_ref[0, :, cols] * weight
                high, low = split_bf16(pick(ahead, taps))
                tile_x = (-(ahead >> 4) & 15).astype(F32).astype(BF16)
                for r in range(grid_n // 16):
                    hit = tile_x == r
                    near_ref[slot, 0, 16 * r:16 * r + 16, :] = jnp.where(hit, high, zero_16)
                    near_ref[slot, 1, 16 * r:16 * r + 16, :] = jnp.where(hit, low, zero_16)
                xh_ref[cols, :] = near_ref[slot, 0].T
                xl_ref[cols, :] = near_ref[slot, 1].T
            ahead = row_16 - idx_ref[1:2, cols]
            line_y = pick(ahead, w_ref[1, :, cols])
            tile = -(ahead >> 4)
            ghost_y = jnp.where(tile[:8] == len_y // 16, line_y[:8], 0.0)
            tile_y = tile.astype(F32).astype(BF16)
            line_z = pick(row_16[:8] - idx_ref[2:3, cols], w_ref[2, :, cols], False)
            sides = [split_bf16(line_y * line_z[z:z + 1]) for z in planes]
            for r in range(len_y // 16):
                hit = tile_y == r
                for k, side in enumerate(sides):
                    first = k * len_y + 16 * r
                    ph_ref[slot, first:first + 16, :] = jnp.where(hit, side[0], zero_16)
                    pl_ref[slot, first:first + 16, :] = jnp.where(hit, side[1], zero_16)
            ghosts = [ghost_y * line_z[z:z + 1] for z in planes]
            if len(planes) % 2:
                ghosts.append(jnp.zeros((8, SUB), F32))
            high, low = split_bf16(jnp.concatenate(ghosts, axis=0))
            top = len(planes) * len_y
            rows = pl.ds(0, top + ghost_rows(group))
            ph_ref[slot, top:top + ghost_rows(group), :] = high
            pl_ref[slot, top:top + ghost_rows(group), :] = low
            if group == 0:
                part = dot3((ph_ref[slot, rows, :], pl_ref[slot, rows, :]), (near_ref[slot, 0], near_ref[slot, 1]), 1)
            else:
                part = dot3((ph_ref[slot, rows, :], pl_ref[slot, rows, :]), (xh_ref[cols, :], xl_ref[cols, :]))
            total = part if total is None else total + part
        acc_refs[group][...] += total

    def transform_send(group):
        planes = GROUPS[group]
        acc_ref, got_ref = acc_refs[group], got_refs[group]
        swap(group).wait()
        sign = (1 - 2 * my_y).astype(F32)
        peak = jnp.full((1, 1), 1e-30, F32)
        for first in range(0, len(planes), 2):
            count = min(2, len(planes) - first)
            for k in range(count):
                block = pl.ds((first + k) * len_y, len_y)
                ghost = pl.ds(len(planes) * len_y + 8 * (first + k), 8)
                even, odd = 2 * k * len_y, (2 * k + 1) * len_y
                grid_ref[pl.ds(even, len_y), :] = acc_ref[block, :] + got_ref[block, :]
                grid_ref[pl.ds(odd, len_y), :] = sign * (acc_ref[block, :] - got_ref[block, :])
                grid_ref[pl.ds(even, 8), :] += acc_ref[ghost, :] + got_ref[ghost, :]
                grid_ref[pl.ds(odd, 8), :] -= sign * (acc_ref[ghost, :] - got_ref[ghost, :])
            size = count * grid_n
            mid_ref[pl.ds(0, size), :] = dot3(split_bf16(grid_ref[pl.ds(0, size), :]), (tx_ref[0], tx_ref[1]))
            for parity in range(2):
                columns = [jnp.concatenate([mid_ref[pl.ds((2 * k + parity) * len_y, len_y), pl.ds(c * half, half)] for c in range(2)], axis=0) for k in range(count)]
                modes = dot3((ty_ref[parity, 0], ty_ref[parity, 1]), split_bf16(jnp.concatenate(columns, axis=1)))
                for block in range(4):
                    for k in range(count):
                        mode_ref[first + k, pl.ds(2 * block + parity, z_devs, stride=8), :] = modes[block * z_devs:(block + 1) * z_devs, k * half:(k + 1) * half]
                peak = jnp.maximum(peak, jnp.max(jnp.abs(modes), keepdims=True))
        power = jnp.ceil(jnp.log2(peak * (1.0 / CODE_MAX)) + 1e-3)
        gain = jnp.exp2(-power)
        for first in range(0, len(planes), 2):
            count = min(2, len(planes) - first)
            scaled = [(mode_ref[first + k] * gain).reshape(z_devs, 8, half) for k in range(count)]
            codes = jnp.round(jnp.concatenate(scaled, axis=1)).astype(jnp.int32).astype(jnp.int16)
            code_refs[group][:, pl.ds(8 * first, 8 * count), :] = codes
        code_refs[group][:, pl.ds(8 * len(planes), 2), :] = jnp.broadcast_to(power.astype(jnp.int32), (z_devs, 2, half)).astype(jnp.int16)

        def start(step):
            send(group, step).start()

        far_first(start)
        recv_refs[group][my_z] = code_refs[group][my_z]

    def await_all(ref, sem):
        pltpu.make_async_copy(ref, ref, sem).wait()

    def await_codes(group):
        await_all(recv_refs[group].at[pl.ds(0, z_devs - 1), used(group)], recv_sem.at[group])

    def decode(group, first, count):
        powers = recv_refs[group][:, pl.ds(8 * len(GROUPS[group]), 2), :].astype(jnp.int32).astype(F32)
        codes = recv_refs[group][:, pl.ds(8 * first, 8 * count), :].astype(jnp.int32).astype(F32)
        return codes * jnp.exp2(powers[:, :1, :])

    def fold(part, planes):
        rows = z_devs * 16
        flat = planes.reshape(rows, half)
        deq_ref[part, pl.ds(16, rows - 16), :] += flat[:rows - 16]
        deq_ref[part, pl.ds(0, 16), :] += flat[rows - 16:]

    def transform_z(part):
        flat = deq_ref.at[part]
        columns = [flat[pl.ds(ky, grid_n, stride=4), :] for ky in range(4)]
        return dot3((tz_ref[part, 0], tz_ref[part, 1]), split_bf16(jnp.concatenate(columns, axis=1)))

    for acc_ref in acc_refs:
        acc_ref[...] = jnp.zeros_like(acc_ref)
    for load in slot_loads(0):
        load.wait()
    for group in range(n_groups):
        @pl.loop(0, slots // CHUNK)
        def _(i):
            if group == 0:
                @pl.when(i == EARLY // CHUNK)
                def _():
                    for load in slot_loads(1):
                        load.wait()

            spread(group, i * CHUNK)
            if group:
                @pl.when(i == STEP_AT[group])
                def _():
                    transform_send(group - 1)

        if group == 0:
            pl.semaphore_wait(barrier, z_devs)
            for load in loads:
                load.wait()
        swap(group).start()
    transform_send(n_groups - 1)

    rows = z_devs * 16
    await_codes(0)
    for part in range(2):
        deq_ref[part] = decode(0, 2 * part, 2).reshape(rows, half)
    await_codes(1)
    fold(0, decode(1, 0, 2))
    zed_ref[...] = transform_z(0)
    zed_ref[...] += transform_z(1)
    await_codes(2)
    message = recv_refs[2][...].astype(jnp.int32).astype(F32)
    late_ref[...] = (message[:, :8] * jnp.exp2(message[:, 8:9])).reshape(z_devs * 8, half)
    row = jnp.zeros((8, half), F32)
    for pair in range(2):
        high, low = split_bf16(jnp.concatenate([late_ref[pl.ds(2 * pair + k, half, stride=4), :] for k in range(2)], axis=1))
        zed = zed_ref[:, pl.ds(pair * grid_n, grid_n)]
        zed += jnp.dot(tl_ref[:, pl.ds(0, grid_n)], jnp.concatenate([high, low], axis=0), preferred_element_type=F32)
        zed += jnp.dot(tl_ref[:, pl.ds(grid_n, half)], high, preferred_element_type=F32)
        power = zed[:grid_n] * zed[:grid_n] + zed[grid_n:] * zed[grid_n:]
        for k in range(2):
            for part in range(2):
                place = pl.ds(4 * part + 2 * pair + k, half, stride=8)
                value = bc_ref[place, :] * power[part * half:(part + 1) * half, k * half:(k + 1) * half].T
                ek_ref[place, :] = value
                row += jnp.sum(value.reshape(half // 8, 8, half), axis=0)
    row_ref[0] = jnp.broadcast_to(jnp.sum(row, axis=0, keepdims=True), (8, half))

    others = rrow_ref.at[pl.ds(0, z_devs - 1), pl.ds(0, 1)]
    pair = pltpu.make_async_remote_copy(src_ref=row_ref.at[0, pl.ds(0, 1)], dst_ref=row_ref.at[1, pl.ds(0, 1)], send_sem=row_sem.at[2], recv_sem=row_sem.at[3], device_id=partner, device_id_type=MESH)
    pair.start()
    pair.wait()
    row_ref[2] = row_ref[0] + row_ref[1]

    def start(step):
        pltpu.make_async_remote_copy(src_ref=row_ref.at[2, pl.ds(0, 1)], dst_ref=rrow_ref.at[my_z, pl.ds(0, 1)], send_sem=row_sem.at[0], recv_sem=row_sem.at[1], device_id={'zdom': chip(step)}, device_id_type=MESH).start()

    far_first(start)
    rrow_ref[my_z, pl.ds(0, 1)] = row_ref[2, pl.ds(0, 1)]
    await_all(others, row_sem.at[1])
    sum_ref[0] = jnp.sum(rrow_ref[:, pl.ds(0, 1), :]) * (0.5 / (grid_n * grid_n * grid_n))
    await_all(others, row_sem.at[0])
    for group in range(n_groups):
        await_all(code_refs[group].at[pl.ds(0, z_devs - 1), used(group)], send_sem.at[group])


def solution(mesh):
    y_devs = mesh.shape['ydom']
    z_devs = mesh.shape['zdom']
    slot_spec = P(('sys', 'ydom', 'zdom'))
    mode_spec = P(('sys', 'ydom'), 'zdom', None)

    def local_energy(charge, real_mask, grid_idx, spline_w, influence):
        grid_n = influence.shape[2]
        slots = charge.shape[0]
        half = grid_n // 2
        n_groups = len(GROUPS)
        table_x, table_y, table_z, late_z = dft_tables(grid_n, y_devs, z_devs)
        any_spec = pl.BlockSpec(memory_space=pl.ANY)
        rows = [len(GROUPS[g]) * (grid_n // y_devs) + ghost_rows(g) for g in range(n_groups)]
        codes = [pltpu.VMEM((z_devs, -(-(8 * len(planes) + 2) // 16) * 16, half), jnp.int16) for planes in GROUPS]
        tiles = jnp.swapaxes(influence.reshape(half, 4, 2, half), 1, 2).reshape(8 * half, half)
        mode_energy, energy = pl.pallas_call(
            functools.partial(energy_kernel, y_devs, z_devs),
            in_specs=[any_spec] * 9,
            out_specs=[pl.BlockSpec(memory_space=pltpu.VMEM), pl.BlockSpec(memory_space=pltpu.SMEM)],
            out_shape=[pltpu.VMEM((8 * half, half), F32), jax.ShapeDtypeStruct((1,), F32)],
            scratch_shapes=[
                pltpu.VMEM((1, slots), F32), pltpu.VMEM((1, slots), jnp.int32), pltpu.VMEM((3, slots), jnp.int32), pltpu.VMEM((3, 4, slots), F32),
                pltpu.VMEM((2, 2, grid_n, SUB), BF16), pltpu.VMEM((slots, grid_n), BF16), pltpu.VMEM((slots, grid_n), BF16),
                pltpu.VMEM((2, rows[0], SUB), BF16), pltpu.VMEM((2, rows[0], SUB), BF16),
                [pltpu.VMEM((r, grid_n), F32) for r in rows], [pltpu.VMEM((r, grid_n), F32) for r in rows],
                pltpu.VMEM((2 * grid_n, grid_n), F32), pltpu.VMEM((2 * grid_n, grid_n), F32), pltpu.VMEM((4, 2 * grid_n, half), F32),
                codes, codes,
                pltpu.VMEM((2, z_devs * 16, half), F32), pltpu.VMEM((2 * grid_n, 4 * half), F32),
                pltpu.VMEM((8 * half, half), F32),
                pltpu.VMEM(table_x.shape[1:], BF16), pltpu.VMEM(table_y.shape, BF16), pltpu.VMEM(table_z.shape, BF16), pltpu.VMEM(late_z.shape, BF16),
                pltpu.VMEM((z_devs * 8, half), F32),
                pltpu.VMEM((3, 8, 128), F32), pltpu.VMEM((z_devs, 8, 128), F32),
                pltpu.SemaphoreType.DMA((2, 4)), pltpu.SemaphoreType.DMA((5,)), pltpu.SemaphoreType.DMA((2, n_groups)),
                pltpu.SemaphoreType.DMA((n_groups,)), pltpu.SemaphoreType.DMA((n_groups,)),
                pltpu.SemaphoreType.DMA((4,)),
            ],
            compiler_params=pltpu.CompilerParams(collective_id=0, has_side_effects=True, vmem_limit_bytes=60 * 1024 * 1024),
            name="energy",
        )(charge.reshape(1, slots), real_mask.reshape(1, slots), grid_idx.T, jnp.transpose(spline_w, (1, 2, 0)), tiles, jnp.asarray(table_x), jnp.asarray(table_y), jnp.asarray(table_z), jnp.asarray(late_z))
        mode_energy = lax.optimization_barrier(0.5 * mode_energy)
        return jnp.swapaxes(mode_energy.reshape(half, 2, 4, half), 1, 2).reshape(influence.shape), energy

    return jax.shard_map(local_energy, mesh=mesh, in_specs=(slot_spec, slot_spec, P(('sys', 'ydom', 'zdom'), None), P(('sys', 'ydom', 'zdom'), None, None), mode_spec), out_specs=(mode_spec, P('sys')), check_vma=False)
```

```python
import functools
import math
import jax
import jax.numpy as jnp
import numpy as np
from jax import lax
from jax.experimental import pallas as pl
from jax.experimental.pallas import tpu as pltpu
from jax.sharding import PartitionSpec as P

F32 = jnp.float32
BF16 = jnp.bfloat16
SUB = 512
CHUNK = 2048
GROUPS = ((0, 1, 2, 3), (4, 5), (6,))
STEP_AT = (0, 2, 2)
EARLY = 2048
CODE_MAX = 32767.0
MESH = pl.DeviceIdType.MESH


def split_bf16(value):
    high = value.astype(BF16)
    return high, (value - high.astype(F32)).astype(BF16)


def dot3(lhs, rhs, rhs_dim=0):
    def dot(a, b):
        return lax.dot_general(a, b, (((1,), (rhs_dim,)), ((), ())), preferred_element_type=F32)
    return dot(lhs[0], rhs[0]) + dot(lhs[1], rhs[0]) + dot(lhs[0], rhs[1])


def pick(ahead, taps, wrap=True):
    place = ahead & 15 if wrap else ahead
    value = jnp.zeros(ahead.shape, F32)
    for t in range(4):
        value = jnp.where(place == t, taps[t:t + 1], value)
    return value


def np_split(value):
    value = np.asarray(value, np.float32)
    high = value.astype(BF16)
    return np.stack([high, (value - high.astype(np.float32)).astype(BF16)])


def dft_tables(grid_n, y_devs, z_devs):
    turn = 2.0 * np.pi / grid_n
    len_y, len_z = grid_n // y_devs, grid_n // z_devs
    x = np.arange(grid_n)
    freq = np.arange(grid_n)
    phase_x = (np.outer(x, freq) % grid_n) * turn
    table_x = np.stack([np_split(np.concatenate([np.cos(phase_x[:, i * len_y:(i + 1) * len_y]), -np.sin(phase_x[:, i * len_y:(i + 1) * len_y])], axis=1)) for i in range(y_devs)])
    table_y = []
    for parity in range(2):
        ky = (np.arange(z_devs)[None, :] * len_z + 2 * np.arange(2)[:, None] + parity).reshape(-1)
        phase_y = (np.outer(ky, np.arange(grid_n // 2)) % grid_n) * turn
        real = np.concatenate([np.cos(phase_y), np.sin(phase_y)], axis=1)
        imag = np.concatenate([-np.sin(phase_y), np.cos(phase_y)], axis=1)
        table_y.append(np_split(np.concatenate([real, imag], axis=0)))

    def z_table(first, count):
        pos = np.arange(z_devs)[:, None] * len_z + first + np.arange(count)[None, :]
        phase_z = ((freq[:, None, None] * pos[None]) % grid_n) * turn
        real = np.stack([np.cos(phase_z), np.sin(phase_z)], axis=3).reshape(grid_n, -1)
        imag = np.stack([-np.sin(phase_z), np.cos(phase_z)], axis=3).reshape(grid_n, -1)
        return np_split(np.concatenate([real, imag], axis=0))

    high, low = z_table(6, 1)
    late_z = np.concatenate([high, high, low], axis=1)
    return table_x, np.stack(table_y), np.stack([z_table(0, 2), z_table(2, 2)]), late_z


def ghost_rows(group):
    return -(-8 * len(GROUPS[group]) // 16) * 16


def energy_kernel(y_devs, z_devs, q_hbm, m_hbm, idx_hbm, w_hbm, bc_hbm, tx_hbm, ty_hbm, tz_hbm, tl_hbm, ek_ref, sum_ref,
                  q_ref, m_ref, idx_ref, w_ref, line_ref, near_ref, xh_ref, xl_ref, ph_ref, pl_ref, acc_refs, got_refs, grid_ref, mid_ref, mode_ref,
                  code_refs, recv_refs,
                  deq_ref, zed_ref, bc_ref, tx_ref, ty_ref, tz_ref, tl_ref, late_ref, row_ref, rrow_ref,
                  early_sem, load_sem, swap_sem, send_sem, recv_sem, row_sem):
    my_y = lax.axis_index('ydom')
    my_z = lax.axis_index('zdom')
    grid_n = xh_ref.shape[1]
    slots = q_ref.shape[1]
    len_y = grid_n // y_devs
    half = grid_n // 2
    n_groups = len(GROUPS)
    barrier = pltpu.get_barrier_semaphore()
    partner = {'ydom': 1 - my_y}

    def chip(step):
        return (my_z + step) & (z_devs - 1)

    def chips_from_far():
        side = round(z_devs ** (1 / 3))
        place = [my_z // side ** axis % side for axis in range(3)]
        there = [[(place[axis] + d) % side * side ** axis for d in range(side)] for axis in range(3)]
        steps = [(a, b, c) for c in range(side) for b in range(side) for a in range(side)][1:]
        steps.sort(key=lambda step: -sum(min(d, side - d) for d in step))
        return [there[0][a] + there[1][b] + there[2][c] for a, b, c in steps]

    def slot_loads(piece):
        cols = pl.ds(0, EARLY) if piece == 0 else pl.ds(EARLY, slots - EARLY)
        return [pltpu.make_async_copy(hbm.at[lead + (cols,)], ref.at[lead + (cols,)], early_sem.at[piece, k])
                for k, (hbm, ref, lead) in enumerate(((q_hbm, q_ref, (slice(None),)), (m_hbm, m_ref, (slice(None),)), (idx_hbm, idx_ref, (slice(None),)), (w_hbm, w_ref, (slice(None), slice(None)))))]

    for piece in range(2):
        for load in slot_loads(piece):
            load.start()

    @pl.loop(1, z_devs)
    def _(step):
        pl.semaphore_signal(barrier, inc=1, device_id={'zdom': chip(step)}, device_id_type=MESH)

    pl.semaphore_signal(barrier, inc=1, device_id=partner, device_id_type=MESH)

    loads = [pltpu.make_async_copy(tx_hbm.at[my_y], tx_ref, load_sem.at[0]), pltpu.make_async_copy(ty_hbm, ty_ref, load_sem.at[1]),
             pltpu.make_async_copy(tz_hbm, tz_ref, load_sem.at[2]), pltpu.make_async_copy(bc_hbm, bc_ref, load_sem.at[3]), pltpu.make_async_copy(tl_hbm, tl_ref, load_sem.at[4])]
    for load in loads:
        load.start()

    def swap(group):
        return pltpu.make_async_remote_copy(src_ref=acc_refs[group], dst_ref=got_refs[group], send_sem=swap_sem.at[0, group], recv_sem=swap_sem.at[1, group], device_id=partner, device_id_type=MESH)

    def used(group):
        return pl.ds(0, 8 * len(GROUPS[group]) + 2)

    def send(group, other):
        return pltpu.make_async_remote_copy(src_ref=code_refs[group].at[other, used(group)], dst_ref=recv_refs[group].at[my_z, used(group)], send_sem=send_sem.at[group], recv_sem=recv_sem.at[group], device_id={'zdom': other}, device_id_type=MESH)

    def spread(group, base):
        planes = GROUPS[group]
        zero_16 = jnp.zeros((16, SUB), BF16)
        total = None
        for sub in range(CHUNK // SUB):
            slot = sub % 2
            cols = pl.ds(pl.multiple_of(base + sub * SUB, SUB), SUB)
            row_16 = lax.broadcasted_iota(jnp.int32, (16, SUB), 0)
            if group == 0:
                weight = q_ref[:, cols] * m_ref[:, cols].astype(F32)
                ahead = row_16 - idx_ref[0:1, cols]
                taps = w_ref[0, :, cols] * weight
                high, low = split_bf16(pick(ahead, taps))
                tile_x = (-(ahead >> 4) & 15).astype(F32).astype(BF16)
                for r in range(grid_n // 16):
                    hit = tile_x == r
                    line_ref[0, 16 * r:16 * r + 16, :] = jnp.where(hit, high, zero_16)
                    line_ref[1, 16 * r:16 * r + 16, :] = jnp.where(hit, low, zero_16)
                for part, far_ref in enumerate((xh_ref, xl_ref)):
                    turned = line_ref[part].T
                    near_ref[slot, part] = turned
                    far_ref[cols, :] = turned
            ahead = row_16 - idx_ref[1:2, cols]
            line_y = pick(ahead, w_ref[1, :, cols])
            tile = -(ahead >> 4)
            ghost_y = jnp.where(tile[:8] == len_y // 16, line_y[:8], 0.0)
            tile_y = tile.astype(F32).astype(BF16)
            line_z = pick(row_16[:8] - idx_ref[2:3, cols], w_ref[2, :, cols], False)
            sides = [split_bf16(line_y * line_z[z:z + 1]) for z in planes]
            for r in range(len_y // 16):
                hit = tile_y == r
                for k, side in enumerate(sides):
                    first = k * len_y + 16 * r
                    ph_ref[slot, first:first + 16, :] = jnp.where(hit, side[0], zero_16)
                    pl_ref[slot, first:first + 16, :] = jnp.where(hit, side[1], zero_16)
            ghosts = [ghost_y * line_z[z:z + 1] for z in planes]
            if len(planes) % 2:
                ghosts.append(jnp.zeros((8, SUB), F32))
            high, low = split_bf16(jnp.concatenate(ghosts, axis=0))
            top = len(planes) * len_y
            rows = pl.ds(0, top + ghost_rows(group))
            ph_ref[slot, top:top + ghost_rows(group), :] = high
            pl_ref[slot, top:top + ghost_rows(group), :] = low
            if group == 0:
                part = dot3((ph_ref[slot, rows, :], pl_ref[slot, rows, :]), (near_ref[slot, 0], near_ref[slot, 1]))
            else:
                part = dot3((ph_ref[slot, rows, :], pl_ref[slot, rows, :]), (xh_ref[cols, :], xl_ref[cols, :]))
            total = part if total is None else total + part
        acc_refs[group][...] += total

    def transform_send(group):
        planes = GROUPS[group]
        acc_ref, got_ref = acc_refs[group], got_refs[group]
        swap(group).wait()
        sign = (1 - 2 * my_y).astype(F32)
        peak = jnp.full((1, 1), 1e-30, F32)
        for first in range(0, len(planes), 2):
            count = min(2, len(planes) - first)
            for k in range(count):
                block = pl.ds((first + k) * len_y, len_y)
                ghost = pl.ds(len(planes) * len_y + 8 * (first + k), 8)
                even, odd = 2 * k * len_y, (2 * k + 1) * len_y
                grid_ref[first // 2, pl.ds(even, len_y), :] = acc_ref[block, :] + got_ref[block, :]
                grid_ref[first // 2, pl.ds(odd, len_y), :] = sign * (acc_ref[block, :] - got_ref[block, :])
                grid_ref[first // 2, pl.ds(even, 8), :] += acc_ref[ghost, :] + got_ref[ghost, :]
                grid_ref[first // 2, pl.ds(odd, 8), :] -= sign * (acc_ref[ghost, :] - got_ref[ghost, :])
            size = count * grid_n
            mid_ref[first // 2, pl.ds(0, size), :] = dot3(split_bf16(grid_ref[first // 2, pl.ds(0, size), :]), (tx_ref[0], tx_ref[1]))
            for parity in range(2):
                columns = [jnp.concatenate([mid_ref[first // 2, pl.ds((2 * k + parity) * len_y, len_y), pl.ds(c * half, half)] for c in range(2)], axis=0) for k in range(count)]
                modes = dot3((ty_ref[parity, 0], ty_ref[parity, 1]), split_bf16(jnp.concatenate(columns, axis=1)))
                for block in range(4):
                    for k in range(count):
                        mode_ref[first + k, pl.ds(2 * block + parity, z_devs, stride=8), :] = modes[block * z_devs:(block + 1) * z_devs, k * half:(k + 1) * half]
                peak = jnp.maximum(peak, jnp.max(jnp.abs(modes), keepdims=True))
        power = jnp.ceil(jnp.log2(peak * (1.0 / CODE_MAX)) + 1e-3)
        gain = jnp.exp2(-power)
        for first in range(0, len(planes), 2):
            count = min(2, len(planes) - first)
            scaled = [(mode_ref[first + k] * gain).reshape(z_devs, 8, half) for k in range(count)]
            codes = jnp.round(jnp.concatenate(scaled, axis=1)).astype(jnp.int32).astype(jnp.int16)
            code_refs[group][:, pl.ds(8 * first, 8 * count), :] = codes
        code_refs[group][:, pl.ds(8 * len(planes), 2), :] = jnp.broadcast_to(power.astype(jnp.int32), (z_devs, 2, half)).astype(jnp.int16)

        if group < n_groups - 1:
            @pl.loop(1, z_devs)
            def _(step):
                send(group, chip(step)).start()
        else:
            for other in chips_from_far():
                send(group, other).start()
        recv_refs[group][my_z] = code_refs[group][my_z]

    def await_all(ref, sem):
        pltpu.make_async_copy(ref, ref, sem).wait()

    def await_codes(group):
        await_all(recv_refs[group].at[pl.ds(0, z_devs - 1), used(group)], recv_sem.at[group])

    def decode(group, first, count):
        powers = recv_refs[group][:, pl.ds(8 * len(GROUPS[group]), 2), :].astype(jnp.int32).astype(F32)
        codes = recv_refs[group][:, pl.ds(8 * first, 8 * count), :].astype(jnp.int32).astype(F32)
        return codes * jnp.exp2(powers[:, :1, :])

    def fold(part, planes):
        rows = z_devs * 16
        flat = planes.reshape(rows, half)
        deq_ref[part, pl.ds(16, rows - 16), :] += flat[:rows - 16]
        deq_ref[part, pl.ds(0, 16), :] += flat[rows - 16:]

    def transform_z(part):
        flat = deq_ref.at[part]
        columns = [flat[pl.ds(ky, grid_n, stride=4), :] for ky in range(4)]
        return dot3((tz_ref[part, 0], tz_ref[part, 1]), split_bf16(jnp.concatenate(columns, axis=1)))

    for acc_ref in acc_refs:
        acc_ref[...] = jnp.zeros_like(acc_ref)
    for load in slot_loads(0):
        load.wait()
    for group in range(n_groups):
        @pl.loop(0, slots // CHUNK)
        def _(i):
            if group == 0:
                @pl.when(i == EARLY // CHUNK)
                def _():
                    for load in slot_loads(1):
                        load.wait()

            spread(group, i * CHUNK)
            if group:
                @pl.when(i == STEP_AT[group])
                def _():
                    transform_send(group - 1)

        if group == 0:
            pl.semaphore_wait(barrier, z_devs)
            for load in loads:
                load.wait()
        swap(group).start()
    transform_send(n_groups - 1)

    rows = z_devs * 16
    await_codes(0)
    for part in range(2):
        deq_ref[part] = decode(0, 2 * part, 2).reshape(rows, half)
    await_codes(1)
    fold(0, decode(1, 0, 2))
    zed_ref[...] = transform_z(0)
    zed_ref[...] += transform_z(1)
    await_codes(2)
    message = recv_refs[2][...].astype(jnp.int32).astype(F32)
    late_ref[...] = (message[:, :8] * jnp.exp2(message[:, 8:9])).reshape(z_devs * 8, half)
    row = jnp.zeros((8, half), F32)
    for pair in range(2):
        high, low = split_bf16(jnp.concatenate([late_ref[pl.ds(2 * pair + k, half, stride=4), :] for k in range(2)], axis=1))
        zed = zed_ref[:, pl.ds(pair * grid_n, grid_n)]
        zed += jnp.dot(tl_ref[:, pl.ds(0, grid_n)], jnp.concatenate([high, low], axis=0), preferred_element_type=F32)
        zed += jnp.dot(tl_ref[:, pl.ds(grid_n, half)], high, preferred_element_type=F32)
        power = zed[:grid_n] * zed[:grid_n] + zed[grid_n:] * zed[grid_n:]
        for k in range(2):
            for part in range(2):
                place = pl.ds(4 * part + 2 * pair + k, half, stride=8)
                value = bc_ref[place, :] * power[part * half:(part + 1) * half, k * half:(k + 1) * half].T
                ek_ref[place, :] = value
                row += jnp.sum(value.reshape(half // 8, 8, half), axis=0)
    row_ref[0] = jnp.broadcast_to(jnp.sum(row, axis=0, keepdims=True), (8, half))

    others = rrow_ref.at[pl.ds(0, z_devs - 1), pl.ds(0, 1)]
    pair = pltpu.make_async_remote_copy(src_ref=row_ref.at[0, pl.ds(0, 1)], dst_ref=row_ref.at[1, pl.ds(0, 1)], send_sem=row_sem.at[2], recv_sem=row_sem.at[3], device_id=partner, device_id_type=MESH)
    pair.start()
    pair.wait()
    row_ref[2] = row_ref[0] + row_ref[1]

    for other in chips_from_far():
        pltpu.make_async_remote_copy(src_ref=row_ref.at[2, pl.ds(0, 1)], dst_ref=rrow_ref.at[my_z, pl.ds(0, 1)], send_sem=row_sem.at[0], recv_sem=row_sem.at[1], device_id={'zdom': other}, device_id_type=MESH).start()

    rrow_ref[my_z, pl.ds(0, 1)] = row_ref[2, pl.ds(0, 1)]
    await_all(others, row_sem.at[1])
    sum_ref[0] = jnp.sum(rrow_ref[:, pl.ds(0, 1), :]) * (0.5 / (grid_n * grid_n * grid_n))
    await_all(others, row_sem.at[0])
    for group in range(n_groups):
        await_all(code_refs[group].at[pl.ds(0, z_devs - 1), used(group)], send_sem.at[group])


def solution(mesh):
    y_devs = mesh.shape['ydom']
    z_devs = mesh.shape['zdom']
    slot_spec = P(('sys', 'ydom', 'zdom'))
    mode_spec = P(('sys', 'ydom'), 'zdom', None)

    def local_energy(charge, real_mask, grid_idx, spline_w, influence):
        grid_n = influence.shape[2]
        slots = charge.shape[0]
        half = grid_n // 2
        n_groups = len(GROUPS)
        table_x, table_y, table_z, late_z = dft_tables(grid_n, y_devs, z_devs)
        any_spec = pl.BlockSpec(memory_space=pl.ANY)
        rows = [len(GROUPS[g]) * (grid_n // y_devs) + ghost_rows(g) for g in range(n_groups)]
        codes = [pltpu.VMEM((z_devs, -(-(8 * len(planes) + 2) // 16) * 16, half), jnp.int16) for planes in GROUPS]
        tiles = jnp.swapaxes(influence.reshape(half, 4, 2, half), 1, 2).reshape(8 * half, half)
        mode_energy, energy = pl.pallas_call(
            functools.partial(energy_kernel, y_devs, z_devs),
            in_specs=[any_spec] * 9,
            out_specs=[pl.BlockSpec(memory_space=pltpu.VMEM), pl.BlockSpec(memory_space=pltpu.SMEM)],
            out_shape=[pltpu.VMEM((8 * half, half), F32), jax.ShapeDtypeStruct((1,), F32)],
            scratch_shapes=[
                pltpu.VMEM((1, slots), F32), pltpu.VMEM((1, slots), jnp.int32), pltpu.VMEM((3, slots), jnp.int32), pltpu.VMEM((3, 4, slots), F32),
                pltpu.VMEM((2, grid_n, SUB), BF16), pltpu.VMEM((2, 2, SUB, grid_n), BF16), pltpu.VMEM((slots, grid_n), BF16), pltpu.VMEM((slots, grid_n), BF16),
                pltpu.VMEM((2, rows[0], SUB), BF16), pltpu.VMEM((2, rows[0], SUB), BF16),
                [pltpu.VMEM((r, grid_n), F32) for r in rows], [pltpu.VMEM((r, grid_n), F32) for r in rows],
                pltpu.VMEM((2, 2 * grid_n, grid_n), F32), pltpu.VMEM((2, 2 * grid_n, grid_n), F32), pltpu.VMEM((4, 2 * grid_n, half), F32),
                codes, codes,
                pltpu.VMEM((2, z_devs * 16, half), F32), pltpu.VMEM((2 * grid_n, 4 * half), F32),
                pltpu.VMEM((8 * half, half), F32),
                pltpu.VMEM(table_x.shape[1:], BF16), pltpu.VMEM(table_y.shape, BF16), pltpu.VMEM(table_z.shape, BF16), pltpu.VMEM(late_z.shape, BF16),
                pltpu.VMEM((z_devs * 8, half), F32),
                pltpu.VMEM((3, 8, 128), F32), pltpu.VMEM((z_devs, 8, 128), F32),
                pltpu.SemaphoreType.DMA((2, 4)), pltpu.SemaphoreType.DMA((5,)), pltpu.SemaphoreType.DMA((2, n_groups)),
                pltpu.SemaphoreType.DMA((n_groups,)), pltpu.SemaphoreType.DMA((n_groups,)),
                pltpu.SemaphoreType.DMA((4,)),
            ],
            compiler_params=pltpu.CompilerParams(collective_id=0, has_side_effects=True, vmem_limit_bytes=60 * 1024 * 1024),
            name="energy",
        )(charge.reshape(1, slots), real_mask.reshape(1, slots), grid_idx.T, jnp.transpose(spline_w, (1, 2, 0)), tiles, jnp.asarray(table_x), jnp.asarray(table_y), jnp.asarray(table_z), jnp.asarray(late_z))
        mode_energy = lax.optimization_barrier(0.5 * mode_energy)
        return jnp.swapaxes(mode_energy.reshape(half, 2, 4, half), 1, 2).reshape(influence.shape), energy

    return jax.shard_map(local_energy, mesh=mesh, in_specs=(slot_spec, slot_spec, P(('sys', 'ydom', 'zdom'), None), P(('sys', 'ydom', 'zdom'), None, None), mode_spec), out_specs=(mode_spec, P('sys')), check_vma=False)
```

```python
import functools
import math
import jax
import jax.numpy as jnp
import numpy as np
from jax import lax
from jax.experimental import pallas as pl
from jax.experimental.pallas import tpu as pltpu
from jax.sharding import PartitionSpec as P

F32 = jnp.float32
BF16 = jnp.bfloat16
SUB = 512
CHUNK = 2048
GROUPS = ((0, 1, 2, 3), (4, 5), (6,))
STEP_AT = (0, 2, 3)
EARLY = 2048
CODE_MAX = 32767.0
MESH = pl.DeviceIdType.MESH


def split_bf16(value):
    high = value.astype(BF16)
    return high, (value - high.astype(F32)).astype(BF16)


def dot3(lhs, rhs, rhs_dim=0):
    def dot(a, b):
        return lax.dot_general(a, b, (((1,), (rhs_dim,)), ((), ())), preferred_element_type=F32)
    return dot(lhs[0], rhs[0]) + dot(lhs[1], rhs[0]) + dot(lhs[0], rhs[1])


def pick(ahead, taps, wrap=True):
    place = ahead & 15 if wrap else ahead
    value = jnp.zeros(ahead.shape, F32)
    for t in range(4):
        value = jnp.where(place == t, taps[t:t + 1], value)
    return value


def np_split(value):
    value = np.asarray(value, np.float32)
    high = value.astype(BF16)
    return np.stack([high, (value - high.astype(np.float32)).astype(BF16)])


def dft_tables(grid_n, y_devs, z_devs):
    turn = 2.0 * np.pi / grid_n
    len_y, len_z = grid_n // y_devs, grid_n // z_devs
    x = np.arange(grid_n)
    freq = np.arange(grid_n)
    phase_x = (np.outer(x, freq) % grid_n) * turn
    table_x = np.stack([np_split(np.concatenate([np.cos(phase_x[:, i * len_y:(i + 1) * len_y]), -np.sin(phase_x[:, i * len_y:(i + 1) * len_y])], axis=1)) for i in range(y_devs)])
    table_y = []
    for parity in range(2):
        ky = (np.arange(z_devs)[None, :] * len_z + 2 * np.arange(2)[:, None] + parity).reshape(-1)
        phase_y = (np.outer(ky, np.arange(grid_n // 2)) % grid_n) * turn
        real = np.concatenate([np.cos(phase_y), np.sin(phase_y)], axis=1)
        imag = np.concatenate([-np.sin(phase_y), np.cos(phase_y)], axis=1)
        table_y.append(np_split(np.concatenate([real, imag], axis=0)))

    def z_table(first, count):
        pos = np.arange(z_devs)[:, None] * len_z + first + np.arange(count)[None, :]
        phase_z = ((freq[:, None, None] * pos[None]) % grid_n) * turn
        real = np.stack([np.cos(phase_z), np.sin(phase_z)], axis=3).reshape(grid_n, -1)
        imag = np.stack([-np.sin(phase_z), np.cos(phase_z)], axis=3).reshape(grid_n, -1)
        return np_split(np.concatenate([real, imag], axis=0))

    high, low = z_table(6, 1)
    late_z = np.concatenate([high, high, low], axis=1)
    return table_x, np.stack(table_y), np.stack([z_table(0, 2), z_table(2, 2)]), late_z


def ghost_rows(group):
    return -(-8 * len(GROUPS[group]) // 16) * 16


def energy_kernel(y_devs, z_devs, q_hbm, m_hbm, idx_hbm, w_hbm, bc_hbm, tx_hbm, ty_hbm, tz_hbm, tl_hbm, ek_ref, sum_ref,
                  q_ref, m_ref, idx_ref, w_ref, line_ref, near_ref, xh_ref, xl_ref, ph_ref, pl_ref, acc_refs, got_refs, grid_ref, mid_ref, mode_ref,
                  code_refs, recv_refs,
                  deq_ref, zed_ref, bc_ref, tx_ref, ty_ref, tz_ref, tl_ref, late_ref, row_ref, rrow_ref,
                  early_sem, load_sem, swap_sem, send_sem, recv_sem, row_sem):
    my_y = lax.axis_index('ydom')
    my_z = lax.axis_index('zdom')
    grid_n = xh_ref.shape[1]
    slots = q_ref.shape[1]
    len_y = grid_n // y_devs
    half = grid_n // 2
    n_groups = len(GROUPS)
    barrier = pltpu.get_barrier_semaphore()
    partner = {'ydom': 1 - my_y}

    def chip(step):
        return (my_z + step) & (z_devs - 1)

    def to_chips(start):
        pl.loop(1, z_devs)(start)

    def slot_loads(piece):
        cols = pl.ds(0, EARLY) if piece == 0 else pl.ds(EARLY, slots - EARLY)
        return [pltpu.make_async_copy(hbm.at[lead + (cols,)], ref.at[lead + (cols,)], early_sem.at[piece, k])
                for k, (hbm, ref, lead) in enumerate(((q_hbm, q_ref, (slice(None),)), (m_hbm, m_ref, (slice(None),)), (idx_hbm, idx_ref, (slice(None),)), (w_hbm, w_ref, (slice(None), slice(None)))))]

    for piece in range(2):
        for load in slot_loads(piece):
            load.start()

    @pl.loop(1, z_devs)
    def _(step):
        pl.semaphore_signal(barrier, inc=1, device_id={'zdom': chip(step)}, device_id_type=MESH)

    pl.semaphore_signal(barrier, inc=1, device_id=partner, device_id_type=MESH)

    loads = [pltpu.make_async_copy(tx_hbm.at[my_y], tx_ref, load_sem.at[0]), pltpu.make_async_copy(ty_hbm, ty_ref, load_sem.at[1]),
             pltpu.make_async_copy(tz_hbm, tz_ref, load_sem.at[2]), pltpu.make_async_copy(bc_hbm, bc_ref, load_sem.at[3]), pltpu.make_async_copy(tl_hbm, tl_ref, load_sem.at[4])]
    for load in loads:
        load.start()

    def swap(group):
        return pltpu.make_async_remote_copy(src_ref=acc_refs[group], dst_ref=got_refs[group], send_sem=swap_sem.at[0, group], recv_sem=swap_sem.at[1, group], device_id=partner, device_id_type=MESH)

    def used(group):
        return pl.ds(0, 8 * len(GROUPS[group]) + 2)

    def send(group, step):
        other = chip(step)
        return pltpu.make_async_remote_copy(src_ref=code_refs[group].at[other, used(group)], dst_ref=recv_refs[group].at[my_z, used(group)], send_sem=send_sem.at[group], recv_sem=recv_sem.at[group], device_id={'zdom': other}, device_id_type=MESH)

    def spread(group, base):
        planes = GROUPS[group]
        zero_16 = jnp.zeros((16, SUB), BF16)
        total = None
        for sub in range(CHUNK // SUB):
            slot = sub % 2
            cols = pl.ds(pl.multiple_of(base + sub * SUB, SUB), SUB)
            row_16 = lax.broadcasted_iota(jnp.int32, (16, SUB), 0)
            if group == 0:
                weight = q_ref[:, cols] * m_ref[:, cols].astype(F32)
                ahead = row_16 - idx_ref[0:1, cols]
                taps = w_ref[0, :, cols] * weight
                high, low = split_bf16(pick(ahead, taps))
                tile_x = (-(ahead >> 4) & 15).astype(F32).astype(BF16)
                for r in range(grid_n // 16):
                    hit = tile_x == r
                    line_ref[0, 16 * r:16 * r + 16, :] = jnp.where(hit, high, zero_16)
                    line_ref[1, 16 * r:16 * r + 16, :] = jnp.where(hit, low, zero_16)
                for part, far_ref in enumerate((xh_ref, xl_ref)):
                    turned = line_ref[part].T
                    near_ref[slot, part] = turned
                    far_ref[cols, :] = turned
            ahead = row_16 - idx_ref[1:2, cols]
            line_y = pick(ahead, w_ref[1, :, cols])
            tile = -(ahead >> 4)
            ghost_y = jnp.where(tile[:8] == len_y // 16, line_y[:8], 0.0)
            tile_y = tile.astype(F32).astype(BF16)
            line_z = pick(row_16[:8] - idx_ref[2:3, cols], w_ref[2, :, cols], False)
            sides = [split_bf16(line_y * line_z[z:z + 1]) for z in planes]
            for r in range(len_y // 16):
                hit = tile_y == r
                for k, side in enumerate(sides):
                    first = k * len_y + 16 * r
                    ph_ref[slot, first:first + 16, :] = jnp.where(hit, side[0], zero_16)
                    pl_ref[slot, first:first + 16, :] = jnp.where(hit, side[1], zero_16)
            ghosts = [ghost_y * line_z[z:z + 1] for z in planes]
            if len(planes) % 2:
                ghosts.append(jnp.zeros((8, SUB), F32))
            high, low = split_bf16(jnp.concatenate(ghosts, axis=0))
            top = len(planes) * len_y
            rows = pl.ds(0, top + ghost_rows(group))
            ph_ref[slot, top:top + ghost_rows(group), :] = high
            pl_ref[slot, top:top + ghost_rows(group), :] = low
            if group == 0:
                part = dot3((ph_ref[slot, rows, :], pl_ref[slot, rows, :]), (near_ref[slot, 0], near_ref[slot, 1]))
            else:
                part = dot3((ph_ref[slot, rows, :], pl_ref[slot, rows, :]), (xh_ref[cols, :], xl_ref[cols, :]))
            total = part if total is None else total + part
        acc_refs[group][...] += total

    def transform_send(group):
        planes = GROUPS[group]
        acc_ref, got_ref = acc_refs[group], got_refs[group]
        swap(group).wait()
        sign = (1 - 2 * my_y).astype(F32)
        peak = jnp.full((1, 1), 1e-30, F32)
        for first in range(0, len(planes), 2):
            count = min(2, len(planes) - first)
            for k in range(count):
                block = pl.ds((first + k) * len_y, len_y)
                ghost = pl.ds(len(planes) * len_y + 8 * (first + k), 8)
                even, odd = 2 * k * len_y, (2 * k + 1) * len_y
                grid_ref[first // 2, pl.ds(even, len_y), :] = acc_ref[block, :] + got_ref[block, :]
                grid_ref[first // 2, pl.ds(odd, len_y), :] = sign * (acc_ref[block, :] - got_ref[block, :])
                grid_ref[first // 2, pl.ds(even, 8), :] += acc_ref[ghost, :] + got_ref[ghost, :]
                grid_ref[first // 2, pl.ds(odd, 8), :] -= sign * (acc_ref[ghost, :] - got_ref[ghost, :])
            size = count * grid_n
            mid_ref[first // 2, pl.ds(0, size), :] = dot3(split_bf16(grid_ref[first // 2, pl.ds(0, size), :]), (tx_ref[0], tx_ref[1]))
            for parity in range(2):
                columns = [jnp.concatenate([mid_ref[first // 2, pl.ds((2 * k + parity) * len_y, len_y), pl.ds(c * half, half)] for c in range(2)], axis=0) for k in range(count)]
                modes = dot3((ty_ref[parity, 0], ty_ref[parity, 1]), split_bf16(jnp.concatenate(columns, axis=1)))
                for block in range(4):
                    for k in range(count):
                        mode_ref[first + k, pl.ds(2 * block + parity, z_devs, stride=8), :] = modes[block * z_devs:(block + 1) * z_devs, k * half:(k + 1) * half]
                peak = jnp.maximum(peak, jnp.max(jnp.abs(modes), keepdims=True))
        power = jnp.ceil(jnp.log2(peak * (1.0 / CODE_MAX)) + 1e-3)
        gain = jnp.exp2(-power)
        for first in range(0, len(planes), 2):
            count = min(2, len(planes) - first)
            scaled = [(mode_ref[first + k] * gain).reshape(z_devs, 8, half) for k in range(count)]
            codes = jnp.round(jnp.concatenate(scaled, axis=1)).astype(jnp.int32).astype(jnp.int16)
            code_refs[group][:, pl.ds(8 * first, 8 * count), :] = codes
        code_refs[group][:, pl.ds(8 * len(planes), 2), :] = jnp.broadcast_to(power.astype(jnp.int32), (z_devs, 2, half)).astype(jnp.int16)

        def start(step):
            send(group, step).start()

        to_chips(start)
        recv_refs[group][my_z] = code_refs[group][my_z]

    def await_all(ref, sem):
        pltpu.make_async_copy(ref, ref, sem).wait()

    def await_codes(group):
        await_all(recv_refs[group].at[pl.ds(0, z_devs - 1), used(group)], recv_sem.at[group])

    def decode(group, first, count):
        powers = recv_refs[group][:, pl.ds(8 * len(GROUPS[group]), 2), :].astype(jnp.int32).astype(F32)
        codes = recv_refs[group][:, pl.ds(8 * first, 8 * count), :].astype(jnp.int32).astype(F32)
        return codes * jnp.exp2(powers[:, :1, :])

    def fold(part, planes):
        rows = z_devs * 16
        flat = planes.reshape(rows, half)
        deq_ref[part, pl.ds(16, rows - 16), :] += flat[:rows - 16]
        deq_ref[part, pl.ds(0, 16), :] += flat[rows - 16:]

    def transform_z(part):
        flat = deq_ref.at[part]
        columns = [flat[pl.ds(ky, grid_n, stride=4), :] for ky in range(4)]
        return dot3((tz_ref[part, 0], tz_ref[part, 1]), split_bf16(jnp.concatenate(columns, axis=1)))

    for acc_ref in acc_refs:
        acc_ref[...] = jnp.zeros_like(acc_ref)
    for load in slot_loads(0):
        load.wait()
    for group in range(n_groups):
        @pl.loop(0, slots // CHUNK)
        def _(i):
            if group == 0:
                @pl.when(i == EARLY // CHUNK)
                def _():
                    for load in slot_loads(1):
                        load.wait()

            spread(group, i * CHUNK)
            if group:
                @pl.when(i == STEP_AT[group])
                def _():
                    transform_send(group - 1)

        if group == 0:
            pl.semaphore_wait(barrier, z_devs)
            for load in loads:
                load.wait()
        swap(group).start()
    transform_send(n_groups - 1)

    rows = z_devs * 16
    await_codes(0)
    for part in range(2):
        deq_ref[part] = decode(0, 2 * part, 2).reshape(rows, half)
    await_codes(1)
    fold(0, decode(1, 0, 2))
    zed_ref[...] = transform_z(0)
    zed_ref[...] += transform_z(1)
    await_codes(2)
    message = recv_refs[2][...].astype(jnp.int32).astype(F32)
    late_ref[...] = (message[:, :8] * jnp.exp2(message[:, 8:9])).reshape(z_devs * 8, half)
    row = jnp.zeros((8, half), F32)
    for pair in range(2):
        high, low = split_bf16(jnp.concatenate([late_ref[pl.ds(2 * pair + k, half, stride=4), :] for k in range(2)], axis=1))
        zed = zed_ref[:, pl.ds(pair * grid_n, grid_n)]
        zed += jnp.dot(tl_ref[:, pl.ds(0, grid_n)], jnp.concatenate([high, low], axis=0), preferred_element_type=F32)
        zed += jnp.dot(tl_ref[:, pl.ds(grid_n, half)], high, preferred_element_type=F32)
        power = zed[:grid_n] * zed[:grid_n] + zed[grid_n:] * zed[grid_n:]
        for k in range(2):
            for part in range(2):
                place = pl.ds(4 * part + 2 * pair + k, half, stride=8)
                value = bc_ref[place, :] * power[part * half:(part + 1) * half, k * half:(k + 1) * half].T
                ek_ref[place, :] = value
                row += jnp.sum(value.reshape(half // 8, 8, half), axis=0)
    row_ref[0] = jnp.broadcast_to(jnp.sum(row, axis=0, keepdims=True), (8, half))

    others = rrow_ref.at[pl.ds(0, z_devs - 1), pl.ds(0, 1)]
    pair = pltpu.make_async_remote_copy(src_ref=row_ref.at[0, pl.ds(0, 1)], dst_ref=row_ref.at[1, pl.ds(0, 1)], send_sem=row_sem.at[2], recv_sem=row_sem.at[3], device_id=partner, device_id_type=MESH)
    pair.start()
    pair.wait()
    row_ref[2] = row_ref[0] + row_ref[1]

    def start(step):
        pltpu.make_async_remote_copy(src_ref=row_ref.at[2, pl.ds(0, 1)], dst_ref=rrow_ref.at[my_z, pl.ds(0, 1)], send_sem=row_sem.at[0], recv_sem=row_sem.at[1], device_id={'zdom': chip(step)}, device_id_type=MESH).start()

    to_chips(start)
    rrow_ref[my_z, pl.ds(0, 1)] = row_ref[2, pl.ds(0, 1)]
    await_all(others, row_sem.at[1])
    sum_ref[0] = jnp.sum(rrow_ref[:, pl.ds(0, 1), :]) * (0.5 / (grid_n * grid_n * grid_n))
    await_all(others, row_sem.at[0])
    for group in range(n_groups):
        await_all(code_refs[group].at[pl.ds(0, z_devs - 1), used(group)], send_sem.at[group])


def solution(mesh):
    y_devs = mesh.shape['ydom']
    z_devs = mesh.shape['zdom']
    slot_spec = P(('sys', 'ydom', 'zdom'))
    mode_spec = P(('sys', 'ydom'), 'zdom', None)

    def local_energy(charge, real_mask, grid_idx, spline_w, influence):
        grid_n = influence.shape[2]
        slots = charge.shape[0]
        half = grid_n // 2
        n_groups = len(GROUPS)
        table_x, table_y, table_z, late_z = dft_tables(grid_n, y_devs, z_devs)
        any_spec = pl.BlockSpec(memory_space=pl.ANY)
        rows = [len(GROUPS[g]) * (grid_n // y_devs) + ghost_rows(g) for g in range(n_groups)]
        codes = [pltpu.VMEM((z_devs, -(-(8 * len(planes) + 2) // 16) * 16, half), jnp.int16) for planes in GROUPS]
        tiles = jnp.swapaxes(influence.reshape(half, 4, 2, half), 1, 2).reshape(8 * half, half)
        mode_energy, energy = pl.pallas_call(
            functools.partial(energy_kernel, y_devs, z_devs),
            in_specs=[any_spec] * 9,
            out_specs=[pl.BlockSpec(memory_space=pltpu.VMEM), pl.BlockSpec(memory_space=pltpu.SMEM)],
            out_shape=[pltpu.VMEM((8 * half, half), F32), jax.ShapeDtypeStruct((1,), F32)],
            scratch_shapes=[
                pltpu.VMEM((1, slots), F32), pltpu.VMEM((1, slots), jnp.int32), pltpu.VMEM((3, slots), jnp.int32), pltpu.VMEM((3, 4, slots), F32),
                pltpu.VMEM((2, grid_n, SUB), BF16), pltpu.VMEM((2, 2, SUB, grid_n), BF16), pltpu.VMEM((slots, grid_n), BF16), pltpu.VMEM((slots, grid_n), BF16),
                pltpu.VMEM((2, rows[0], SUB), BF16), pltpu.VMEM((2, rows[0], SUB), BF16),
                [pltpu.VMEM((r, grid_n), F32) for r in rows], [pltpu.VMEM((r, grid_n), F32) for r in rows],
                pltpu.VMEM((2, 2 * grid_n, grid_n), F32), pltpu.VMEM((2, 2 * grid_n, grid_n), F32), pltpu.VMEM((4, 2 * grid_n, half), F32),
                codes, codes,
                pltpu.VMEM((2, z_devs * 16, half), F32), pltpu.VMEM((2 * grid_n, 4 * half), F32),
                pltpu.VMEM((8 * half, half), F32),
                pltpu.VMEM(table_x.shape[1:], BF16), pltpu.VMEM(table_y.shape, BF16), pltpu.VMEM(table_z.shape, BF16), pltpu.VMEM(late_z.shape, BF16),
                pltpu.VMEM((z_devs * 8, half), F32),
                pltpu.VMEM((3, 8, 128), F32), pltpu.VMEM((z_devs, 8, 128), F32),
                pltpu.SemaphoreType.DMA((2, 4)), pltpu.SemaphoreType.DMA((5,)), pltpu.SemaphoreType.DMA((2, n_groups)),
                pltpu.SemaphoreType.DMA((n_groups,)), pltpu.SemaphoreType.DMA((n_groups,)),
                pltpu.SemaphoreType.DMA((4,)),
            ],
            compiler_params=pltpu.CompilerParams(collective_id=0, has_side_effects=True, vmem_limit_bytes=60 * 1024 * 1024),
            name="energy",
        )(charge.reshape(1, slots), real_mask.reshape(1, slots), grid_idx.T, jnp.transpose(spline_w, (1, 2, 0)), tiles, jnp.asarray(table_x), jnp.asarray(table_y), jnp.asarray(table_z), jnp.asarray(late_z))
        mode_energy = lax.optimization_barrier(0.5 * mode_energy)
        return jnp.swapaxes(mode_energy.reshape(half, 2, 4, half), 1, 2).reshape(influence.shape), energy

    return jax.shard_map(local_energy, mesh=mesh, in_specs=(slot_spec, slot_spec, P(('sys', 'ydom', 'zdom'), None), P(('sys', 'ydom', 'zdom'), None, None), mode_spec), out_specs=(mode_spec, P('sys')), check_vma=False)
```

```python
import functools
import math
import jax
import jax.numpy as jnp
import numpy as np
from jax import lax
from jax.experimental import pallas as pl
from jax.experimental.pallas import tpu as pltpu
from jax.sharding import PartitionSpec as P

F32 = jnp.float32
BF16 = jnp.bfloat16
SUB = 512
CHUNK = 2048
GROUPS = ((0, 1, 2, 3), (4, 5), (6,))
STEP_AT = (0, 2, 3)
EARLY = 2048
CODE_MAX = 32767.0
MESH = pl.DeviceIdType.MESH


def split_bf16(value):
    high = value.astype(BF16)
    return high, (value - high.astype(F32)).astype(BF16)


def dot3(lhs, rhs, rhs_dim=0):
    def dot(a, b):
        return lax.dot_general(a, b, (((1,), (rhs_dim,)), ((), ())), preferred_element_type=F32)
    return dot(lhs[0], rhs[0]) + dot(lhs[1], rhs[0]) + dot(lhs[0], rhs[1])


def pick(ahead, taps, wrap=True):
    place = ahead & 15 if wrap else ahead
    value = jnp.zeros(ahead.shape, F32)
    for t in range(4):
        value = jnp.where(place == t, taps[t:t + 1], value)
    return value


def np_split(value):
    value = np.asarray(value, np.float32)
    high = value.astype(BF16)
    return np.stack([high, (value - high.astype(np.float32)).astype(BF16)])


def dft_tables(grid_n, y_devs, z_devs):
    turn = 2.0 * np.pi / grid_n
    len_y, len_z = grid_n // y_devs, grid_n // z_devs
    x = np.arange(grid_n)
    freq = np.arange(grid_n)
    phase_x = (np.outer(x, freq) % grid_n) * turn
    table_x = np.stack([np_split(np.concatenate([np.cos(phase_x[:, i * len_y:(i + 1) * len_y]), -np.sin(phase_x[:, i * len_y:(i + 1) * len_y])], axis=1)) for i in range(y_devs)])
    table_y = []
    for parity in range(2):
        ky = (np.arange(z_devs)[None, :] * len_z + 2 * np.arange(2)[:, None] + parity).reshape(-1)
        phase_y = (np.outer(ky, np.arange(grid_n // 2)) % grid_n) * turn
        real = np.concatenate([np.cos(phase_y), np.sin(phase_y)], axis=1)
        imag = np.concatenate([-np.sin(phase_y), np.cos(phase_y)], axis=1)
        table_y.append(np_split(np.concatenate([real, imag], axis=0)))

    def z_table(first, count):
        pos = np.arange(z_devs)[:, None] * len_z + first + np.arange(count)[None, :]
        phase_z = ((freq[:, None, None] * pos[None]) % grid_n) * turn
        real = np.stack([np.cos(phase_z), np.sin(phase_z)], axis=3).reshape(grid_n, -1)
        imag = np.stack([-np.sin(phase_z), np.cos(phase_z)], axis=3).reshape(grid_n, -1)
        return np_split(np.concatenate([real, imag], axis=0))

    high, low = z_table(6, 1)
    late_z = np.concatenate([high, high, low], axis=1)
    return table_x, np.stack(table_y), np.stack([z_table(0, 2), z_table(2, 2)]), late_z


def ghost_rows(group):
    return -(-8 * len(GROUPS[group]) // 16) * 16


def energy_kernel(y_devs, z_devs, q_hbm, m_hbm, idx_hbm, w_hbm, bc_hbm, tx_hbm, ty_hbm, tz_hbm, tl_hbm, ek_ref, sum_ref,
                  q_ref, m_ref, idx_ref, w_ref, line_ref, near_ref, xh_ref, xl_ref, ph_ref, pl_ref, acc_refs, got_refs, grid_ref, mid_ref, mode_ref,
                  code_refs, recv_refs,
                  deq_ref, zed_ref, bc_ref, tx_ref, ty_ref, tz_ref, tl_ref, late_ref, row_ref, rrow_ref,
                  early_sem, load_sem, swap_sem, send_sem, recv_sem, row_sem):
    my_y = lax.axis_index('ydom')
    my_z = lax.axis_index('zdom')
    grid_n = xh_ref.shape[1]
    slots = q_ref.shape[1]
    len_y = grid_n // y_devs
    half = grid_n // 2
    n_groups = len(GROUPS)
    barrier = pltpu.get_barrier_semaphore()
    partner = {'ydom': 1 - my_y}

    def chip(step):
        return (my_z + step) & (z_devs - 1)

    def far_first(start):
        pl.loop(z_devs // 2, z_devs)(start)
        pl.loop(1, z_devs // 2)(start)

    def slot_loads(piece):
        cols = pl.ds(0, EARLY) if piece == 0 else pl.ds(EARLY, slots - EARLY)
        return [pltpu.make_async_copy(hbm.at[lead + (cols,)], ref.at[lead + (cols,)], early_sem.at[piece, k])
                for k, (hbm, ref, lead) in enumerate(((q_hbm, q_ref, (slice(None),)), (m_hbm, m_ref, (slice(None),)), (idx_hbm, idx_ref, (slice(None),)), (w_hbm, w_ref, (slice(None), slice(None)))))]

    for piece in range(2):
        for load in slot_loads(piece):
            load.start()

    @pl.loop(1, z_devs)
    def _(step):
        pl.semaphore_signal(barrier, inc=1, device_id={'zdom': chip(step)}, device_id_type=MESH)

    pl.semaphore_signal(barrier, inc=1, device_id=partner, device_id_type=MESH)

    loads = [pltpu.make_async_copy(tx_hbm.at[my_y], tx_ref, load_sem.at[0]), pltpu.make_async_copy(ty_hbm, ty_ref, load_sem.at[1]),
             pltpu.make_async_copy(tz_hbm, tz_ref, load_sem.at[2]), pltpu.make_async_copy(bc_hbm, bc_ref, load_sem.at[3]), pltpu.make_async_copy(tl_hbm, tl_ref, load_sem.at[4])]
    for load in loads:
        load.start()

    def swap(group):
        return pltpu.make_async_remote_copy(src_ref=acc_refs[group], dst_ref=got_refs[group], send_sem=swap_sem.at[0, group], recv_sem=swap_sem.at[1, group], device_id=partner, device_id_type=MESH)

    def used(group):
        return pl.ds(0, 8 * len(GROUPS[group]) + 2)

    def send(group, step):
        other = chip(step)
        return pltpu.make_async_remote_copy(src_ref=code_refs[group].at[other, used(group)], dst_ref=recv_refs[group].at[my_z, used(group)], send_sem=send_sem.at[group], recv_sem=recv_sem.at[group], device_id={'zdom': other}, device_id_type=MESH)

    def spread(group, base):
        planes = GROUPS[group]
        zero_16 = jnp.zeros((16, SUB), BF16)
        total = None
        for sub in range(CHUNK // SUB):
            slot = sub % 2
            cols = pl.ds(pl.multiple_of(base + sub * SUB, SUB), SUB)
            row_16 = lax.broadcasted_iota(jnp.int32, (16, SUB), 0)
            if group == 0:
                weight = q_ref[:, cols] * m_ref[:, cols].astype(F32)
                ahead = row_16 - idx_ref[0:1, cols]
                taps = w_ref[0, :, cols] * weight
                high, low = split_bf16(pick(ahead, taps))
                tile_x = (-(ahead >> 4) & 15).astype(F32).astype(BF16)
                for r in range(grid_n // 16):
                    hit = tile_x == r
                    line_ref[0, 16 * r:16 * r + 16, :] = jnp.where(hit, high, zero_16)
                    line_ref[1, 16 * r:16 * r + 16, :] = jnp.where(hit, low, zero_16)
                for part, far_ref in enumerate((xh_ref, xl_ref)):
                    turned = line_ref[part].T
                    near_ref[slot, part] = turned
                    far_ref[cols, :] = turned
            ahead = row_16 - idx_ref[1:2, cols]
            line_y = pick(ahead, w_ref[1, :, cols])
            tile = -(ahead >> 4)
            ghost_y = jnp.where(tile[:8] == len_y // 16, line_y[:8], 0.0)
            tile_y = tile.astype(F32).astype(BF16)
            line_z = pick(row_16[:8] - idx_ref[2:3, cols], w_ref[2, :, cols], False)
            sides = [split_bf16(line_y * line_z[z:z + 1]) for z in planes]
            for r in range(len_y // 16):
                hit = tile_y == r
                for k, side in enumerate(sides):
                    first = k * len_y + 16 * r
                    ph_ref[slot, first:first + 16, :] = jnp.where(hit, side[0], zero_16)
                    pl_ref[slot, first:first + 16, :] = jnp.where(hit, side[1], zero_16)
            ghosts = [ghost_y * line_z[z:z + 1] for z in planes]
            if len(planes) % 2:
                ghosts.append(jnp.zeros((8, SUB), F32))
            high, low = split_bf16(jnp.concatenate(ghosts, axis=0))
            top = len(planes) * len_y
            rows = pl.ds(0, top + ghost_rows(group))
            ph_ref[slot, top:top + ghost_rows(group), :] = high
            pl_ref[slot, top:top + ghost_rows(group), :] = low
            if group == 0:
                part = dot3((ph_ref[slot, rows, :], pl_ref[slot, rows, :]), (near_ref[slot, 0], near_ref[slot, 1]))
            else:
                part = dot3((ph_ref[slot, rows, :], pl_ref[slot, rows, :]), (xh_ref[cols, :], xl_ref[cols, :]))
            total = part if total is None else total + part
        acc_refs[group][...] += total

    def transform_send(group):
        planes = GROUPS[group]
        acc_ref, got_ref = acc_refs[group], got_refs[group]
        swap(group).wait()
        sign = (1 - 2 * my_y).astype(F32)
        peak = jnp.full((1, 1), 1e-30, F32)
        for first in range(0, len(planes), 2):
            count = min(2, len(planes) - first)
            for k in range(count):
                block = pl.ds((first + k) * len_y, len_y)
                ghost = pl.ds(len(planes) * len_y + 8 * (first + k), 8)
                even, odd = 2 * k * len_y, (2 * k + 1) * len_y
                grid_ref[first // 2, pl.ds(even, len_y), :] = acc_ref[block, :] + got_ref[block, :]
                grid_ref[first // 2, pl.ds(odd, len_y), :] = sign * (acc_ref[block, :] - got_ref[block, :])
                grid_ref[first // 2, pl.ds(even, 8), :] += acc_ref[ghost, :] + got_ref[ghost, :]
                grid_ref[first // 2, pl.ds(odd, 8), :] -= sign * (acc_ref[ghost, :] - got_ref[ghost, :])
            size = count * grid_n
            mid_ref[first // 2, pl.ds(0, size), :] = dot3(split_bf16(grid_ref[first // 2, pl.ds(0, size), :]), (tx_ref[0], tx_ref[1]))
            for parity in range(2):
                columns = [jnp.concatenate([mid_ref[first // 2, pl.ds((2 * k + parity) * len_y, len_y), pl.ds(c * half, half)] for c in range(2)], axis=0) for k in range(count)]
                modes = dot3((ty_ref[parity, 0], ty_ref[parity, 1]), split_bf16(jnp.concatenate(columns, axis=1)))
                for block in range(4):
                    for k in range(count):
                        mode_ref[first + k, pl.ds(2 * block + parity, z_devs, stride=8), :] = modes[block * z_devs:(block + 1) * z_devs, k * half:(k + 1) * half]
                peak = jnp.maximum(peak, jnp.max(jnp.abs(modes), keepdims=True))
        power = jnp.ceil(jnp.log2(peak * (1.0 / CODE_MAX)) + 1e-3)
        gain = jnp.exp2(-power)
        for first in range(0, len(planes), 2):
            count = min(2, len(planes) - first)
            scaled = [(mode_ref[first + k] * gain).reshape(z_devs, 8, half) for k in range(count)]
            codes = jnp.round(jnp.concatenate(scaled, axis=1)).astype(jnp.int32).astype(jnp.int16)
            code_refs[group][:, pl.ds(8 * first, 8 * count), :] = codes
        code_refs[group][:, pl.ds(8 * len(planes), 2), :] = jnp.broadcast_to(power.astype(jnp.int32), (z_devs, 2, half)).astype(jnp.int16)

        def start(step):
            send(group, step).start()

        far_first(start)
        recv_refs[group][my_z] = code_refs[group][my_z]

    def await_all(ref, sem):
        pltpu.make_async_copy(ref, ref, sem).wait()

    def await_codes(group):
        await_all(recv_refs[group].at[pl.ds(0, z_devs - 1), used(group)], recv_sem.at[group])

    def decode(group, first, count):
        powers = recv_refs[group][:, pl.ds(8 * len(GROUPS[group]), 2), :].astype(jnp.int32).astype(F32)
        codes = recv_refs[group][:, pl.ds(8 * first, 8 * count), :].astype(jnp.int32).astype(F32)
        return codes * jnp.exp2(powers[:, :1, :])

    def fold(part, planes):
        rows = z_devs * 16
        flat = planes.reshape(rows, half)
        deq_ref[part, pl.ds(16, rows - 16), :] += flat[:rows - 16]
        deq_ref[part, pl.ds(0, 16), :] += flat[rows - 16:]

    def transform_z(part):
        flat = deq_ref.at[part]
        columns = [flat[pl.ds(ky, grid_n, stride=4), :] for ky in range(4)]
        return dot3((tz_ref[part, 0], tz_ref[part, 1]), split_bf16(jnp.concatenate(columns, axis=1)))

    for acc_ref in acc_refs:
        acc_ref[...] = jnp.zeros_like(acc_ref)
    for load in slot_loads(0):
        load.wait()
    for group in range(n_groups):
        @pl.loop(0, slots // CHUNK)
        def _(i):
            if group == 0:
                @pl.when(i == EARLY // CHUNK)
                def _():
                    for load in slot_loads(1):
                        load.wait()

            spread(group, i * CHUNK)
            if group:
                @pl.when(i == STEP_AT[group])
                def _():
                    transform_send(group - 1)

        if group == 0:
            pl.semaphore_wait(barrier, z_devs)
            for load in loads:
                load.wait()
        swap(group).start()
    transform_send(n_groups - 1)

    rows = z_devs * 16
    await_codes(0)
    for part in range(2):
        deq_ref[part] = decode(0, 2 * part, 2).reshape(rows, half)
    await_codes(1)
    fold(0, decode(1, 0, 2))
    zed_ref[...] = transform_z(0)
    zed_ref[...] += transform_z(1)
    await_codes(2)
    message = recv_refs[2][...].astype(jnp.int32).astype(F32)
    late_ref[...] = (message[:, :8] * jnp.exp2(message[:, 8:9])).reshape(z_devs * 8, half)
    row = jnp.zeros((8, half), F32)
    for pair in range(2):
        high, low = split_bf16(jnp.concatenate([late_ref[pl.ds(2 * pair + k, half, stride=4), :] for k in range(2)], axis=1))
        zed = zed_ref[:, pl.ds(pair * grid_n, grid_n)]
        zed += jnp.dot(tl_ref[:, pl.ds(0, grid_n)], jnp.concatenate([high, low], axis=0), preferred_element_type=F32)
        zed += jnp.dot(tl_ref[:, pl.ds(grid_n, half)], high, preferred_element_type=F32)
        power = zed[:grid_n] * zed[:grid_n] + zed[grid_n:] * zed[grid_n:]
        for k in range(2):
            for part in range(2):
                place = pl.ds(4 * part + 2 * pair + k, half, stride=8)
                value = bc_ref[place, :] * power[part * half:(part + 1) * half, k * half:(k + 1) * half].T
                ek_ref[place, :] = value
                row += jnp.sum(value.reshape(half // 8, 8, half), axis=0)
    row_ref[0] = jnp.broadcast_to(jnp.sum(row, axis=0, keepdims=True), (8, half))

    others = rrow_ref.at[pl.ds(0, z_devs - 1), pl.ds(0, 1)]
    pair = pltpu.make_async_remote_copy(src_ref=row_ref.at[0, pl.ds(0, 1)], dst_ref=row_ref.at[1, pl.ds(0, 1)], send_sem=row_sem.at[2], recv_sem=row_sem.at[3], device_id=partner, device_id_type=MESH)
    pair.start()
    pair.wait()
    row_ref[2] = row_ref[0] + row_ref[1]

    def start(step):
        pltpu.make_async_remote_copy(src_ref=row_ref.at[2, pl.ds(0, 1)], dst_ref=rrow_ref.at[my_z, pl.ds(0, 1)], send_sem=row_sem.at[0], recv_sem=row_sem.at[1], device_id={'zdom': chip(step)}, device_id_type=MESH).start()

    far_first(start)
    rrow_ref[my_z, pl.ds(0, 1)] = row_ref[2, pl.ds(0, 1)]
    await_all(others, row_sem.at[1])
    sum_ref[0] = jnp.sum(rrow_ref[:, pl.ds(0, 1), :]) * (0.5 / (grid_n * grid_n * grid_n))
    await_all(others, row_sem.at[0])
    for group in range(n_groups):
        await_all(code_refs[group].at[pl.ds(0, z_devs - 1), used(group)], send_sem.at[group])


def solution(mesh):
    y_devs = mesh.shape['ydom']
    z_devs = mesh.shape['zdom']
    slot_spec = P(('sys', 'ydom', 'zdom'))
    mode_spec = P(('sys', 'ydom'), 'zdom', None)

    def local_energy(charge, real_mask, grid_idx, spline_w, influence):
        grid_n = influence.shape[2]
        slots = charge.shape[0]
        half = grid_n // 2
        n_groups = len(GROUPS)
        table_x, table_y, table_z, late_z = dft_tables(grid_n, y_devs, z_devs)
        any_spec = pl.BlockSpec(memory_space=pl.ANY)
        rows = [len(GROUPS[g]) * (grid_n // y_devs) + ghost_rows(g) for g in range(n_groups)]
        codes = [pltpu.VMEM((z_devs, -(-(8 * len(planes) + 2) // 16) * 16, half), jnp.int16) for planes in GROUPS]
        tiles = jnp.swapaxes(influence.reshape(half, 4, 2, half), 1, 2).reshape(8 * half, half)
        mode_energy, energy = pl.pallas_call(
            functools.partial(energy_kernel, y_devs, z_devs),
            in_specs=[any_spec] * 9,
            out_specs=[pl.BlockSpec(memory_space=pltpu.VMEM), pl.BlockSpec(memory_space=pltpu.SMEM)],
            out_shape=[pltpu.VMEM((8 * half, half), F32), jax.ShapeDtypeStruct((1,), F32)],
            scratch_shapes=[
                pltpu.VMEM((1, slots), F32), pltpu.VMEM((1, slots), jnp.int32), pltpu.VMEM((3, slots), jnp.int32), pltpu.VMEM((3, 4, slots), F32),
                pltpu.VMEM((2, grid_n, SUB), BF16), pltpu.VMEM((2, 2, SUB, grid_n), BF16), pltpu.VMEM((slots, grid_n), BF16), pltpu.VMEM((slots, grid_n), BF16),
                pltpu.VMEM((2, rows[0], SUB), BF16), pltpu.VMEM((2, rows[0], SUB), BF16),
                [pltpu.VMEM((r, grid_n), F32) for r in rows], [pltpu.VMEM((r, grid_n), F32) for r in rows],
                pltpu.VMEM((2, 2 * grid_n, grid_n), F32), pltpu.VMEM((2, 2 * grid_n, grid_n), F32), pltpu.VMEM((4, 2 * grid_n, half), F32),
                codes, codes,
                pltpu.VMEM((2, z_devs * 16, half), F32), pltpu.VMEM((2 * grid_n, 4 * half), F32),
                pltpu.VMEM((8 * half, half), F32),
                pltpu.VMEM(table_x.shape[1:], BF16), pltpu.VMEM(table_y.shape, BF16), pltpu.VMEM(table_z.shape, BF16), pltpu.VMEM(late_z.shape, BF16),
                pltpu.VMEM((z_devs * 8, half), F32),
                pltpu.VMEM((3, 8, 128), F32), pltpu.VMEM((z_devs, 8, 128), F32),
                pltpu.SemaphoreType.DMA((2, 4)), pltpu.SemaphoreType.DMA((5,)), pltpu.SemaphoreType.DMA((2, n_groups)),
                pltpu.SemaphoreType.DMA((n_groups,)), pltpu.SemaphoreType.DMA((n_groups,)),
                pltpu.SemaphoreType.DMA((4,)),
            ],
            compiler_params=pltpu.CompilerParams(collective_id=0, has_side_effects=True, vmem_limit_bytes=60 * 1024 * 1024),
            name="energy",
        )(charge.reshape(1, slots), real_mask.reshape(1, slots), grid_idx.T, jnp.transpose(spline_w, (1, 2, 0)), tiles, jnp.asarray(table_x), jnp.asarray(table_y), jnp.asarray(table_z), jnp.asarray(late_z))
        mode_energy = lax.optimization_barrier(0.5 * mode_energy)
        return jnp.swapaxes(mode_energy.reshape(half, 2, 4, half), 1, 2).reshape(influence.shape), energy

    return jax.shard_map(local_energy, mesh=mesh, in_specs=(slot_spec, slot_spec, P(('sys', 'ydom', 'zdom'), None), P(('sys', 'ydom', 'zdom'), None, None), mode_spec), out_specs=(mode_spec, P('sys')), check_vma=False)
```

```python
import functools
import math
import jax
import jax.numpy as jnp
import numpy as np
from jax import lax
from jax.experimental import pallas as pl
from jax.experimental.pallas import tpu as pltpu
from jax.sharding import PartitionSpec as P

F32 = jnp.float32
BF16 = jnp.bfloat16
SUB = 512
CHUNK = 2048
GROUPS = ((0, 1, 2, 3), (4, 5), (6,))
STEP_AT = (0, 1, 2)
EARLY = 2048
CODE_MAX = 32767.0
MESH = pl.DeviceIdType.MESH


def split_bf16(value):
    high = value.astype(BF16)
    return high, (value - high.astype(F32)).astype(BF16)


def dot3(lhs, rhs, rhs_dim=0):
    def dot(a, b):
        return lax.dot_general(a, b, (((1,), (rhs_dim,)), ((), ())), preferred_element_type=F32)
    return dot(lhs[0], rhs[0]) + dot(lhs[1], rhs[0]) + dot(lhs[0], rhs[1])


def pick(ahead, taps, wrap=True):
    place = ahead & 15 if wrap else ahead
    value = jnp.zeros(ahead.shape, F32)
    for t in range(4):
        value = jnp.where(place == t, taps[t:t + 1], value)
    return value


def np_split(value):
    value = np.asarray(value, np.float32)
    high = value.astype(BF16)
    return np.stack([high, (value - high.astype(np.float32)).astype(BF16)])


def dft_tables(grid_n, y_devs, z_devs):
    turn = 2.0 * np.pi / grid_n
    len_y, len_z = grid_n // y_devs, grid_n // z_devs
    x = np.arange(grid_n)
    freq = np.arange(grid_n)
    phase_x = (np.outer(x, freq) % grid_n) * turn
    table_x = np.stack([np_split(np.concatenate([np.cos(phase_x[:, i * len_y:(i + 1) * len_y]), -np.sin(phase_x[:, i * len_y:(i + 1) * len_y])], axis=1)) for i in range(y_devs)])
    table_y = []
    for parity in range(2):
        ky = (np.arange(z_devs)[None, :] * len_z + 2 * np.arange(2)[:, None] + parity).reshape(-1)
        phase_y = (np.outer(ky, np.arange(grid_n // 2)) % grid_n) * turn
        real = np.concatenate([np.cos(phase_y), np.sin(phase_y)], axis=1)
        imag = np.concatenate([-np.sin(phase_y), np.cos(phase_y)], axis=1)
        table_y.append(np_split(np.concatenate([real, imag], axis=0)))

    def z_table(first, count):
        pos = np.arange(z_devs)[:, None] * len_z + first + np.arange(count)[None, :]
        phase_z = ((freq[:, None, None] * pos[None]) % grid_n) * turn
        real = np.stack([np.cos(phase_z), np.sin(phase_z)], axis=3).reshape(grid_n, -1)
        imag = np.stack([-np.sin(phase_z), np.cos(phase_z)], axis=3).reshape(grid_n, -1)
        return np_split(np.concatenate([real, imag], axis=0))

    high, low = z_table(6, 1)
    late_z = np.concatenate([high, high, low], axis=1)
    return table_x, np.stack(table_y), np.stack([z_table(0, 2), z_table(2, 2)]), late_z


def ghost_rows(group):
    return -(-8 * len(GROUPS[group]) // 16) * 16


def energy_kernel(y_devs, z_devs, q_hbm, m_hbm, idx_hbm, w_hbm, bc_hbm, tx_hbm, ty_hbm, tz_hbm, tl_hbm, ek_ref, sum_ref,
                  q_ref, m_ref, idx_ref, w_ref, near_ref, xh_ref, xl_ref, ph_ref, pl_ref, acc_refs, got_refs, grid_ref, mid_ref, mode_ref,
                  code_refs, recv_refs,
                  deq_ref, zed_ref, bc_ref, tx_ref, ty_ref, tz_ref, tl_ref, late_ref, row_ref, rrow_ref,
                  early_sem, load_sem, swap_sem, send_sem, recv_sem, row_sem):
    my_y = lax.axis_index('ydom')
    my_z = lax.axis_index('zdom')
    grid_n = xh_ref.shape[1]
    slots = q_ref.shape[1]
    len_y = grid_n // y_devs
    half = grid_n // 2
    n_groups = len(GROUPS)
    barrier = pltpu.get_barrier_semaphore()
    partner = {'ydom': 1 - my_y}

    def chip(step):
        return (my_z + step) & (z_devs - 1)

    def far_first(start):
        pl.loop(z_devs // 2, z_devs)(start)
        pl.loop(1, z_devs // 2)(start)

    def slot_loads(piece):
        cols = pl.ds(0, EARLY) if piece == 0 else pl.ds(EARLY, slots - EARLY)
        return [pltpu.make_async_copy(hbm.at[lead + (cols,)], ref.at[lead + (cols,)], early_sem.at[piece, k])
                for k, (hbm, ref, lead) in enumerate(((q_hbm, q_ref, (slice(None),)), (m_hbm, m_ref, (slice(None),)), (idx_hbm, idx_ref, (slice(None),)), (w_hbm, w_ref, (slice(None), slice(None)))))]

    for piece in range(2):
        for load in slot_loads(piece):
            load.start()

    @pl.loop(1, z_devs)
    def _(step):
        pl.semaphore_signal(barrier, inc=1, device_id={'zdom': chip(step)}, device_id_type=MESH)

    pl.semaphore_signal(barrier, inc=1, device_id=partner, device_id_type=MESH)

    loads = [pltpu.make_async_copy(tx_hbm.at[my_y], tx_ref, load_sem.at[0]), pltpu.make_async_copy(ty_hbm, ty_ref, load_sem.at[1]),
             pltpu.make_async_copy(tz_hbm, tz_ref, load_sem.at[2]), pltpu.make_async_copy(bc_hbm, bc_ref, load_sem.at[3]), pltpu.make_async_copy(tl_hbm, tl_ref, load_sem.at[4])]
    for load in loads:
        load.start()

    def swap(group):
        return pltpu.make_async_remote_copy(src_ref=acc_refs[group], dst_ref=got_refs[group], send_sem=swap_sem.at[0, group], recv_sem=swap_sem.at[1, group], device_id=partner, device_id_type=MESH)

    def used(group):
        return pl.ds(0, 8 * len(GROUPS[group]) + 2)

    def send(group, step):
        other = chip(step)
        return pltpu.make_async_remote_copy(src_ref=code_refs[group].at[other, used(group)], dst_ref=recv_refs[group].at[my_z, used(group)], send_sem=send_sem.at[group], recv_sem=recv_sem.at[group], device_id={'zdom': other}, device_id_type=MESH)

    def spread(group, base):
        planes = GROUPS[group]
        zero_16 = jnp.zeros((16, SUB), BF16)
        total = None
        for sub in range(CHUNK // SUB):
            slot = sub % 2
            cols = pl.ds(pl.multiple_of(base + sub * SUB, SUB), SUB)
            row_16 = lax.broadcasted_iota(jnp.int32, (16, SUB), 0)
            if group == 0:
                weight = q_ref[:, cols] * m_ref[:, cols].astype(F32)
                ahead = row_16 - idx_ref[0:1, cols]
                taps = w_ref[0, :, cols] * weight
                high, low = split_bf16(pick(ahead, taps))
                tile_x = (-(ahead >> 4) & 15).astype(F32).astype(BF16)
                for r in range(grid_n // 16):
                    hit = tile_x == r
                    near_ref[slot, 0, 16 * r:16 * r + 16, :] = jnp.where(hit, high, zero_16)
                    near_ref[slot, 1, 16 * r:16 * r + 16, :] = jnp.where(hit, low, zero_16)
                xh_ref[cols, :] = near_ref[slot, 0].T
                xl_ref[cols, :] = near_ref[slot, 1].T
            ahead = row_16 - idx_ref[1:2, cols]
            line_y = pick(ahead, w_ref[1, :, cols])
            tile = -(ahead >> 4)
            ghost_y = jnp.where(tile[:8] == len_y // 16, line_y[:8], 0.0)
            tile_y = tile.astype(F32).astype(BF16)
            line_z = pick(row_16[:8] - idx_ref[2:3, cols], w_ref[2, :, cols], False)
            sides = [split_bf16(line_y * line_z[z:z + 1]) for z in planes]
            for r in range(len_y // 16):
                hit = tile_y == r
                for k, side in enumerate(sides):
                    first = k * len_y + 16 * r
                    ph_ref[slot, first:first + 16, :] = jnp.where(hit, side[0], zero_16)
                    pl_ref[slot, first:first + 16, :] = jnp.where(hit, side[1], zero_16)
            ghosts = [ghost_y * line_z[z:z + 1] for z in planes]
            if len(planes) % 2:
                ghosts.append(jnp.zeros((8, SUB), F32))
            high, low = split_bf16(jnp.concatenate(ghosts, axis=0))
            top = len(planes) * len_y
            rows = pl.ds(0, top + ghost_rows(group))
            ph_ref[slot, top:top + ghost_rows(group), :] = high
            pl_ref[slot, top:top + ghost_rows(group), :] = low
            if group == 0:
                part = dot3((ph_ref[slot, rows, :], pl_ref[slot, rows, :]), (near_ref[slot, 0], near_ref[slot, 1]), 1)
            else:
                part = dot3((ph_ref[slot, rows, :], pl_ref[slot, rows, :]), (xh_ref[cols, :], xl_ref[cols, :]))
            total = part if total is None else total + part
        acc_refs[group][...] += total

    def transform_send(group):
        planes = GROUPS[group]
        acc_ref, got_ref = acc_refs[group], got_refs[group]
        swap(group).wait()
        sign = (1 - 2 * my_y).astype(F32)
        peak = jnp.full((1, 1), 1e-30, F32)
        for first in range(0, len(planes), 2):
            count = min(2, len(planes) - first)
            for k in range(count):
                block = pl.ds((first + k) * len_y, len_y)
                ghost = pl.ds(len(planes) * len_y + 8 * (first + k), 8)
                even, odd = 2 * k * len_y, (2 * k + 1) * len_y
                grid_ref[pl.ds(even, len_y), :] = acc_ref[block, :] + got_ref[block, :]
                grid_ref[pl.ds(odd, len_y), :] = sign * (acc_ref[block, :] - got_ref[block, :])
                grid_ref[pl.ds(even, 8), :] += acc_ref[ghost, :] + got_ref[ghost, :]
                grid_ref[pl.ds(odd, 8), :] -= sign * (acc_ref[ghost, :] - got_ref[ghost, :])
            size = count * grid_n
            mid_ref[pl.ds(0, size), :] = dot3(split_bf16(grid_ref[pl.ds(0, size), :]), (tx_ref[0], tx_ref[1]))
            for parity in range(2):
                columns = [jnp.concatenate([mid_ref[pl.ds((2 * k + parity) * len_y, len_y), pl.ds(c * half, half)] for c in range(2)], axis=0) for k in range(count)]
                modes = dot3((ty_ref[parity, 0], ty_ref[parity, 1]), split_bf16(jnp.concatenate(columns, axis=1)))
                for block in range(4):
                    for k in range(count):
                        mode_ref[first + k, pl.ds(2 * block + parity, z_devs, stride=8), :] = modes[block * z_devs:(block + 1) * z_devs, k * half:(k + 1) * half]
                peak = jnp.maximum(peak, jnp.max(jnp.abs(modes), keepdims=True))
        power = jnp.ceil(jnp.log2(peak * (1.0 / CODE_MAX)) + 1e-3)
        gain = jnp.exp2(-power)
        for first in range(0, len(planes), 2):
            count = min(2, len(planes) - first)
            scaled = [(mode_ref[first + k] * gain).reshape(z_devs, 8, half) for k in range(count)]
            codes = jnp.round(jnp.concatenate(scaled, axis=1)).astype(jnp.int32).astype(jnp.int16)
            code_refs[group][:, pl.ds(8 * first, 8 * count), :] = codes
        code_refs[group][:, pl.ds(8 * len(planes), 2), :] = jnp.broadcast_to(power.astype(jnp.int32), (z_devs, 2, half)).astype(jnp.int16)

        def start(step):
            send(group, step).start()

        far_first(start)
        recv_refs[group][my_z] = code_refs[group][my_z]

    def await_all(ref, sem):
        pltpu.make_async_copy(ref, ref, sem).wait()

    def await_codes(group):
        await_all(recv_refs[group].at[pl.ds(0, z_devs - 1), used(group)], recv_sem.at[group])

    def decode(group, first, count):
        powers = recv_refs[group][:, pl.ds(8 * len(GROUPS[group]), 2), :].astype(jnp.int32).astype(F32)
        codes = recv_refs[group][:, pl.ds(8 * first, 8 * count), :].astype(jnp.int32).astype(F32)
        return codes * jnp.exp2(powers[:, :1, :])

    def fold(part, planes):
        rows = z_devs * 16
        flat = planes.reshape(rows, half)
        deq_ref[part, pl.ds(16, rows - 16), :] += flat[:rows - 16]
        deq_ref[part, pl.ds(0, 16), :] += flat[rows - 16:]

    def transform_z(part):
        flat = deq_ref.at[part]
        columns = [flat[pl.ds(ky, grid_n, stride=4), :] for ky in range(4)]
        return dot3((tz_ref[part, 0], tz_ref[part, 1]), split_bf16(jnp.concatenate(columns, axis=1)))

    for acc_ref in acc_refs:
        acc_ref[...] = jnp.zeros_like(acc_ref)
    for load in slot_loads(0):
        load.wait()
    for group in range(n_groups):
        @pl.loop(0, slots // CHUNK)
        def _(i):
            if group == 0:
                @pl.when(i == EARLY // CHUNK)
                def _():
                    for load in slot_loads(1):
                        load.wait()

            spread(group, i * CHUNK)
            if group:
                @pl.when(i == STEP_AT[group])
                def _():
                    transform_send(group - 1)

        if group == 0:
            pl.semaphore_wait(barrier, z_devs)
            for load in loads:
                load.wait()
        swap(group).start()
    transform_send(n_groups - 1)

    rows = z_devs * 16
    await_codes(0)
    for part in range(2):
        deq_ref[part] = decode(0, 2 * part, 2).reshape(rows, half)
    await_codes(1)
    fold(0, decode(1, 0, 2))
    zed_ref[...] = transform_z(0)
    zed_ref[...] += transform_z(1)
    await_codes(2)
    message = recv_refs[2][...].astype(jnp.int32).astype(F32)
    late_ref[...] = (message[:, :8] * jnp.exp2(message[:, 8:9])).reshape(z_devs * 8, half)
    row = jnp.zeros((8, half), F32)
    for pair in range(2):
        high, low = split_bf16(jnp.concatenate([late_ref[pl.ds(2 * pair + k, half, stride=4), :] for k in range(2)], axis=1))
        zed = zed_ref[:, pl.ds(pair * grid_n, grid_n)]
        zed += jnp.dot(tl_ref[:, pl.ds(0, grid_n)], jnp.concatenate([high, low], axis=0), preferred_element_type=F32)
        zed += jnp.dot(tl_ref[:, pl.ds(grid_n, half)], high, preferred_element_type=F32)
        power = zed[:grid_n] * zed[:grid_n] + zed[grid_n:] * zed[grid_n:]
        for k in range(2):
            for part in range(2):
                place = pl.ds(4 * part + 2 * pair + k, half, stride=8)
                value = bc_ref[place, :] * power[part * half:(part + 1) * half, k * half:(k + 1) * half].T
                ek_ref[place, :] = value
                row += jnp.sum(value.reshape(half // 8, 8, half), axis=0)
    row_ref[0] = jnp.broadcast_to(jnp.sum(row, axis=0, keepdims=True), (8, half))

    others = rrow_ref.at[pl.ds(0, z_devs - 1), pl.ds(0, 1)]
    pair = pltpu.make_async_remote_copy(src_ref=row_ref.at[0, pl.ds(0, 1)], dst_ref=row_ref.at[1, pl.ds(0, 1)], send_sem=row_sem.at[2], recv_sem=row_sem.at[3], device_id=partner, device_id_type=MESH)
    pair.start()
    pair.wait()
    row_ref[2] = row_ref[0] + row_ref[1]

    def start(step):
        pltpu.make_async_remote_copy(src_ref=row_ref.at[2, pl.ds(0, 1)], dst_ref=rrow_ref.at[my_z, pl.ds(0, 1)], send_sem=row_sem.at[0], recv_sem=row_sem.at[1], device_id={'zdom': chip(step)}, device_id_type=MESH).start()

    far_first(start)
    rrow_ref[my_z, pl.ds(0, 1)] = row_ref[2, pl.ds(0, 1)]
    await_all(others, row_sem.at[1])
    sum_ref[0] = jnp.sum(rrow_ref[:, pl.ds(0, 1), :]) * (0.5 / (grid_n * grid_n * grid_n))
    await_all(others, row_sem.at[0])
    for group in range(n_groups):
        await_all(code_refs[group].at[pl.ds(0, z_devs - 1), used(group)], send_sem.at[group])


def solution(mesh):
    y_devs = mesh.shape['ydom']
    z_devs = mesh.shape['zdom']
    slot_spec = P(('sys', 'ydom', 'zdom'))
    mode_spec = P(('sys', 'ydom'), 'zdom', None)

    def local_energy(charge, real_mask, grid_idx, spline_w, influence):
        grid_n = influence.shape[2]
        slots = charge.shape[0]
        half = grid_n // 2
        n_groups = len(GROUPS)
        table_x, table_y, table_z, late_z = dft_tables(grid_n, y_devs, z_devs)
        any_spec = pl.BlockSpec(memory_space=pl.ANY)
        rows = [len(GROUPS[g]) * (grid_n // y_devs) + ghost_rows(g) for g in range(n_groups)]
        codes = [pltpu.VMEM((z_devs, -(-(8 * len(planes) + 2) // 16) * 16, half), jnp.int16) for planes in GROUPS]
        tiles = jnp.swapaxes(influence.reshape(half, 4, 2, half), 1, 2).reshape(8 * half, half)
        mode_energy, energy = pl.pallas_call(
            functools.partial(energy_kernel, y_devs, z_devs),
            in_specs=[any_spec] * 9,
            out_specs=[pl.BlockSpec(memory_space=pltpu.VMEM), pl.BlockSpec(memory_space=pltpu.SMEM)],
            out_shape=[pltpu.VMEM((8 * half, half), F32), jax.ShapeDtypeStruct((1,), F32)],
            scratch_shapes=[
                pltpu.VMEM((1, slots), F32), pltpu.VMEM((1, slots), jnp.int32), pltpu.VMEM((3, slots), jnp.int32), pltpu.VMEM((3, 4, slots), F32),
                pltpu.VMEM((2, 2, grid_n, SUB), BF16), pltpu.VMEM((slots, grid_n), BF16), pltpu.VMEM((slots, grid_n), BF16),
                pltpu.VMEM((2, rows[0], SUB), BF16), pltpu.VMEM((2, rows[0], SUB), BF16),
                [pltpu.VMEM((r, grid_n), F32) for r in rows], [pltpu.VMEM((r, grid_n), F32) for r in rows],
                pltpu.VMEM((2 * grid_n, grid_n), F32), pltpu.VMEM((2 * grid_n, grid_n), F32), pltpu.VMEM((4, 2 * grid_n, half), F32),
                codes, codes,
                pltpu.VMEM((2, z_devs * 16, half), F32), pltpu.VMEM((2 * grid_n, 4 * half), F32),
                pltpu.VMEM((8 * half, half), F32),
                pltpu.VMEM(table_x.shape[1:], BF16), pltpu.VMEM(table_y.shape, BF16), pltpu.VMEM(table_z.shape, BF16), pltpu.VMEM(late_z.shape, BF16),
                pltpu.VMEM((z_devs * 8, half), F32),
                pltpu.VMEM((3, 8, 128), F32), pltpu.VMEM((z_devs, 8, 128), F32),
                pltpu.SemaphoreType.DMA((2, 4)), pltpu.SemaphoreType.DMA((5,)), pltpu.SemaphoreType.DMA((2, n_groups)),
                pltpu.SemaphoreType.DMA((n_groups,)), pltpu.SemaphoreType.DMA((n_groups,)),
                pltpu.SemaphoreType.DMA((4,)),
            ],
            compiler_params=pltpu.CompilerParams(collective_id=0, has_side_effects=True, vmem_limit_bytes=60 * 1024 * 1024),
            name="energy",
        )(charge.reshape(1, slots), real_mask.reshape(1, slots), grid_idx.T, jnp.transpose(spline_w, (1, 2, 0)), tiles, jnp.asarray(table_x), jnp.asarray(table_y), jnp.asarray(table_z), jnp.asarray(late_z))
        mode_energy = lax.optimization_barrier(0.5 * mode_energy)
        return jnp.swapaxes(mode_energy.reshape(half, 2, 4, half), 1, 2).reshape(influence.shape), energy

    return jax.shard_map(local_energy, mesh=mesh, in_specs=(slot_spec, slot_spec, P(('sys', 'ydom', 'zdom'), None), P(('sys', 'ydom', 'zdom'), None, None), mode_spec), out_specs=(mode_spec, P('sys')), check_vma=False)
```

```python
import functools
import math
import jax
import jax.numpy as jnp
import numpy as np
from jax import lax
from jax.experimental import pallas as pl
from jax.experimental.pallas import tpu as pltpu
from jax.sharding import PartitionSpec as P

F32 = jnp.float32
BF16 = jnp.bfloat16
SUB = 512
CHUNK = 2048
GROUPS = ((0, 1, 2, 3), (4, 5), (6,))
STEP_AT = (0, 2, 3)
EARLY = 2048
CODE_MAX = 32767.0
MESH = pl.DeviceIdType.MESH


def split_bf16(value):
    high = value.astype(BF16)
    return high, (value - high.astype(F32)).astype(BF16)


def dot3(lhs, rhs, rhs_dim=0):
    def dot(a, b):
        return lax.dot_general(a, b, (((1,), (rhs_dim,)), ((), ())), preferred_element_type=F32)
    return dot(lhs[0], rhs[0]) + dot(lhs[1], rhs[0]) + dot(lhs[0], rhs[1])


def pick(ahead, taps, wrap=True):
    place = ahead & 15 if wrap else ahead
    value = jnp.zeros(ahead.shape, F32)
    for t in range(4):
        value = jnp.where(place == t, taps[t:t + 1], value)
    return value


def np_split(value):
    value = np.asarray(value, np.float32)
    high = value.astype(BF16)
    return np.stack([high, (value - high.astype(np.float32)).astype(BF16)])


def dft_tables(grid_n, y_devs, z_devs):
    turn = 2.0 * np.pi / grid_n
    len_y, len_z = grid_n // y_devs, grid_n // z_devs
    x = np.arange(grid_n)
    freq = np.arange(grid_n)
    phase_x = (np.outer(x, freq) % grid_n) * turn
    table_x = np.stack([np_split(np.concatenate([np.cos(phase_x[:, i * len_y:(i + 1) * len_y]), -np.sin(phase_x[:, i * len_y:(i + 1) * len_y])], axis=1)) for i in range(y_devs)])
    table_y = []
    for parity in range(2):
        ky = (np.arange(z_devs)[None, :] * len_z + 2 * np.arange(2)[:, None] + parity).reshape(-1)
        phase_y = (np.outer(ky, np.arange(grid_n // 2)) % grid_n) * turn
        real = np.concatenate([np.cos(phase_y), np.sin(phase_y)], axis=1)
        imag = np.concatenate([-np.sin(phase_y), np.cos(phase_y)], axis=1)
        table_y.append(np_split(np.concatenate([real, imag], axis=0)))

    def z_table(first, count):
        pos = np.arange(z_devs)[:, None] * len_z + first + np.arange(count)[None, :]
        phase_z = ((freq[:, None, None] * pos[None]) % grid_n) * turn
        real = np.stack([np.cos(phase_z), np.sin(phase_z)], axis=3).reshape(grid_n, -1)
        imag = np.stack([-np.sin(phase_z), np.cos(phase_z)], axis=3).reshape(grid_n, -1)
        return np_split(np.concatenate([real, imag], axis=0))

    high, low = z_table(6, 1)
    late_z = np.concatenate([high, high, low], axis=1)
    return table_x, np.stack(table_y), np.stack([z_table(0, 2), z_table(2, 2)]), late_z


def ghost_rows(group):
    return -(-8 * len(GROUPS[group]) // 16) * 16


def energy_kernel(y_devs, z_devs, q_hbm, m_hbm, idx_hbm, w_hbm, bc_hbm, tx_hbm, ty_hbm, tz_hbm, tl_hbm, ek_ref, sum_ref,
                  q_ref, m_ref, idx_ref, w_ref, near_ref, xh_ref, xl_ref, ph_ref, pl_ref, acc_refs, got_refs, grid_ref, mid_ref, mode_ref,
                  code_refs, recv_refs,
                  deq_ref, zed_ref, bc_ref, tx_ref, ty_ref, tz_ref, tl_ref, late_ref, row_ref, rrow_ref,
                  early_sem, load_sem, swap_sem, send_sem, recv_sem, row_sem):
    my_y = lax.axis_index('ydom')
    my_z = lax.axis_index('zdom')
    grid_n = xh_ref.shape[1]
    slots = q_ref.shape[1]
    len_y = grid_n // y_devs
    half = grid_n // 2
    n_groups = len(GROUPS)
    barrier = pltpu.get_barrier_semaphore()
    partner = {'ydom': 1 - my_y}

    def chip(step):
        return (my_z + step) & (z_devs - 1)

    def far_first(start):
        for first in (2, 1, 3, 0):
            pl.loop(max(1, first * z_devs // 4), (first + 1) * z_devs // 4)(start)

    def slot_loads(piece):
        cols = pl.ds(0, EARLY) if piece == 0 else pl.ds(EARLY, slots - EARLY)
        return [pltpu.make_async_copy(hbm.at[lead + (cols,)], ref.at[lead + (cols,)], early_sem.at[piece, k])
                for k, (hbm, ref, lead) in enumerate(((q_hbm, q_ref, (slice(None),)), (m_hbm, m_ref, (slice(None),)), (idx_hbm, idx_ref, (slice(None),)), (w_hbm, w_ref, (slice(None), slice(None)))))]

    for piece in range(2):
        for load in slot_loads(piece):
            load.start()

    @pl.loop(1, z_devs)
    def _(step):
        pl.semaphore_signal(barrier, inc=1, device_id={'zdom': chip(step)}, device_id_type=MESH)

    pl.semaphore_signal(barrier, inc=1, device_id=partner, device_id_type=MESH)

    loads = [pltpu.make_async_copy(tx_hbm.at[my_y], tx_ref, load_sem.at[0]), pltpu.make_async_copy(ty_hbm, ty_ref, load_sem.at[1]),
             pltpu.make_async_copy(tz_hbm, tz_ref, load_sem.at[2]), pltpu.make_async_copy(bc_hbm, bc_ref, load_sem.at[3]), pltpu.make_async_copy(tl_hbm, tl_ref, load_sem.at[4])]
    for load in loads:
        load.start()

    def swap(group):
        return pltpu.make_async_remote_copy(src_ref=acc_refs[group], dst_ref=got_refs[group], send_sem=swap_sem.at[0, group], recv_sem=swap_sem.at[1, group], device_id=partner, device_id_type=MESH)

    def used(group):
        return pl.ds(0, 8 * len(GROUPS[group]) + 2)

    def send(group, step):
        other = chip(step)
        return pltpu.make_async_remote_copy(src_ref=code_refs[group].at[other, used(group)], dst_ref=recv_refs[group].at[my_z, used(group)], send_sem=send_sem.at[group], recv_sem=recv_sem.at[group], device_id={'zdom': other}, device_id_type=MESH)

    def spread(group, base):
        planes = GROUPS[group]
        zero_16 = jnp.zeros((16, SUB), BF16)
        total = None
        for sub in range(CHUNK // SUB):
            slot = sub % 2
            cols = pl.ds(pl.multiple_of(base + sub * SUB, SUB), SUB)
            row_16 = lax.broadcasted_iota(jnp.int32, (16, SUB), 0)
            if group == 0:
                weight = q_ref[:, cols] * m_ref[:, cols].astype(F32)
                ahead = row_16 - idx_ref[0:1, cols]
                taps = w_ref[0, :, cols] * weight
                high, low = split_bf16(pick(ahead, taps))
                tile_x = (-(ahead >> 4) & 15).astype(F32).astype(BF16)
                for r in range(grid_n // 16):
                    hit = tile_x == r
                    near_ref[slot, 0, 16 * r:16 * r + 16, :] = jnp.where(hit, high, zero_16)
                    near_ref[slot, 1, 16 * r:16 * r + 16, :] = jnp.where(hit, low, zero_16)
                xh_ref[cols, :] = near_ref[slot, 0].T
                xl_ref[cols, :] = near_ref[slot, 1].T
            ahead = row_16 - idx_ref[1:2, cols]
            line_y = pick(ahead, w_ref[1, :, cols])
            tile = -(ahead >> 4)
            ghost_y = jnp.where(tile[:8] == len_y // 16, line_y[:8], 0.0)
            tile_y = tile.astype(F32).astype(BF16)
            line_z = pick(row_16[:8] - idx_ref[2:3, cols], w_ref[2, :, cols], False)
            sides = [split_bf16(line_y * line_z[z:z + 1]) for z in planes]
            for r in range(len_y // 16):
                hit = tile_y == r
                for k, side in enumerate(sides):
                    first = k * len_y + 16 * r
                    ph_ref[slot, first:first + 16, :] = jnp.where(hit, side[0], zero_16)
                    pl_ref[slot, first:first + 16, :] = jnp.where(hit, side[1], zero_16)
            ghosts = [ghost_y * line_z[z:z + 1] for z in planes]
            if len(planes) % 2:
                ghosts.append(jnp.zeros((8, SUB), F32))
            high, low = split_bf16(jnp.concatenate(ghosts, axis=0))
            top = len(planes) * len_y
            rows = pl.ds(0, top + ghost_rows(group))
            ph_ref[slot, top:top + ghost_rows(group), :] = high
            pl_ref[slot, top:top + ghost_rows(group), :] = low
            if group == 0:
                part = dot3((ph_ref[slot, rows, :], pl_ref[slot, rows, :]), (near_ref[slot, 0], near_ref[slot, 1]), 1)
            else:
                part = dot3((ph_ref[slot, rows, :], pl_ref[slot, rows, :]), (xh_ref[cols, :], xl_ref[cols, :]))
            total = part if total is None else total + part
        acc_refs[group][...] += total

    def transform_send(group):
        planes = GROUPS[group]
        acc_ref, got_ref = acc_refs[group], got_refs[group]
        swap(group).wait()
        sign = (1 - 2 * my_y).astype(F32)
        peak = jnp.full((1, 1), 1e-30, F32)
        for first in range(0, len(planes), 2):
            count = min(2, len(planes) - first)
            for k in range(count):
                block = pl.ds((first + k) * len_y, len_y)
                ghost = pl.ds(len(planes) * len_y + 8 * (first + k), 8)
                even, odd = 2 * k * len_y, (2 * k + 1) * len_y
                grid_ref[pl.ds(even, len_y), :] = acc_ref[block, :] + got_ref[block, :]
                grid_ref[pl.ds(odd, len_y), :] = sign * (acc_ref[block, :] - got_ref[block, :])
                grid_ref[pl.ds(even, 8), :] += acc_ref[ghost, :] + got_ref[ghost, :]
                grid_ref[pl.ds(odd, 8), :] -= sign * (acc_ref[ghost, :] - got_ref[ghost, :])
            size = count * grid_n
            mid_ref[pl.ds(0, size), :] = dot3(split_bf16(grid_ref[pl.ds(0, size), :]), (tx_ref[0], tx_ref[1]))
            for parity in range(2):
                columns = [jnp.concatenate([mid_ref[pl.ds((2 * k + parity) * len_y, len_y), pl.ds(c * half, half)] for c in range(2)], axis=0) for k in range(count)]
                modes = dot3((ty_ref[parity, 0], ty_ref[parity, 1]), split_bf16(jnp.concatenate(columns, axis=1)))
                for block in range(4):
                    for k in range(count):
                        mode_ref[first + k, pl.ds(2 * block + parity, z_devs, stride=8), :] = modes[block * z_devs:(block + 1) * z_devs, k * half:(k + 1) * half]
                peak = jnp.maximum(peak, jnp.max(jnp.abs(modes), keepdims=True))
        power = jnp.ceil(jnp.log2(peak * (1.0 / CODE_MAX)) + 1e-3)
        gain = jnp.exp2(-power)
        for first in range(0, len(planes), 2):
            count = min(2, len(planes) - first)
            scaled = [(mode_ref[first + k] * gain).reshape(z_devs, 8, half) for k in range(count)]
            codes = jnp.round(jnp.concatenate(scaled, axis=1)).astype(jnp.int32).astype(jnp.int16)
            code_refs[group][:, pl.ds(8 * first, 8 * count), :] = codes
        code_refs[group][:, pl.ds(8 * len(planes), 2), :] = jnp.broadcast_to(power.astype(jnp.int32), (z_devs, 2, half)).astype(jnp.int16)

        def start(step):
            send(group, step).start()

        far_first(start)
        recv_refs[group][my_z] = code_refs[group][my_z]

    def await_all(ref, sem):
        pltpu.make_async_copy(ref, ref, sem).wait()

    def await_codes(group):
        await_all(recv_refs[group].at[pl.ds(0, z_devs - 1), used(group)], recv_sem.at[group])

    def decode(group, first, count):
        powers = recv_refs[group][:, pl.ds(8 * len(GROUPS[group]), 2), :].astype(jnp.int32).astype(F32)
        codes = recv_refs[group][:, pl.ds(8 * first, 8 * count), :].astype(jnp.int32).astype(F32)
        return codes * jnp.exp2(powers[:, :1, :])

    def fold(part, planes):
        rows = z_devs * 16
        flat = planes.reshape(rows, half)
        deq_ref[part, pl.ds(16, rows - 16), :] += flat[:rows - 16]
        deq_ref[part, pl.ds(0, 16), :] += flat[rows - 16:]

    def transform_z(part):
        flat = deq_ref.at[part]
        columns = [flat[pl.ds(ky, grid_n, stride=4), :] for ky in range(4)]
        return dot3((tz_ref[part, 0], tz_ref[part, 1]), split_bf16(jnp.concatenate(columns, axis=1)))

    for acc_ref in acc_refs:
        acc_ref[...] = jnp.zeros_like(acc_ref)
    for load in slot_loads(0):
        load.wait()
    for group in range(n_groups):
        @pl.loop(0, slots // CHUNK)
        def _(i):
            if group == 0:
                @pl.when(i == EARLY // CHUNK)
                def _():
                    for load in slot_loads(1):
                        load.wait()

            spread(group, i * CHUNK)
            if group:
                @pl.when(i == STEP_AT[group])
                def _():
                    transform_send(group - 1)

        if group == 0:
            pl.semaphore_wait(barrier, z_devs)
            for load in loads:
                load.wait()
        swap(group).start()
    transform_send(n_groups - 1)

    rows = z_devs * 16
    await_codes(0)
    for part in range(2):
        deq_ref[part] = decode(0, 2 * part, 2).reshape(rows, half)
    await_codes(1)
    fold(0, decode(1, 0, 2))
    zed_ref[...] = transform_z(0)
    zed_ref[...] += transform_z(1)
    await_codes(2)
    message = recv_refs[2][...].astype(jnp.int32).astype(F32)
    late_ref[...] = (message[:, :8] * jnp.exp2(message[:, 8:9])).reshape(z_devs * 8, half)
    row = jnp.zeros((8, half), F32)
    for pair in range(2):
        high, low = split_bf16(jnp.concatenate([late_ref[pl.ds(2 * pair + k, half, stride=4), :] for k in range(2)], axis=1))
        zed = zed_ref[:, pl.ds(pair * grid_n, grid_n)]
        zed += jnp.dot(tl_ref[:, pl.ds(0, grid_n)], jnp.concatenate([high, low], axis=0), preferred_element_type=F32)
        zed += jnp.dot(tl_ref[:, pl.ds(grid_n, half)], high, preferred_element_type=F32)
        power = zed[:grid_n] * zed[:grid_n] + zed[grid_n:] * zed[grid_n:]
        for k in range(2):
            for part in range(2):
                place = pl.ds(4 * part + 2 * pair + k, half, stride=8)
                value = bc_ref[place, :] * power[part * half:(part + 1) * half, k * half:(k + 1) * half].T
                ek_ref[place, :] = value
                row += jnp.sum(value.reshape(half // 8, 8, half), axis=0)
    row_ref[0] = jnp.broadcast_to(jnp.sum(row, axis=0, keepdims=True), (8, half))

    others = rrow_ref.at[pl.ds(0, z_devs - 1), pl.ds(0, 1)]
    pair = pltpu.make_async_remote_copy(src_ref=row_ref.at[0, pl.ds(0, 1)], dst_ref=row_ref.at[1, pl.ds(0, 1)], send_sem=row_sem.at[2], recv_sem=row_sem.at[3], device_id=partner, device_id_type=MESH)
    pair.start()
    pair.wait()
    row_ref[2] = row_ref[0] + row_ref[1]

    def start(step):
        pltpu.make_async_remote_copy(src_ref=row_ref.at[2, pl.ds(0, 1)], dst_ref=rrow_ref.at[my_z, pl.ds(0, 1)], send_sem=row_sem.at[0], recv_sem=row_sem.at[1], device_id={'zdom': chip(step)}, device_id_type=MESH).start()

    far_first(start)
    rrow_ref[my_z, pl.ds(0, 1)] = row_ref[2, pl.ds(0, 1)]
    await_all(others, row_sem.at[1])
    sum_ref[0] = jnp.sum(rrow_ref[:, pl.ds(0, 1), :]) * (0.5 / (grid_n * grid_n * grid_n))
    await_all(others, row_sem.at[0])
    for group in range(n_groups):
        await_all(code_refs[group].at[pl.ds(0, z_devs - 1), used(group)], send_sem.at[group])


def solution(mesh):
    y_devs = mesh.shape['ydom']
    z_devs = mesh.shape['zdom']
    slot_spec = P(('sys', 'ydom', 'zdom'))
    mode_spec = P(('sys', 'ydom'), 'zdom', None)

    def local_energy(charge, real_mask, grid_idx, spline_w, influence):
        grid_n = influence.shape[2]
        slots = charge.shape[0]
        half = grid_n // 2
        n_groups = len(GROUPS)
        table_x, table_y, table_z, late_z = dft_tables(grid_n, y_devs, z_devs)
        any_spec = pl.BlockSpec(memory_space=pl.ANY)
        rows = [len(GROUPS[g]) * (grid_n // y_devs) + ghost_rows(g) for g in range(n_groups)]
        codes = [pltpu.VMEM((z_devs, -(-(8 * len(planes) + 2) // 16) * 16, half), jnp.int16) for planes in GROUPS]
        tiles = jnp.swapaxes(influence.reshape(half, 4, 2, half), 1, 2).reshape(8 * half, half)
        mode_energy, energy = pl.pallas_call(
            functools.partial(energy_kernel, y_devs, z_devs),
            in_specs=[any_spec] * 9,
            out_specs=[pl.BlockSpec(memory_space=pltpu.VMEM), pl.BlockSpec(memory_space=pltpu.SMEM)],
            out_shape=[pltpu.VMEM((8 * half, half), F32), jax.ShapeDtypeStruct((1,), F32)],
            scratch_shapes=[
                pltpu.VMEM((1, slots), F32), pltpu.VMEM((1, slots), jnp.int32), pltpu.VMEM((3, slots), jnp.int32), pltpu.VMEM((3, 4, slots), F32),
                pltpu.VMEM((2, 2, grid_n, SUB), BF16), pltpu.VMEM((slots, grid_n), BF16), pltpu.VMEM((slots, grid_n), BF16),
                pltpu.VMEM((2, rows[0], SUB), BF16), pltpu.VMEM((2, rows[0], SUB), BF16),
                [pltpu.VMEM((r, grid_n), F32) for r in rows], [pltpu.VMEM((r, grid_n), F32) for r in rows],
                pltpu.VMEM((2 * grid_n, grid_n), F32), pltpu.VMEM((2 * grid_n, grid_n), F32), pltpu.VMEM((4, 2 * grid_n, half), F32),
                codes, codes,
                pltpu.VMEM((2, z_devs * 16, half), F32), pltpu.VMEM((2 * grid_n, 4 * half), F32),
                pltpu.VMEM((8 * half, half), F32),
                pltpu.VMEM(table_x.shape[1:], BF16), pltpu.VMEM(table_y.shape, BF16), pltpu.VMEM(table_z.shape, BF16), pltpu.VMEM(late_z.shape, BF16),
                pltpu.VMEM((z_devs * 8, half), F32),
                pltpu.VMEM((3, 8, 128), F32), pltpu.VMEM((z_devs, 8, 128), F32),
                pltpu.SemaphoreType.DMA((2, 4)), pltpu.SemaphoreType.DMA((5,)), pltpu.SemaphoreType.DMA((2, n_groups)),
                pltpu.SemaphoreType.DMA((n_groups,)), pltpu.SemaphoreType.DMA((n_groups,)),
                pltpu.SemaphoreType.DMA((4,)),
            ],
            compiler_params=pltpu.CompilerParams(collective_id=0, has_side_effects=True, vmem_limit_bytes=60 * 1024 * 1024),
            name="energy",
        )(charge.reshape(1, slots), real_mask.reshape(1, slots), grid_idx.T, jnp.transpose(spline_w, (1, 2, 0)), tiles, jnp.asarray(table_x), jnp.asarray(table_y), jnp.asarray(table_z), jnp.asarray(late_z))
        mode_energy = lax.optimization_barrier(0.5 * mode_energy)
        return jnp.swapaxes(mode_energy.reshape(half, 2, 4, half), 1, 2).reshape(influence.shape), energy

    return jax.shard_map(local_energy, mesh=mesh, in_specs=(slot_spec, slot_spec, P(('sys', 'ydom', 'zdom'), None), P(('sys', 'ydom', 'zdom'), None, None), mode_spec), out_specs=(mode_spec, P('sys')), check_vma=False)
```

```python
import functools
import math
import jax
import jax.numpy as jnp
import numpy as np
from jax import lax
from jax.experimental import pallas as pl
from jax.experimental.pallas import tpu as pltpu
from jax.sharding import PartitionSpec as P

F32 = jnp.float32
BF16 = jnp.bfloat16
SUB = 512
CHUNK = 2048
GROUPS = ((0, 1, 2, 3), (4, 5), (6,))
STEP_AT = (0, 2, 3)
EARLY = 2048
CODE_MAX = 32767.0
MESH = pl.DeviceIdType.MESH


def split_bf16(value):
    high = value.astype(BF16)
    return high, (value - high.astype(F32)).astype(BF16)


def dot3(lhs, rhs, rhs_dim=0):
    def dot(a, b):
        return lax.dot_general(a, b, (((1,), (rhs_dim,)), ((), ())), preferred_element_type=F32)
    return dot(lhs[0], rhs[0]) + dot(lhs[1], rhs[0]) + dot(lhs[0], rhs[1])


def pick(ahead, taps, wrap=True):
    place = ahead & 15 if wrap else ahead
    value = jnp.zeros(ahead.shape, F32)
    for t in range(4):
        value = jnp.where(place == t, taps[t:t + 1], value)
    return value


def np_split(value):
    value = np.asarray(value, np.float32)
    high = value.astype(BF16)
    return np.stack([high, (value - high.astype(np.float32)).astype(BF16)])


def dft_tables(grid_n, y_devs, z_devs):
    turn = 2.0 * np.pi / grid_n
    len_y, len_z = grid_n // y_devs, grid_n // z_devs
    x = np.arange(grid_n)
    freq = np.arange(grid_n)
    phase_x = (np.outer(x, freq) % grid_n) * turn
    table_x = np.stack([np_split(np.concatenate([np.cos(phase_x[:, i * len_y:(i + 1) * len_y]), -np.sin(phase_x[:, i * len_y:(i + 1) * len_y])], axis=1)) for i in range(y_devs)])
    table_y = []
    for parity in range(2):
        ky = (np.arange(z_devs)[None, :] * len_z + 2 * np.arange(2)[:, None] + parity).reshape(-1)
        phase_y = (np.outer(ky, np.arange(grid_n // 2)) % grid_n) * turn
        real = np.concatenate([np.cos(phase_y), np.sin(phase_y)], axis=1)
        imag = np.concatenate([-np.sin(phase_y), np.cos(phase_y)], axis=1)
        table_y.append(np_split(np.concatenate([real, imag], axis=0)))

    def z_table(first, count):
        pos = np.arange(z_devs)[:, None] * len_z + first + np.arange(count)[None, :]
        phase_z = ((freq[:, None, None] * pos[None]) % grid_n) * turn
        real = np.stack([np.cos(phase_z), np.sin(phase_z)], axis=3).reshape(grid_n, -1)
        imag = np.stack([-np.sin(phase_z), np.cos(phase_z)], axis=3).reshape(grid_n, -1)
        return np_split(np.concatenate([real, imag], axis=0))

    high, low = z_table(6, 1)
    late_z = np.concatenate([high, high, low], axis=1)
    return table_x, np.stack(table_y), np.stack([z_table(0, 2), z_table(2, 2)]), late_z


def ghost_rows(group):
    return -(-8 * len(GROUPS[group]) // 16) * 16


def energy_kernel(y_devs, z_devs, q_hbm, m_hbm, idx_hbm, w_hbm, bc_hbm, tx_hbm, ty_hbm, tz_hbm, tl_hbm, ek_ref, sum_ref,
                  q_ref, m_ref, idx_ref, w_ref, near_ref, xh_ref, xl_ref, ph_ref, pl_ref, acc_refs, got_refs, grid_ref, mid_ref, mode_ref,
                  code_refs, recv_refs,
                  deq_ref, zed_ref, bc_ref, tx_ref, ty_ref, tz_ref, tl_ref, late_ref, row_ref, rrow_ref,
                  early_sem, load_sem, swap_sem, send_sem, recv_sem, row_sem):
    my_y = lax.axis_index('ydom')
    my_z = lax.axis_index('zdom')
    grid_n = xh_ref.shape[1]
    slots = q_ref.shape[1]
    len_y = grid_n // y_devs
    half = grid_n // 2
    n_groups = len(GROUPS)
    barrier = pltpu.get_barrier_semaphore()
    partner = {'ydom': 1 - my_y}

    def chip(step):
        return (my_z + step) & (z_devs - 1)

    def far_first(start):
        pl.loop(z_devs // 2, z_devs)(start)
        pl.loop(1, z_devs // 2)(start)

    def slot_loads(piece):
        cols = pl.ds(0, EARLY) if piece == 0 else pl.ds(EARLY, slots - EARLY)
        return [pltpu.make_async_copy(hbm.at[lead + (cols,)], ref.at[lead + (cols,)], early_sem.at[piece, k])
                for k, (hbm, ref, lead) in enumerate(((q_hbm, q_ref, (slice(None),)), (m_hbm, m_ref, (slice(None),)), (idx_hbm, idx_ref, (slice(None),)), (w_hbm, w_ref, (slice(None), slice(None)))))]

    for piece in range(2):
        for load in slot_loads(piece):
            load.start()

    @pl.loop(1, z_devs)
    def _(step):
        for core in range(y_devs):
            pl.semaphore_signal(barrier, inc=1, device_id={'zdom': chip(step), 'ydom': core}, device_id_type=MESH)

    pl.semaphore_signal(barrier, inc=1, device_id=partner, device_id_type=MESH)

    loads = [pltpu.make_async_copy(tx_hbm.at[my_y], tx_ref, load_sem.at[0]), pltpu.make_async_copy(ty_hbm, ty_ref, load_sem.at[1]),
             pltpu.make_async_copy(tz_hbm, tz_ref, load_sem.at[2]), pltpu.make_async_copy(bc_hbm, bc_ref, load_sem.at[3]), pltpu.make_async_copy(tl_hbm, tl_ref, load_sem.at[4])]
    for load in loads:
        load.start()

    def swap(group):
        return pltpu.make_async_remote_copy(src_ref=acc_refs[group], dst_ref=got_refs[group], send_sem=swap_sem.at[0, group], recv_sem=swap_sem.at[1, group], device_id=partner, device_id_type=MESH)

    def used(group):
        return pl.ds(0, 8 * len(GROUPS[group]) + 2)

    def send(group, step):
        other = chip(step)
        return pltpu.make_async_remote_copy(src_ref=code_refs[group].at[other, used(group)], dst_ref=recv_refs[group].at[my_z, used(group)], send_sem=send_sem.at[group], recv_sem=recv_sem.at[group], device_id={'zdom': other}, device_id_type=MESH)

    def spread(group, base):
        planes = GROUPS[group]
        zero_16 = jnp.zeros((16, SUB), BF16)
        total = None
        for sub in range(CHUNK // SUB):
            slot = sub % 2
            cols = pl.ds(pl.multiple_of(base + sub * SUB, SUB), SUB)
            row_16 = lax.broadcasted_iota(jnp.int32, (16, SUB), 0)
            if group == 0:
                weight = q_ref[:, cols] * m_ref[:, cols].astype(F32)
                ahead = row_16 - idx_ref[0:1, cols]
                taps = w_ref[0, :, cols] * weight
                high, low = split_bf16(pick(ahead, taps))
                tile_x = (-(ahead >> 4) & 15).astype(F32).astype(BF16)
                for r in range(grid_n // 16):
                    hit = tile_x == r
                    near_ref[slot, 0, 16 * r:16 * r + 16, :] = jnp.where(hit, high, zero_16)
                    near_ref[slot, 1, 16 * r:16 * r + 16, :] = jnp.where(hit, low, zero_16)
                xh_ref[cols, :] = near_ref[slot, 0].T
                xl_ref[cols, :] = near_ref[slot, 1].T
            ahead = row_16 - idx_ref[1:2, cols]
            line_y = pick(ahead, w_ref[1, :, cols])
            tile = -(ahead >> 4)
            ghost_y = jnp.where(tile[:8] == len_y // 16, line_y[:8], 0.0)
            tile_y = tile.astype(F32).astype(BF16)
            line_z = pick(row_16[:8] - idx_ref[2:3, cols], w_ref[2, :, cols], False)
            sides = [split_bf16(line_y * line_z[z:z + 1]) for z in planes]
            for r in range(len_y // 16):
                hit = tile_y == r
                for k, side in enumerate(sides):
                    first = k * len_y + 16 * r
                    ph_ref[slot, first:first + 16, :] = jnp.where(hit, side[0], zero_16)
                    pl_ref[slot, first:first + 16, :] = jnp.where(hit, side[1], zero_16)
            ghosts = [ghost_y * line_z[z:z + 1] for z in planes]
            if len(planes) % 2:
                ghosts.append(jnp.zeros((8, SUB), F32))
            high, low = split_bf16(jnp.concatenate(ghosts, axis=0))
            top = len(planes) * len_y
            rows = pl.ds(0, top + ghost_rows(group))
            ph_ref[slot, top:top + ghost_rows(group), :] = high
            pl_ref[slot, top:top + ghost_rows(group), :] = low
            if group == 0:
                part = dot3((ph_ref[slot, rows, :], pl_ref[slot, rows, :]), (near_ref[slot, 0], near_ref[slot, 1]), 1)
            else:
                part = dot3((ph_ref[slot, rows, :], pl_ref[slot, rows, :]), (xh_ref[cols, :], xl_ref[cols, :]))
            total = part if total is None else total + part
        acc_refs[group][...] += total

    def transform_send(group):
        planes = GROUPS[group]
        acc_ref, got_ref = acc_refs[group], got_refs[group]
        swap(group).wait()
        sign = (1 - 2 * my_y).astype(F32)
        peak = jnp.full((1, 1), 1e-30, F32)
        for first in range(0, len(planes), 2):
            count = min(2, len(planes) - first)
            for k in range(count):
                block = pl.ds((first + k) * len_y, len_y)
                ghost = pl.ds(len(planes) * len_y + 8 * (first + k), 8)
                even, odd = 2 * k * len_y, (2 * k + 1) * len_y
                grid_ref[pl.ds(even, len_y), :] = acc_ref[block, :] + got_ref[block, :]
                grid_ref[pl.ds(odd, len_y), :] = sign * (acc_ref[block, :] - got_ref[block, :])
                grid_ref[pl.ds(even, 8), :] += acc_ref[ghost, :] + got_ref[ghost, :]
                grid_ref[pl.ds(odd, 8), :] -= sign * (acc_ref[ghost, :] - got_ref[ghost, :])
            size = count * grid_n
            mid_ref[pl.ds(0, size), :] = dot3(split_bf16(grid_ref[pl.ds(0, size), :]), (tx_ref[0], tx_ref[1]))
            for parity in range(2):
                columns = [jnp.concatenate([mid_ref[pl.ds((2 * k + parity) * len_y, len_y), pl.ds(c * half, half)] for c in range(2)], axis=0) for k in range(count)]
                modes = dot3((ty_ref[parity, 0], ty_ref[parity, 1]), split_bf16(jnp.concatenate(columns, axis=1)))
                for block in range(4):
                    for k in range(count):
                        mode_ref[first + k, pl.ds(2 * block + parity, z_devs, stride=8), :] = modes[block * z_devs:(block + 1) * z_devs, k * half:(k + 1) * half]
                peak = jnp.maximum(peak, jnp.max(jnp.abs(modes), keepdims=True))
        power = jnp.ceil(jnp.log2(peak * (1.0 / CODE_MAX)) + 1e-3)
        gain = jnp.exp2(-power)
        for first in range(0, len(planes), 2):
            count = min(2, len(planes) - first)
            scaled = [(mode_ref[first + k] * gain).reshape(z_devs, 8, half) for k in range(count)]
            codes = jnp.round(jnp.concatenate(scaled, axis=1)).astype(jnp.int32).astype(jnp.int16)
            code_refs[group][:, pl.ds(8 * first, 8 * count), :] = codes
        code_refs[group][:, pl.ds(8 * len(planes), 2), :] = jnp.broadcast_to(power.astype(jnp.int32), (z_devs, 2, half)).astype(jnp.int16)

        def start(step):
            send(group, step).start()

        far_first(start)
        recv_refs[group][my_z] = code_refs[group][my_z]

    def await_all(ref, sem):
        pltpu.make_async_copy(ref, ref, sem).wait()

    def await_codes(group):
        await_all(recv_refs[group].at[pl.ds(0, z_devs - 1), used(group)], recv_sem.at[group])

    def decode(group, first, count):
        powers = recv_refs[group][:, pl.ds(8 * len(GROUPS[group]), 2), :].astype(jnp.int32).astype(F32)
        codes = recv_refs[group][:, pl.ds(8 * first, 8 * count), :].astype(jnp.int32).astype(F32)
        return codes * jnp.exp2(powers[:, :1, :])

    def fold(part, planes):
        rows = z_devs * 16
        flat = planes.reshape(rows, half)
        deq_ref[part, pl.ds(16, rows - 16), :] += flat[:rows - 16]
        deq_ref[part, pl.ds(0, 16), :] += flat[rows - 16:]

    def transform_z(part):
        flat = deq_ref.at[part]
        columns = [flat[pl.ds(ky, grid_n, stride=4), :] for ky in range(4)]
        return dot3((tz_ref[part, 0], tz_ref[part, 1]), split_bf16(jnp.concatenate(columns, axis=1)))

    for acc_ref in acc_refs:
        acc_ref[...] = jnp.zeros_like(acc_ref)
    for load in slot_loads(0):
        load.wait()
    for group in range(n_groups):
        @pl.loop(0, slots // CHUNK)
        def _(i):
            if group == 0:
                @pl.when(i == EARLY // CHUNK)
                def _():
                    for load in slot_loads(1):
                        load.wait()

            spread(group, i * CHUNK)
            if group:
                @pl.when(i == STEP_AT[group])
                def _():
                    transform_send(group - 1)

        if group == 0:
            pl.semaphore_wait(barrier, y_devs * z_devs - 1)
            for load in loads:
                load.wait()
        swap(group).start()
    transform_send(n_groups - 1)

    rows = z_devs * 16
    await_codes(0)
    for part in range(2):
        deq_ref[part] = decode(0, 2 * part, 2).reshape(rows, half)
    await_codes(1)
    fold(0, decode(1, 0, 2))
    zed_ref[...] = transform_z(0)
    zed_ref[...] += transform_z(1)
    await_codes(2)
    message = recv_refs[2][...].astype(jnp.int32).astype(F32)
    late_ref[...] = (message[:, :8] * jnp.exp2(message[:, 8:9])).reshape(z_devs * 8, half)
    row = jnp.zeros((8, half), F32)
    for pair in range(2):
        high, low = split_bf16(jnp.concatenate([late_ref[pl.ds(2 * pair + k, half, stride=4), :] for k in range(2)], axis=1))
        zed = zed_ref[:, pl.ds(pair * grid_n, grid_n)]
        zed += jnp.dot(tl_ref[:, pl.ds(0, grid_n)], jnp.concatenate([high, low], axis=0), preferred_element_type=F32)
        zed += jnp.dot(tl_ref[:, pl.ds(grid_n, half)], high, preferred_element_type=F32)
        power = zed[:grid_n] * zed[:grid_n] + zed[grid_n:] * zed[grid_n:]
        for k in range(2):
            for part in range(2):
                place = pl.ds(4 * part + 2 * pair + k, half, stride=8)
                value = bc_ref[place, :] * power[part * half:(part + 1) * half, k * half:(k + 1) * half].T
                ek_ref[place, :] = value
                row += jnp.sum(value.reshape(half // 8, 8, half), axis=0)
    row_ref[0] = jnp.broadcast_to(jnp.sum(row, axis=0, keepdims=True), (8, half))

    me = my_z * y_devs + my_y
    others = rrow_ref.at[pl.ds(0, y_devs * z_devs - 1), pl.ds(0, 1)]

    def row_copy(device):
        return pltpu.make_async_remote_copy(src_ref=row_ref.at[0, pl.ds(0, 1)], dst_ref=rrow_ref.at[me, pl.ds(0, 1)], send_sem=row_sem.at[0], recv_sem=row_sem.at[1], device_id=device, device_id_type=MESH)

    def start(step):
        for core in range(y_devs):
            row_copy({'zdom': chip(step), 'ydom': core}).start()

    far_first(start)
    row_copy(partner).start()
    rrow_ref[me, pl.ds(0, 1)] = row_ref[0, pl.ds(0, 1)]
    await_all(others, row_sem.at[1])
    sum_ref[0] = jnp.sum(rrow_ref[:, pl.ds(0, 1), :]) * (0.5 / (grid_n * grid_n * grid_n))
    await_all(others, row_sem.at[0])
    for group in range(n_groups):
        await_all(code_refs[group].at[pl.ds(0, z_devs - 1), used(group)], send_sem.at[group])


def solution(mesh):
    y_devs = mesh.shape['ydom']
    z_devs = mesh.shape['zdom']
    slot_spec = P(('sys', 'ydom', 'zdom'))
    mode_spec = P(('sys', 'ydom'), 'zdom', None)

    def local_energy(charge, real_mask, grid_idx, spline_w, influence):
        grid_n = influence.shape[2]
        slots = charge.shape[0]
        half = grid_n // 2
        n_groups = len(GROUPS)
        table_x, table_y, table_z, late_z = dft_tables(grid_n, y_devs, z_devs)
        any_spec = pl.BlockSpec(memory_space=pl.ANY)
        rows = [len(GROUPS[g]) * (grid_n // y_devs) + ghost_rows(g) for g in range(n_groups)]
        codes = [pltpu.VMEM((z_devs, -(-(8 * len(planes) + 2) // 16) * 16, half), jnp.int16) for planes in GROUPS]
        tiles = jnp.swapaxes(influence.reshape(half, 4, 2, half), 1, 2).reshape(8 * half, half)
        mode_energy, energy = pl.pallas_call(
            functools.partial(energy_kernel, y_devs, z_devs),
            in_specs=[any_spec] * 9,
            out_specs=[pl.BlockSpec(memory_space=pltpu.VMEM), pl.BlockSpec(memory_space=pltpu.SMEM)],
            out_shape=[pltpu.VMEM((8 * half, half), F32), jax.ShapeDtypeStruct((1,), F32)],
            scratch_shapes=[
                pltpu.VMEM((1, slots), F32), pltpu.VMEM((1, slots), jnp.int32), pltpu.VMEM((3, slots), jnp.int32), pltpu.VMEM((3, 4, slots), F32),
                pltpu.VMEM((2, 2, grid_n, SUB), BF16), pltpu.VMEM((slots, grid_n), BF16), pltpu.VMEM((slots, grid_n), BF16),
                pltpu.VMEM((2, rows[0], SUB), BF16), pltpu.VMEM((2, rows[0], SUB), BF16),
                [pltpu.VMEM((r, grid_n), F32) for r in rows], [pltpu.VMEM((r, grid_n), F32) for r in rows],
                pltpu.VMEM((2 * grid_n, grid_n), F32), pltpu.VMEM((2 * grid_n, grid_n), F32), pltpu.VMEM((4, 2 * grid_n, half), F32),
                codes, codes,
                pltpu.VMEM((2, z_devs * 16, half), F32), pltpu.VMEM((2 * grid_n, 4 * half), F32),
                pltpu.VMEM((8 * half, half), F32),
                pltpu.VMEM(table_x.shape[1:], BF16), pltpu.VMEM(table_y.shape, BF16), pltpu.VMEM(table_z.shape, BF16), pltpu.VMEM(late_z.shape, BF16),
                pltpu.VMEM((z_devs * 8, half), F32),
                pltpu.VMEM((3, 8, 128), F32), pltpu.VMEM((y_devs * z_devs, 8, 128), F32),
                pltpu.SemaphoreType.DMA((2, 4)), pltpu.SemaphoreType.DMA((5,)), pltpu.SemaphoreType.DMA((2, n_groups)),
                pltpu.SemaphoreType.DMA((n_groups,)), pltpu.SemaphoreType.DMA((n_groups,)),
                pltpu.SemaphoreType.DMA((4,)),
            ],
            compiler_params=pltpu.CompilerParams(collective_id=0, has_side_effects=True, vmem_limit_bytes=60 * 1024 * 1024),
            name="energy",
        )(charge.reshape(1, slots), real_mask.reshape(1, slots), grid_idx.T, jnp.transpose(spline_w, (1, 2, 0)), tiles, jnp.asarray(table_x), jnp.asarray(table_y), jnp.asarray(table_z), jnp.asarray(late_z))
        mode_energy = lax.optimization_barrier(0.5 * mode_energy)
        return jnp.swapaxes(mode_energy.reshape(half, 2, 4, half), 1, 2).reshape(influence.shape), energy

    return jax.shard_map(local_energy, mesh=mesh, in_specs=(slot_spec, slot_spec, P(('sys', 'ydom', 'zdom'), None), P(('sys', 'ydom', 'zdom'), None, None), mode_spec), out_specs=(mode_spec, P('sys')), check_vma=False)
```

```python
import functools
import math
import jax
import jax.numpy as jnp
import numpy as np
from jax import lax
from jax.experimental import pallas as pl
from jax.experimental.pallas import tpu as pltpu
from jax.sharding import PartitionSpec as P

F32 = jnp.float32
BF16 = jnp.bfloat16
SUB = 512
CHUNK = 2048
GROUPS = ((0, 1, 2, 3), (4, 5), (6,))
STEP_AT = (0, 2, 3)
EARLY = 2048
CODE_MAX = 32767.0
MESH = pl.DeviceIdType.MESH


def split_bf16(value):
    high = value.astype(BF16)
    return high, (value - high.astype(F32)).astype(BF16)


def dot3(lhs, rhs, rhs_dim=0):
    def dot(a, b):
        return lax.dot_general(a, b, (((1,), (rhs_dim,)), ((), ())), preferred_element_type=F32)
    return dot(lhs[0], rhs[0]) + dot(lhs[1], rhs[0]) + dot(lhs[0], rhs[1])


def pick(ahead, taps, wrap=True):
    place = ahead & 15 if wrap else ahead
    value = jnp.zeros(ahead.shape, F32)
    for t in range(4):
        value = jnp.where(place == t, taps[t:t + 1], value)
    return value


def np_split(value):
    value = np.asarray(value, np.float32)
    high = value.astype(BF16)
    return np.stack([high, (value - high.astype(np.float32)).astype(BF16)])


def dft_tables(grid_n, y_devs, z_devs):
    turn = 2.0 * np.pi / grid_n
    len_y, len_z = grid_n // y_devs, grid_n // z_devs
    x = np.arange(grid_n)
    freq = np.arange(grid_n)
    phase_x = (np.outer(x, freq) % grid_n) * turn
    table_x = np.stack([np_split(np.concatenate([np.cos(phase_x[:, i * len_y:(i + 1) * len_y]), -np.sin(phase_x[:, i * len_y:(i + 1) * len_y])], axis=1)) for i in range(y_devs)])
    table_y = []
    for parity in range(2):
        ky = (np.arange(z_devs)[None, :] * len_z + 2 * np.arange(2)[:, None] + parity).reshape(-1)
        phase_y = (np.outer(ky, np.arange(grid_n // 2)) % grid_n) * turn
        real = np.concatenate([np.cos(phase_y), np.sin(phase_y)], axis=1)
        imag = np.concatenate([-np.sin(phase_y), np.cos(phase_y)], axis=1)
        table_y.append(np_split(np.concatenate([real, imag], axis=0)))

    def z_table(first, count):
        pos = np.arange(z_devs)[:, None] * len_z + first + np.arange(count)[None, :]
        phase_z = ((freq[:, None, None] * pos[None]) % grid_n) * turn
        real = np.stack([np.cos(phase_z), np.sin(phase_z)], axis=3).reshape(grid_n, -1)
        imag = np.stack([-np.sin(phase_z), np.cos(phase_z)], axis=3).reshape(grid_n, -1)
        return np_split(np.concatenate([real, imag], axis=0))

    high, low = z_table(6, 1)
    late_z = np.concatenate([high, high, low], axis=1)
    return table_x, np.stack(table_y), np.stack([z_table(0, 2), z_table(2, 2)]), late_z


def ghost_rows(group):
    return -(-8 * len(GROUPS[group]) // 16) * 16


def energy_kernel(y_devs, z_devs, q_hbm, m_hbm, idx_hbm, w_hbm, bc_hbm, tx_hbm, ty_hbm, tz_hbm, tl_hbm, ek_ref, sum_ref,
                  q_ref, m_ref, idx_ref, w_ref, near_ref, xh_ref, xl_ref, ph_ref, pl_ref, acc_refs, got_refs, grid_ref, mid_ref, mode_ref,
                  code_refs, recv_refs,
                  deq_ref, zed_ref, bc_ref, tx_ref, ty_ref, tz_ref, tl_ref, late_ref, row_ref, rrow_ref,
                  early_sem, load_sem, swap_sem, send_sem, recv_sem, row_sem):
    my_y = lax.axis_index('ydom')
    my_z = lax.axis_index('zdom')
    grid_n = xh_ref.shape[1]
    slots = q_ref.shape[1]
    len_y = grid_n // y_devs
    half = grid_n // 2
    n_groups = len(GROUPS)
    barrier = pltpu.get_barrier_semaphore()
    partner = {'ydom': 1 - my_y}

    def chip(step):
        return (my_z + step) & (z_devs - 1)

    def far_first(start):
        pl.loop(z_devs // 2, z_devs)(start)
        pl.loop(1, z_devs // 2)(start)

    def slot_loads(piece):
        cols = pl.ds(0, EARLY) if piece == 0 else pl.ds(EARLY, slots - EARLY)
        return [pltpu.make_async_copy(hbm.at[lead + (cols,)], ref.at[lead + (cols,)], early_sem.at[piece, k])
                for k, (hbm, ref, lead) in enumerate(((q_hbm, q_ref, (slice(None),)), (m_hbm, m_ref, (slice(None),)), (idx_hbm, idx_ref, (slice(None),)), (w_hbm, w_ref, (slice(None), slice(None)))))]

    for load in slot_loads(0):
        load.start()

    @pl.loop(1, z_devs)
    def _(step):
        for core in range(y_devs):
            pl.semaphore_signal(barrier, inc=1, device_id={'zdom': chip(step), 'ydom': core}, device_id_type=MESH)

    pl.semaphore_signal(barrier, inc=1, device_id=partner, device_id_type=MESH)

    loads = [pltpu.make_async_copy(tx_hbm.at[my_y], tx_ref, load_sem.at[0]), pltpu.make_async_copy(ty_hbm, ty_ref, load_sem.at[1]),
             pltpu.make_async_copy(tz_hbm, tz_ref, load_sem.at[2]), pltpu.make_async_copy(bc_hbm, bc_ref, load_sem.at[3]), pltpu.make_async_copy(tl_hbm, tl_ref, load_sem.at[4])]
    for load in slot_loads(1) + loads:
        load.start()

    def swap(group):
        return pltpu.make_async_remote_copy(src_ref=acc_refs[group], dst_ref=got_refs[group], send_sem=swap_sem.at[0, group], recv_sem=swap_sem.at[1, group], device_id=partner, device_id_type=MESH)

    def used(group):
        return pl.ds(0, 8 * len(GROUPS[group]) + 2)

    def send(group, step):
        other = chip(step)
        return pltpu.make_async_remote_copy(src_ref=code_refs[group].at[other, used(group)], dst_ref=recv_refs[group].at[my_z, used(group)], send_sem=send_sem.at[group], recv_sem=recv_sem.at[group], device_id={'zdom': other}, device_id_type=MESH)

    def spread(group, base):
        planes = GROUPS[group]
        zero_16 = jnp.zeros((16, SUB), BF16)
        total = None
        for sub in range(CHUNK // SUB):
            slot = sub % 2
            cols = pl.ds(pl.multiple_of(base + sub * SUB, SUB), SUB)
            row_16 = lax.broadcasted_iota(jnp.int32, (16, SUB), 0)
            if group == 0:
                weight = q_ref[:, cols] * m_ref[:, cols].astype(F32)
                ahead = row_16 - idx_ref[0:1, cols]
                taps = w_ref[0, :, cols] * weight
                high, low = split_bf16(pick(ahead, taps))
                tile_x = (-(ahead >> 4) & 15).astype(F32).astype(BF16)
                for r in range(grid_n // 16):
                    hit = tile_x == r
                    near_ref[slot, 0, 16 * r:16 * r + 16, :] = jnp.where(hit, high, zero_16)
                    near_ref[slot, 1, 16 * r:16 * r + 16, :] = jnp.where(hit, low, zero_16)
                xh_ref[cols, :] = near_ref[slot, 0].T
                xl_ref[cols, :] = near_ref[slot, 1].T
            ahead = row_16 - idx_ref[1:2, cols]
            line_y = pick(ahead, w_ref[1, :, cols])
            tile = -(ahead >> 4)
            ghost_y = jnp.where(tile[:8] == len_y // 16, line_y[:8], 0.0)
            tile_y = tile.astype(F32).astype(BF16)
            line_z = pick(row_16[:8] - idx_ref[2:3, cols], w_ref[2, :, cols], False)
            sides = [split_bf16(line_y * line_z[z:z + 1]) for z in planes]
            for r in range(len_y // 16):
                hit = tile_y == r
                for k, side in enumerate(sides):
                    first = k * len_y + 16 * r
                    ph_ref[slot, first:first + 16, :] = jnp.where(hit, side[0], zero_16)
                    pl_ref[slot, first:first + 16, :] = jnp.where(hit, side[1], zero_16)
            ghosts = [ghost_y * line_z[z:z + 1] for z in planes]
            if len(planes) % 2:
                ghosts.append(jnp.zeros((8, SUB), F32))
            high, low = split_bf16(jnp.concatenate(ghosts, axis=0))
            top = len(planes) * len_y
            rows = pl.ds(0, top + ghost_rows(group))
            ph_ref[slot, top:top + ghost_rows(group), :] = high
            pl_ref[slot, top:top + ghost_rows(group), :] = low
            if group == 0:
                part = dot3((ph_ref[slot, rows, :], pl_ref[slot, rows, :]), (near_ref[slot, 0], near_ref[slot, 1]), 1)
            else:
                part = dot3((ph_ref[slot, rows, :], pl_ref[slot, rows, :]), (xh_ref[cols, :], xl_ref[cols, :]))
            total = part if total is None else total + part
        acc_refs[group][...] += total

    def transform_send(group):
        planes = GROUPS[group]
        acc_ref, got_ref = acc_refs[group], got_refs[group]
        swap(group).wait()
        sign = (1 - 2 * my_y).astype(F32)
        peak = jnp.full((1, 1), 1e-30, F32)
        for first in range(0, len(planes), 2):
            count = min(2, len(planes) - first)
            for k in range(count):
                block = pl.ds((first + k) * len_y, len_y)
                ghost = pl.ds(len(planes) * len_y + 8 * (first + k), 8)
                even, odd = 2 * k * len_y, (2 * k + 1) * len_y
                grid_ref[first // 2, pl.ds(even, len_y), :] = acc_ref[block, :] + got_ref[block, :]
                grid_ref[first // 2, pl.ds(odd, len_y), :] = sign * (acc_ref[block, :] - got_ref[block, :])
                grid_ref[first // 2, pl.ds(even, 8), :] += acc_ref[ghost, :] + got_ref[ghost, :]
                grid_ref[first // 2, pl.ds(odd, 8), :] -= sign * (acc_ref[ghost, :] - got_ref[ghost, :])
            size = count * grid_n
            mid_ref[first // 2, pl.ds(0, size), :] = dot3(split_bf16(grid_ref[first // 2, pl.ds(0, size), :]), (tx_ref[0], tx_ref[1]))
            for parity in range(2):
                columns = [jnp.concatenate([mid_ref[first // 2, pl.ds((2 * k + parity) * len_y, len_y), pl.ds(c * half, half)] for c in range(2)], axis=0) for k in range(count)]
                modes = dot3((ty_ref[parity, 0], ty_ref[parity, 1]), split_bf16(jnp.concatenate(columns, axis=1)))
                for block in range(4):
                    for k in range(count):
                        mode_ref[first + k, pl.ds(2 * block + parity, z_devs, stride=8), :] = modes[block * z_devs:(block + 1) * z_devs, k * half:(k + 1) * half]
                peak = jnp.maximum(peak, jnp.max(jnp.abs(modes), keepdims=True))
        power = jnp.ceil(jnp.log2(peak * (1.0 / CODE_MAX)) + 1e-3)
        gain = jnp.exp2(-power)
        for first in range(0, len(planes), 2):
            count = min(2, len(planes) - first)
            scaled = [(mode_ref[first + k] * gain).reshape(z_devs, 8, half) for k in range(count)]
            codes = jnp.round(jnp.concatenate(scaled, axis=1)).astype(jnp.int32).astype(jnp.int16)
            code_refs[group][:, pl.ds(8 * first, 8 * count), :] = codes
        code_refs[group][:, pl.ds(8 * len(planes), 2), :] = jnp.broadcast_to(power.astype(jnp.int32), (z_devs, 2, half)).astype(jnp.int16)

        def start(step):
            send(group, step).start()

        far_first(start)
        recv_refs[group][my_z] = code_refs[group][my_z]

    def await_all(ref, sem):
        pltpu.make_async_copy(ref, ref, sem).wait()

    def await_codes(group):
        await_all(recv_refs[group].at[pl.ds(0, z_devs - 1), used(group)], recv_sem.at[group])

    def decode(group, first, count):
        powers = recv_refs[group][:, pl.ds(8 * len(GROUPS[group]), 2), :].astype(jnp.int32).astype(F32)
        codes = recv_refs[group][:, pl.ds(8 * first, 8 * count), :].astype(jnp.int32).astype(F32)
        return codes * jnp.exp2(powers[:, :1, :])

    def fold(part, planes):
        rows = z_devs * 16
        flat = planes.reshape(rows, half)
        deq_ref[part, pl.ds(16, rows - 16), :] += flat[:rows - 16]
        deq_ref[part, pl.ds(0, 16), :] += flat[rows - 16:]

    def transform_z(part):
        flat = deq_ref.at[part]
        columns = [flat[pl.ds(ky, grid_n, stride=4), :] for ky in range(4)]
        return dot3((tz_ref[part, 0], tz_ref[part, 1]), split_bf16(jnp.concatenate(columns, axis=1)))

    for acc_ref in acc_refs:
        acc_ref[...] = jnp.zeros_like(acc_ref)
    for load in slot_loads(0):
        load.wait()
    for group in range(n_groups):
        @pl.loop(0, slots // CHUNK)
        def _(i):
            if group == 0:
                @pl.when(i == EARLY // CHUNK)
                def _():
                    for load in slot_loads(1):
                        load.wait()

            spread(group, i * CHUNK)
            if group:
                @pl.when(i == STEP_AT[group])
                def _():
                    transform_send(group - 1)

        if group == 0:
            pl.semaphore_wait(barrier, y_devs * z_devs - 1)
            for load in loads:
                load.wait()
        swap(group).start()
    transform_send(n_groups - 1)

    rows = z_devs * 16
    await_codes(0)
    for part in range(2):
        deq_ref[part] = decode(0, 2 * part, 2).reshape(rows, half)
    await_codes(1)
    fold(0, decode(1, 0, 2))
    zed_ref[...] = transform_z(0)
    zed_ref[...] += transform_z(1)
    await_codes(2)
    message = recv_refs[2][...].astype(jnp.int32).astype(F32)
    late_ref[...] = (message[:, :8] * jnp.exp2(message[:, 8:9])).reshape(z_devs * 8, half)
    row = jnp.zeros((8, half), F32)
    for pair in range(2):
        high, low = split_bf16(jnp.concatenate([late_ref[pl.ds(2 * pair + k, half, stride=4), :] for k in range(2)], axis=1))
        zed = zed_ref[:, pl.ds(pair * grid_n, grid_n)]
        zed += jnp.dot(tl_ref[:, pl.ds(0, grid_n)], jnp.concatenate([high, low], axis=0), preferred_element_type=F32)
        zed += jnp.dot(tl_ref[:, pl.ds(grid_n, half)], high, preferred_element_type=F32)
        power = zed[:grid_n] * zed[:grid_n] + zed[grid_n:] * zed[grid_n:]
        for k in range(2):
            for part in range(2):
                place = pl.ds(4 * part + 2 * pair + k, half, stride=8)
                value = bc_ref[place, :] * power[part * half:(part + 1) * half, k * half:(k + 1) * half].T
                ek_ref[place, :] = value
                row += jnp.sum(value.reshape(half // 8, 8, half), axis=0)
    row_ref[0] = jnp.broadcast_to(jnp.sum(row, axis=0, keepdims=True), (8, half))

    me = my_z * y_devs + my_y
    others = rrow_ref.at[pl.ds(0, y_devs * z_devs - 1), pl.ds(0, 1)]

    def row_copy(device):
        return pltpu.make_async_remote_copy(src_ref=row_ref.at[0, pl.ds(0, 1)], dst_ref=rrow_ref.at[me, pl.ds(0, 1)], send_sem=row_sem.at[0], recv_sem=row_sem.at[1], device_id=device, device_id_type=MESH)

    def start(step):
        for core in range(y_devs):
            row_copy({'zdom': chip(step), 'ydom': core}).start()

    far_first(start)
    row_copy(partner).start()
    rrow_ref[me, pl.ds(0, 1)] = row_ref[0, pl.ds(0, 1)]
    await_all(others, row_sem.at[1])
    sum_ref[0] = jnp.sum(rrow_ref[:, pl.ds(0, 1), :]) * (0.5 / (grid_n * grid_n * grid_n))
    await_all(others, row_sem.at[0])
    for group in range(n_groups):
        await_all(code_refs[group].at[pl.ds(0, z_devs - 1), used(group)], send_sem.at[group])


def solution(mesh):
    y_devs = mesh.shape['ydom']
    z_devs = mesh.shape['zdom']
    slot_spec = P(('sys', 'ydom', 'zdom'))
    mode_spec = P(('sys', 'ydom'), 'zdom', None)

    def local_energy(charge, real_mask, grid_idx, spline_w, influence):
        grid_n = influence.shape[2]
        slots = charge.shape[0]
        half = grid_n // 2
        n_groups = len(GROUPS)
        table_x, table_y, table_z, late_z = dft_tables(grid_n, y_devs, z_devs)
        any_spec = pl.BlockSpec(memory_space=pl.ANY)
        rows = [len(GROUPS[g]) * (grid_n // y_devs) + ghost_rows(g) for g in range(n_groups)]
        codes = [pltpu.VMEM((z_devs, -(-(8 * len(planes) + 2) // 16) * 16, half), jnp.int16) for planes in GROUPS]
        tiles = jnp.swapaxes(influence.reshape(half, 4, 2, half), 1, 2).reshape(8 * half, half)
        mode_energy, energy = pl.pallas_call(
            functools.partial(energy_kernel, y_devs, z_devs),
            in_specs=[any_spec] * 9,
            out_specs=[pl.BlockSpec(memory_space=pltpu.VMEM), pl.BlockSpec(memory_space=pltpu.SMEM)],
            out_shape=[pltpu.VMEM((8 * half, half), F32), jax.ShapeDtypeStruct((1,), F32)],
            scratch_shapes=[
                pltpu.VMEM((1, slots), F32), pltpu.VMEM((1, slots), jnp.int32), pltpu.VMEM((3, slots), jnp.int32), pltpu.VMEM((3, 4, slots), F32),
                pltpu.VMEM((2, 2, grid_n, SUB), BF16), pltpu.VMEM((slots, grid_n), BF16), pltpu.VMEM((slots, grid_n), BF16),
                pltpu.VMEM((2, rows[0], SUB), BF16), pltpu.VMEM((2, rows[0], SUB), BF16),
                [pltpu.VMEM((r, grid_n), F32) for r in rows], [pltpu.VMEM((r, grid_n), F32) for r in rows],
                pltpu.VMEM((2, 2 * grid_n, grid_n), F32), pltpu.VMEM((2, 2 * grid_n, grid_n), F32), pltpu.VMEM((4, 2 * grid_n, half), F32),
                codes, codes,
                pltpu.VMEM((2, z_devs * 16, half), F32), pltpu.VMEM((2 * grid_n, 4 * half), F32),
                pltpu.VMEM((8 * half, half), F32),
                pltpu.VMEM(table_x.shape[1:], BF16), pltpu.VMEM(table_y.shape, BF16), pltpu.VMEM(table_z.shape, BF16), pltpu.VMEM(late_z.shape, BF16),
                pltpu.VMEM((z_devs * 8, half), F32),
                pltpu.VMEM((3, 8, 128), F32), pltpu.VMEM((y_devs * z_devs, 8, 128), F32),
                pltpu.SemaphoreType.DMA((2, 4)), pltpu.SemaphoreType.DMA((5,)), pltpu.SemaphoreType.DMA((2, n_groups)),
                pltpu.SemaphoreType.DMA((n_groups,)), pltpu.SemaphoreType.DMA((n_groups,)),
                pltpu.SemaphoreType.DMA((4,)),
            ],
            compiler_params=pltpu.CompilerParams(collective_id=0, has_side_effects=True, vmem_limit_bytes=60 * 1024 * 1024),
            name="energy",
        )(charge.reshape(1, slots), real_mask.reshape(1, slots), grid_idx.T, jnp.transpose(spline_w, (1, 2, 0)), tiles, jnp.asarray(table_x), jnp.asarray(table_y), jnp.asarray(table_z), jnp.asarray(late_z))
        mode_energy = lax.optimization_barrier(0.5 * mode_energy)
        return jnp.swapaxes(mode_energy.reshape(half, 2, 4, half), 1, 2).reshape(influence.shape), energy

    return jax.shard_map(local_energy, mesh=mesh, in_specs=(slot_spec, slot_spec, P(('sys', 'ydom', 'zdom'), None), P(('sys', 'ydom', 'zdom'), None, None), mode_spec), out_specs=(mode_spec, P('sys')), check_vma=False)
```
